8 devices in a mesh: dp: 2 (over z, y), tp: 4 (over x, core).
Axes of the slice: x: 2, y: 2, z: 1, core: 2. Of those that a mesh axis runs over, the one named last changes fastest.
Arguments:
- patches: bfloat16 [128, 256, 768], P('dp', 'tp'), parts along dimension 0
- patch_w: bfloat16 [768, 768], replicated
- patch_b: bfloat16 [768], replicated
- pos_emb: bfloat16 [256, 768], P('tp')
- ln_scale: bfloat16 [2, 768], replicated
- ln_bias: bfloat16 [2, 768], replicated
- qkv_w: bfloat16 [3, 768, 12, 64], P(None, None, 'tp')
- qkv_b: bfloat16 [3, 12, 64], P(None, 'tp')
- out_w: bfloat16 [12, 64, 768], P('tp')
- out_b: bfloat16 [768], replicated
- fc1_w: bfloat16 [768, 3072], P(None, 'tp')
- fc1_b: bfloat16 [3072], P('tp')
- fc2_w: bfloat16 [3072, 768], P('tp')
- fc2_b: bfloat16 [768], replicated
- d_out: bfloat16 [128, 256, 768], P('dp', 'tp'), parts along dimension 0
Outputs:
- output 1: bfloat16 [128, 256, 768], P('dp', 'tp'), parts along dimension 0
- output 2: bfloat16 [1536, 768], P('dp'), parts along dimension 0
- output 3: bfloat16 [1536], P('dp'), parts along dimension 0
- output 4: bfloat16 [512, 768], P(('dp', 'tp')), parts along dimension 0
- output 5: bfloat16 [4, 768], P('dp'), parts along dimension 0
- output 6: bfloat16 [4, 768], P('dp'), parts along dimension 0
- output 7: bfloat16 [6, 768, 12, 64], P('dp', None, 'tp'), parts along dimension 0
- output 8: bfloat16 [6, 12, 64], P('dp', 'tp'), parts along dimension 0
- output 9: bfloat16 [24, 64, 768], P(('dp', 'tp')), parts along dimension 0
- output 10: bfloat16 [1536], P('dp'), parts along dimension 0
- output 11: bfloat16 [1536, 3072], P('dp', 'tp'), parts along dimension 0
- output 12: bfloat16 [6144], P(('dp', 'tp')), parts along dimension 0
- output 13: bfloat16 [6144, 768], P(('dp', 'tp')), parts along dimension 0
- output 14: bfloat16 [1536], P('dp'), parts along dimension 0
There are 2 independent parts. The reference program is written for one: setup_inputs(seed, part) draws one part's arguments, and reference() takes and returns one part's arrays. A program takes and returns all parts, laid end to end along the dimension named above; an argument that names none is the same for every part.
All inputs are finite; a program needn't handle non-finite values.
Results may differ from the reference program's by a relative error of at most 0.0189636.
Values are sent between devices in bfloat16 or wider.
A program may use at most 1 GiB of HBM per device.

```python
import functools
import jax
import jax.numpy as jnp
from jax import lax

NUM_IMAGES = 64
NUM_TOKENS = 256
PATCH_DIM = 768
MODEL_DIM = 768
NUM_HEADS = 12
HEAD_DIM = 64
MLP_DIM = 3072
LN_EPS = 1e-6


def draw_normal(key, shape, scale):
    return (jax.random.normal(key, shape, jnp.float32) * scale).astype(jnp.bfloat16)


def setup_inputs(seed: int = 0, part: int = 0) -> dict:
    base_key = jax.random.key(seed)
    part_key = jax.random.fold_in(base_key, part)
    weight_keys = jax.random.split(base_key, 13)
    data_keys = jax.random.split(part_key, 2)
    qk_gain = 1.6 * MODEL_DIM ** -0.5
    qkv_gain = jnp.array([qk_gain, qk_gain, MODEL_DIM ** -0.5], jnp.float32).reshape(3, 1, 1, 1)
    ln_gain = 1.0 + 0.3 * jax.random.normal(weight_keys[3], (2, MODEL_DIM), jnp.float32)
    qkv_raw = jax.random.normal(weight_keys[5], (3, MODEL_DIM, NUM_HEADS, HEAD_DIM), jnp.float32)
    return {
        'patches': draw_normal(data_keys[0], (NUM_IMAGES, NUM_TOKENS, PATCH_DIM), 1.0),
        'patch_w': draw_normal(weight_keys[0], (PATCH_DIM, MODEL_DIM), PATCH_DIM ** -0.5),
        'patch_b': draw_normal(weight_keys[1], (MODEL_DIM,), 0.5),
        'pos_emb': draw_normal(weight_keys[2], (NUM_TOKENS, MODEL_DIM), 0.5),
        'ln_scale': ln_gain.astype(jnp.bfloat16),
        'ln_bias': draw_normal(weight_keys[4], (2, MODEL_DIM), 0.3),
        'qkv_w': (qkv_raw * qkv_gain).astype(jnp.bfloat16),
        'qkv_b': draw_normal(weight_keys[6], (3, NUM_HEADS, HEAD_DIM), 0.3),
        'out_w': draw_normal(weight_keys[7], (NUM_HEADS, HEAD_DIM, MODEL_DIM), MODEL_DIM ** -0.5),
        'out_b': draw_normal(weight_keys[8], (MODEL_DIM,), 0.5),
        'fc1_w': draw_normal(weight_keys[9], (MODEL_DIM, MLP_DIM), MODEL_DIM ** -0.5),
        'fc1_b': draw_normal(weight_keys[10], (MLP_DIM,), 0.5),
        'fc2_w': draw_normal(weight_keys[11], (MLP_DIM, MODEL_DIM), MLP_DIM ** -0.5),
        'fc2_b': draw_normal(weight_keys[12], (MODEL_DIM,), 0.5),
        'd_out': draw_normal(data_keys[1], (NUM_IMAGES, NUM_TOKENS, MODEL_DIM), 1.0),
    }


def layer_norm(x_val, scale, bias):
    row_mean = jnp.mean(x_val, axis=-1, keepdims=True)
    centered = x_val - row_mean
    row_var = jnp.mean(centered * centered, axis=-1, keepdims=True)
    return centered * lax.rsqrt(row_var + LN_EPS) * scale.astype(jnp.float32) + bias.astype(jnp.float32)


def attend_image(qkv_img):
    query = qkv_img[:, 0].astype(jnp.float32)
    keys_img = qkv_img[:, 1].astype(jnp.float32)
    values = qkv_img[:, 2].astype(jnp.float32)
    scores = jnp.einsum('qhc,khc->hqk', query, keys_img) * HEAD_DIM ** -0.5
    probs = jax.nn.softmax(scores, axis=-1).astype(jnp.bfloat16)
    context = jnp.einsum('hqk,khc->qhc', probs.astype(jnp.float32), values)
    return context.astype(jnp.bfloat16)


def forward(patches, params):
    patch_w, patch_b, pos_emb, ln_scale, ln_bias, qkv_w, qkv_b, out_w, out_b, fc1_w, fc1_b, fc2_w, fc2_b = params
    emb = jnp.einsum('btp,pd->btd', patches.astype(jnp.float32), patch_w.astype(jnp.float32))
    emb_f = (emb + patch_b.astype(jnp.float32) + pos_emb.astype(jnp.float32)).astype(jnp.bfloat16).astype(jnp.float32)
    h_one = layer_norm(emb_f, ln_scale[0], ln_bias[0]).astype(jnp.bfloat16)
    qkv = jnp.einsum('btd,sdhc->btshc', h_one.astype(jnp.float32), qkv_w.astype(jnp.float32)) + qkv_b.astype(jnp.float32)
    context = lax.map(jax.checkpoint(attend_image), qkv.astype(jnp.bfloat16))
    attn_out = jnp.einsum('bthc,hcd->btd', context.astype(jnp.float32), out_w.astype(jnp.float32)) + out_b.astype(jnp.float32)
    x_one_f = (emb_f + attn_out).astype(jnp.bfloat16).astype(jnp.float32)
    h_two = layer_norm(x_one_f, ln_scale[1], ln_bias[1]).astype(jnp.bfloat16)
    pre_act = jnp.einsum('btd,df->btf', h_two.astype(jnp.float32), fc1_w.astype(jnp.float32)) + fc1_b.astype(jnp.float32)
    hidden = jax.nn.gelu(pre_act, approximate=True).astype(jnp.bfloat16)
    mlp_out = jnp.einsum('btf,fd->btd', hidden.astype(jnp.float32), fc2_w.astype(jnp.float32)) + fc2_b.astype(jnp.float32)
    return (x_one_f + mlp_out).astype(jnp.bfloat16)


def reference(patches, patch_w, patch_b, pos_emb, ln_scale, ln_bias, qkv_w, qkv_b, out_w, out_b, fc1_w, fc1_b, fc2_w, fc2_b, d_out):
    params = (patch_w, patch_b, pos_emb, ln_scale, ln_bias, qkv_w, qkv_b, out_w, out_b, fc1_w, fc1_b, fc2_w, fc2_b)
    x_two, pull_back = jax.vjp(functools.partial(forward, patches), params)
    grads = pull_back(d_out)[0]
    return (x_two, grads[0], grads[1], grads[2], grads[3], grads[4], grads[5], grads[6], grads[7], grads[8], grads[9], grads[10], grads[11], grads[12])
```

```python
import jax
import jax.numpy as jnp
from jax import lax
from jax.sharding import PartitionSpec as P

LN_EPS = 1e-6
TP = 4


def permute_xor(x, k):
    return lax.ppermute(x, 'tp', [(i, i ^ k) for i in range(TP)])


def exchange(x, me):
    blocks = x.reshape((TP, x.shape[0] // TP) + x.shape[1:])
    out = []
    for k in range(TP):
        block = lax.dynamic_index_in_dim(blocks, me ^ k, 0, keepdims=False)
        out.append(block if k == 0 else permute_xor(block, k))
    return out


def give_back(slots, me):
    out = jnp.zeros((TP,) + slots[0].shape, slots[0].dtype)
    for k in range(TP):
        block = slots[k] if k == 0 else permute_xor(slots[k], k)
        out = lax.dynamic_update_index_in_dim(out, block, me ^ k, 0)
    return out.reshape((-1,) + slots[0].shape[1:])


def gather(w):
    w2 = permute_xor(w, 2)
    w1 = permute_xor(w, 1)
    w3 = permute_xor(w2, 1)
    return [w, w1, w2, w3]


def reduce_slots(g):
    r1 = permute_xor(g[1], 1)
    r3 = permute_xor(g[3], 1)
    a2 = g[2] + r3
    return (g[0] + r1) + permute_xor(a2, 2)


def layer_norm(x_val, scale_f, bias_f):
    row_mean = jnp.mean(x_val, axis=-1, keepdims=True)
    centered = x_val - row_mean
    row_var = jnp.mean(centered * centered, axis=-1, keepdims=True)
    return centered * lax.rsqrt(row_var + LN_EPS) * scale_f + bias_f


def gelu_tanh(pre_act):
    return jax.nn.gelu(pre_act, approximate=True)


def group_step(patches, patch_w, patch_b, pos_emb, ln_scale, ln_bias, qkv_w, qkv_b, out_w, out_b, fc1_w, fc1_b, fc2_w, fc2_b, d_out):
    wide = jnp.float32
    half = jnp.bfloat16
    me = lax.axis_index('tp')
    scale = qkv_w.shape[-1] ** -0.5
    ln_scale_f = ln_scale.astype(wide)
    ln_bias_f = ln_bias.astype(wide)
    patches = jnp.concatenate(exchange(patches, me), axis=1)
    pos_emb = jnp.concatenate(gather(pos_emb), axis=0)
    qkv_w = jnp.concatenate(gather(qkv_w), axis=2)
    qkv_b = jnp.concatenate(gather(qkv_b), axis=1)
    out_w = jnp.concatenate(gather(out_w), axis=0)
    fc1_w = jnp.concatenate(gather(fc1_w), axis=1)
    fc1_b = jnp.concatenate(gather(fc1_b), axis=0)
    fc2_w = jnp.concatenate(gather(fc2_w), axis=0)
    d_out = jnp.concatenate(exchange(d_out, me), axis=1)
    emb = jnp.einsum('btp,pd->btd', patches, patch_w, preferred_element_type=wide)
    emb_f = (emb + patch_b.astype(wide) + pos_emb.astype(wide)).astype(half).astype(wide)
    h_one_f, ln_one_vjp = jax.vjp(layer_norm, emb_f, ln_scale_f[0], ln_bias_f[0])
    h_one_all = h_one_f.astype(half)
    qkv = jnp.einsum('btd,sdhc->btshc', h_one_all, qkv_w, preferred_element_type=wide)
    qkv = (qkv + qkv_b.astype(wide)).astype(half)
    query = qkv[:, :, 0]
    keys_all = qkv[:, :, 1]
    values = qkv[:, :, 2]
    scores = jnp.einsum('bqhc,bkhc->bhqk', query, keys_all, preferred_element_type=wide) * scale
    probs = jax.nn.softmax(scores, axis=-1)
    probs_h = probs.astype(half)
    context = jnp.einsum('bhqk,bkhc->bqhc', probs_h, values, preferred_element_type=wide).astype(half)
    attn_out = jnp.einsum('crid,ide->cre', context, out_w, preferred_element_type=wide)
    x_one_f = (emb_f + (attn_out + out_b.astype(wide))).astype(half).astype(wide)
    h_two_f, ln_two_vjp = jax.vjp(layer_norm, x_one_f, ln_scale_f[1], ln_bias_f[1])
    h_two_all = h_two_f.astype(half)
    pre_act = jnp.einsum('btd,df->btf', h_two_all, fc1_w, preferred_element_type=wide) + fc1_b.astype(wide)
    hidden_f, gelu_vjp = jax.vjp(gelu_tanh, pre_act)
    hidden = hidden_f.astype(half)
    mlp_out = jnp.einsum('btf,fd->btd', hidden, fc2_w, preferred_element_type=wide)
    x_two = (x_one_f + (mlp_out + fc2_b.astype(wide))).astype(half)
    x_two = give_back([x_two[:, 64 * k:64 * k + 64] for k in range(TP)], me)
    d_two_f = d_out.astype(wide)
    d_fc2_b = jnp.sum(d_two_f, axis=(0, 1))
    d_fc2_w = jnp.einsum('btf,btd->fd', hidden, d_out, preferred_element_type=wide)
    d_hidden = jnp.einsum('btd,fd->btf', d_out, fc2_w, preferred_element_type=wide).astype(half)
    d_pre = gelu_vjp(d_hidden.astype(wide))[0]
    d_fc1_b = jnp.sum(d_pre, axis=(0, 1))
    d_pre_h = d_pre.astype(half)
    d_fc1_w = jnp.einsum('btd,btf->df', h_two_all, d_pre_h, preferred_element_type=wide)
    d_h_two = jnp.einsum('btf,df->btd', d_pre_h, fc1_w, preferred_element_type=wide).astype(half)
    d_x_ln, d_ln2_scale, d_ln2_bias = ln_two_vjp(d_h_two.astype(wide))
    d_x_one = (d_two_f + d_x_ln).astype(half)
    d_out_b = jnp.sum(d_x_one, axis=(0, 1), dtype=wide)
    d_out_w = jnp.einsum('crid,cre->ide', context, d_x_one, preferred_element_type=wide)
    d_context = jnp.einsum('cre,ide->crid', d_x_one, out_w, preferred_element_type=wide).astype(half)
    d_values = jnp.einsum('bhqk,bqhc->bkhc', probs_h, d_context, preferred_element_type=wide).astype(half)
    d_probs = jnp.einsum('bqhc,bkhc->bhqk', d_context, values, preferred_element_type=wide).astype(half).astype(wide)
    d_scores = probs * (d_probs - jnp.sum(d_probs * probs, axis=-1, keepdims=True))
    d_scores_h = (d_scores * scale).astype(half)
    d_query = jnp.einsum('bhqk,bkhc->bqhc', d_scores_h, keys_all, preferred_element_type=wide).astype(half)
    d_keys = jnp.einsum('bhqk,bqhc->bkhc', d_scores_h, query, preferred_element_type=wide).astype(half)
    d_qkv = jnp.stack([d_query, d_keys, d_values], axis=2)
    d_qkv_b = jnp.sum(d_qkv, axis=(0, 1), dtype=wide)
    d_qkv_w = jnp.einsum('btd,btshc->sdhc', h_one_all, d_qkv, preferred_element_type=wide)
    d_h_one = jnp.einsum('btshc,sdhc->btd', d_qkv, qkv_w, preferred_element_type=wide).astype(half)
    d_emb_ln, d_ln1_scale, d_ln1_bias = ln_one_vjp(d_h_one.astype(wide))
    d_emb = (d_x_one.astype(wide) + d_emb_ln).astype(half)
    d_pos = jnp.sum(d_emb, axis=0, dtype=wide)
    d_patch_b = jnp.sum(d_emb, axis=(0, 1), dtype=wide)
    d_patch_w = jnp.einsum('btp,btd->pd', patches, d_emb, preferred_element_type=wide)
    d_fc2_w = reduce_slots([d_fc2_w[768 * k:768 * k + 768] for k in range(TP)])
    d_fc1_w = reduce_slots([d_fc1_w[:, 768 * k:768 * k + 768] for k in range(TP)])
    d_out_w = reduce_slots([d_out_w[3 * k:3 * k + 3] for k in range(TP)])
    d_qkv_w = reduce_slots([d_qkv_w[:, :, 3 * k:3 * k + 3] for k in range(TP)])
    d_fc1_b = reduce_slots([d_fc1_b[768 * k:768 * k + 768] for k in range(TP)])
    d_qkv_b = reduce_slots([d_qkv_b[:, 3 * k:3 * k + 3] for k in range(TP)])
    d_pos = reduce_slots([d_pos[64 * k:64 * k + 64] for k in range(TP)])
    vec = jnp.stack([d_patch_b, d_ln1_scale, d_ln2_scale, d_ln1_bias, d_ln2_bias, d_out_b, d_fc2_b, d_fc2_b])
    vec = vec + permute_xor(vec, 1)
    vec = (vec + permute_xor(vec, 2)).astype(half)
    core = me % 2
    halves = d_patch_w.reshape(2, 384, 768)
    mine = lax.dynamic_index_in_dim(halves, core, 0, keepdims=False)
    other = lax.dynamic_index_in_dim(halves, 1 - core, 0, keepdims=False)
    mine = mine + permute_xor(other, 1)
    mine = (mine + permute_xor(mine, 2)).astype(half)
    theirs = permute_xor(mine, 1)
    first = core == 0
    d_patch_w = jnp.concatenate([jnp.where(first, mine, theirs), jnp.where(first, theirs, mine)], axis=0)
    return (x_two, d_patch_w, vec[0], d_pos.astype(half), vec[1:3], vec[3:5], d_qkv_w.astype(half), d_qkv_b.astype(half), d_out_w.astype(half), vec[5], d_fc1_w.astype(half), d_fc1_b.astype(half), d_fc2_w.astype(half), vec[6])


def solution(mesh):
    in_specs = (P('dp', 'tp', None), P(), P(), P('tp', None), P(), P(), P(None, None, 'tp', None), P(None, 'tp', None), P('tp', None, None), P(), P(None, 'tp'), P('tp'), P('tp', None), P(), P('dp', 'tp', None))
    out_specs = (P('dp', 'tp', None), P('dp', None), P('dp'), P(('dp', 'tp'), None), P('dp', None), P('dp', None), P('dp', None, 'tp', None), P('dp', 'tp', None), P(('dp', 'tp'), None, None), P('dp'), P('dp', 'tp'), P(('dp', 'tp')), P(('dp', 'tp'), None), P('dp'))
    return jax.shard_map(group_step, mesh=mesh, in_specs=in_specs, out_specs=out_specs, check_vma=False)
```

```python
import functools
import jax
import jax.numpy as jnp
from jax import lax
from jax.experimental import pallas as pl
from jax.experimental.pallas import tpu as pltpu
from jax.sharding import PartitionSpec as P

LN_EPS = 1e-6
TP = 4
WIDE = jnp.float32
HALF = jnp.bfloat16
IMAGES = 16
TOK = 256
PART = 64
DIM = 768
GROUP = 2
ROWS = GROUP * TOK
STEPS = IMAGES // GROUP
PAIRS = 6
EXP_SCALE = 0.125 * 1.4426950408889634
GELU_C = 0.7978845608028654
GELU_A = 0.044715


def dot_nn(a, b):
    return lax.dot_general(a, b, (((1,), (0,)), ((), ())), preferred_element_type=WIDE)


def dot_nt(a, b):
    return lax.dot_general(a, b, (((1,), (1,)), ((), ())), preferred_element_type=WIDE)


def dot_tn(a, b):
    return lax.dot_general(a, b, (((0,), (0,)), ((), ())), preferred_element_type=WIDE)


def rows_of(slot_refs):
    return jnp.concatenate([r[g] for g in range(GROUP) for r in slot_refs], axis=0)


def stack_rows(refs, s):
    return jnp.concatenate([r[s] for r in refs], axis=0)


def join_rows(refs):
    return jnp.concatenate([r[...] for r in refs], axis=0)


def normalize(x_f):
    mean = jnp.sum(x_f, axis=-1, keepdims=True) * (1.0 / DIM)
    centered = x_f - mean
    var = jnp.sum(centered * centered, axis=-1, keepdims=True) * (1.0 / DIM)
    inv = lax.rsqrt(var + LN_EPS)
    return centered * inv, inv


def norm_back(d_out_f, xhat, inv, scale):
    d_hat = d_out_f * scale
    m1 = jnp.sum(d_hat, axis=-1, keepdims=True) * (1.0 / DIM)
    m2 = jnp.sum(d_hat * xhat, axis=-1, keepdims=True) * (1.0 / DIM)
    return (d_hat - m1 - xhat * m2) * inv


def lane_half(j):
    lane = lax.broadcasted_iota(jnp.int32, (1, 128), 1)
    return (lane < 64) if j == 0 else (lane >= 64)


def mask_half(x, j):
    return jnp.where(lane_half(j), x, jnp.zeros_like(x))


def col_sum(x):
    return jnp.sum(x, axis=0, keepdims=True)


def attn_fwd_kernel(p0, p1, p2, p3, pos, wp, vec, wq0, wq1, wq2, wq3, bqkv, wo0, wo1, wo2, wo3, e_ref, qkv_ref, o_ref, x1_ref):
    x = rows_of((p0, p1, p2, p3))
    posb = pos[...].astype(WIDE) + vec[0:1]
    emb = dot_nn(x, wp[...]) + jnp.concatenate([posb] * GROUP, axis=0)
    e_h = emb.astype(HALF)
    for g in range(GROUP):
        e_ref[g] = e_h[TOK * g:TOK * g + TOK]
    e_f = e_h.astype(WIDE)
    xhat, _ = normalize(e_f)
    h1 = (xhat * vec[1:2] + vec[2:3]).astype(HALF)
    for s in range(3):
        part = (dot_nt(h1, stack_rows((wq0, wq1, wq2, wq3), s)) + bqkv[s:s + 1]).astype(HALF)
        for g in range(GROUP):
            qkv_ref[g, :, DIM * s:DIM * s + DIM] = part[TOK * g:TOK * g + TOK]
    for g in range(GROUP):
        for pr in range(PAIRS):
            q = qkv_ref[g, :, 128 * pr:128 * pr + 128]
            k = qkv_ref[g, :, DIM + 128 * pr:DIM + 128 * pr + 128]
            v = qkv_ref[g, :, 2 * DIM + 128 * pr:2 * DIM + 128 * pr + 128]
            probs = []
            for j in range(2):
                s = dot_nt(mask_half(q, j), k)
                m = jnp.max(s, axis=-1, keepdims=True)
                e = jnp.exp2((s - m) * EXP_SCALE)
                l = jnp.sum(e, axis=-1, keepdims=True)
                probs.append((e * (1.0 / l)).astype(HALF))
            pv = dot_nn(jnp.concatenate(probs, axis=1), jnp.concatenate([mask_half(v, 0), mask_half(v, 1)], axis=0))
            o_ref[g, :, 128 * pr:128 * pr + 128] = pv.astype(HALF)
    o = jnp.concatenate([o_ref[g] for g in range(GROUP)], axis=0)
    e_f = jnp.concatenate([e_ref[g] for g in range(GROUP)], axis=0).astype(WIDE)
    x1 = (e_f + (dot_nn(o, join_rows((wo0, wo1, wo2, wo3))) + vec[3:4])).astype(HALF)
    for g in range(GROUP):
        x1_ref[g] = x1[TOK * g:TOK * g + TOK]


def fixed(shape):
    return pl.BlockSpec(shape, lambda i: (0,) * len(shape), pipeline_mode=pl.Buffered(1))


def slot_spec():
    return pl.BlockSpec((GROUP, PART, DIM), lambda i: (i, 0, 0))


def image_spec(width):
    return pl.BlockSpec((GROUP, TOK, width), lambda i: (i, 0, 0))


def params():
    return pltpu.CompilerParams(dimension_semantics=('arbitrary',), vmem_limit_bytes=63 * 1024 * 1024)


def image_shape(width):
    return jax.ShapeDtypeStruct((IMAGES, TOK, width), HALF)


def attn_fwd(p, pos, wp, vec, wqkv, bqkv, wo):
    return pl.pallas_call(
        attn_fwd_kernel,
        grid=(STEPS,),
        in_specs=[slot_spec()] * 4 + [fixed((TOK, DIM)), fixed((DIM, DIM)), fixed((8, DIM))] + [fixed((3, 192, DIM))] * 4 + [fixed((8, DIM))] + [fixed((192, DIM))] * 4,
        out_specs=[image_spec(DIM), image_spec(3 * DIM), image_spec(DIM), image_spec(DIM)],
        out_shape=[image_shape(DIM), image_shape(3 * DIM), image_shape(DIM), image_shape(DIM)],
        compiler_params=params(),
        cost_estimate=pl.CostEstimate(flops=60_000_000_000, bytes_accessed=50_000_000, transcendentals=12_000_000),
        name='attn_fwd',
    )(*p, pos, wp, vec, *wqkv, bqkv, *wo)


def mlp_kernel(x1_ref, o_ref, d0, d1, d2, d3, w10, w11, w12, w13, b1, w20, w21, w22, w23, wo0, wo1, wo2, wo3, vec, y0, y1, y2, y3, dx1_ref, do_ref, dw1_out, dw2_out, dwo_out, dvec_ref, db1_ref, dw1, dw2, dwo, sems):
    step = pl.program_id(0)
    w1 = (w10, w11, w12, w13)
    w2 = (w20, w21, w22, w23)

    @pl.when(step == 0)
    def _():
        dw1[...] = jnp.zeros_like(dw1)
        dw2[...] = jnp.zeros_like(dw2)
        dwo[...] = jnp.zeros_like(dwo)
        dvec_ref[...] = jnp.zeros_like(dvec_ref)
        db1_ref[...] = jnp.zeros_like(db1_ref)

    x1 = jnp.concatenate([x1_ref[g] for g in range(GROUP)], axis=0)
    dout = rows_of((d0, d1, d2, d3))
    xhat, inv = normalize(x1.astype(WIDE))
    h2 = (xhat * vec[0:1] + vec[1:2]).astype(HALF)
    y = None
    dh2 = None
    for f in range(TP):
        pre = dot_nn(h2, w1[f][...]) + b1[f:f + 1]
        sq = pre * pre
        t = jnp.tanh(pre * (GELU_C + (GELU_C * GELU_A) * sq))
        half_pre = 0.5 * pre
        hid = (half_pre + half_pre * t).astype(HALF)
        slope = (0.5 + 0.5 * t) + (half_pre * (1.0 - t * t)) * (GELU_C + (3.0 * GELU_C * GELU_A) * sq)
        dhid = dot_nt(dout, w2[f][...]).astype(HALF).astype(WIDE)
        dpre = dhid * slope
        db1_ref[f:f + 1] += col_sum(dpre)
        dpre_h = dpre.astype(HALF)
        part_y = dot_nn(hid, w2[f][...])
        part_h = dot_nt(dpre_h, w1[f][...])
        y = part_y if y is None else y + part_y
        dh2 = part_h if dh2 is None else dh2 + part_h
        dw1[f] += dot_tn(h2, dpre_h)
        dw2[f] += dot_tn(dout, hid)
    x2 = (x1.astype(WIDE) + (y + vec[2:3])).astype(HALF)
    for g in range(GROUP):
        for k, ref in enumerate((y0, y1, y2, y3)):
            ref[g] = x2[TOK * g + PART * k:TOK * g + PART * k + PART]
    dh2 = dh2.astype(HALF).astype(WIDE)
    xhat, inv = normalize(x1.astype(WIDE))
    dout_f = dout.astype(WIDE)
    dx1 = (dout_f + norm_back(dh2, xhat, inv, vec[0:1])).astype(HALF)
    dvec_ref[0:1] += col_sum(dh2 * xhat)
    dvec_ref[1:2] += col_sum(dh2)
    dvec_ref[2:3] += col_sum(dout_f)
    dvec_ref[3:4] += col_sum(dx1.astype(WIDE))
    d_o = dot_nt(dx1, join_rows((wo0, wo1, wo2, wo3))).astype(HALF)
    for g in range(GROUP):
        dx1_ref[g] = dx1[TOK * g:TOK * g + TOK]
        do_ref[g] = d_o[TOK * g:TOK * g + TOK]
    o = jnp.concatenate([o_ref[g] for g in range(GROUP)], axis=0)
    dwo[...] += dot_tn(o, dx1)

    @pl.when(step == STEPS - 1)
    def _():
        copies = [pltpu.make_async_copy(src, dst, sems.at[n]) for n, (src, dst) in enumerate(((dw1, dw1_out), (dw2, dw2_out), (dwo, dwo_out)))]
        for c in copies:
            c.start()
        for c in copies:
            c.wait()


def mlp(x1, o, dout, w1, b1, w2, wo, vec):
    any_spec = pl.BlockSpec(memory_space=pl.ANY)
    slot_shape = jax.ShapeDtypeStruct((IMAGES, PART, DIM), HALF)
    return pl.pallas_call(
        mlp_kernel,
        grid=(STEPS,),
        in_specs=[image_spec(DIM), image_spec(DIM)] + [slot_spec()] * 4 + [fixed((DIM, DIM))] * 4 + [fixed((8, DIM))] + [fixed((DIM, DIM))] * 4 + [fixed((192, DIM))] * 4 + [fixed((8, DIM))],
        out_specs=[slot_spec()] * 4 + [image_spec(DIM), image_spec(DIM), any_spec, any_spec, any_spec, pl.BlockSpec((8, DIM), lambda i: (0, 0)), pl.BlockSpec((8, DIM), lambda i: (0, 0))],
        out_shape=[slot_shape] * 4 + [image_shape(DIM), image_shape(DIM), jax.ShapeDtypeStruct((TP, DIM, DIM), WIDE), jax.ShapeDtypeStruct((TP, DIM, DIM), WIDE), jax.ShapeDtypeStruct((DIM, DIM), WIDE), jax.ShapeDtypeStruct((8, DIM), WIDE), jax.ShapeDtypeStruct((8, DIM), WIDE)],
        scratch_shapes=[pltpu.VMEM((TP, DIM, DIM), WIDE), pltpu.VMEM((TP, DIM, DIM), WIDE), pltpu.VMEM((DIM, DIM), WIDE), pltpu.SemaphoreType.DMA((3,))],
        compiler_params=params(),
        cost_estimate=pl.CostEstimate(flops=130_000_000_000, bytes_accessed=80_000_000, transcendentals=12_000_000),
        name='mlp',
    )(x1, o, *dout, *w1, b1, *w2, *wo, vec)


def attn_bwd_kernel(e_ref, qkv_ref, do_ref, dx1_ref, p0, p1, p2, p3, wq0, wq1, wq2, wq3, vec, dwqkv_out, dwp_out, dpos_ref, dvec_ref, dbqkv_ref, dqkv, dwqkv, dwp, sems):
    step = pl.program_id(0)

    @pl.when(step == 0)
    def _():
        dwqkv[...] = jnp.zeros_like(dwqkv)
        dwp[...] = jnp.zeros_like(dwp)
        dpos_ref[...] = jnp.zeros_like(dpos_ref)
        dvec_ref[...] = jnp.zeros_like(dvec_ref)
        dbqkv_ref[...] = jnp.zeros_like(dbqkv_ref)

    for g in range(GROUP):
        rows = slice(TOK * g, TOK * g + TOK)
        for pr in range(PAIRS):
            cols = slice(128 * pr, 128 * pr + 128)
            q = qkv_ref[g, :, 128 * pr:128 * pr + 128]
            k = qkv_ref[g, :, DIM + 128 * pr:DIM + 128 * pr + 128]
            v = qkv_ref[g, :, 2 * DIM + 128 * pr:2 * DIM + 128 * pr + 128]
            d_o = do_ref[g, :, 128 * pr:128 * pr + 128]
            probs = []
            dscores = []
            for j in range(2):
                s = dot_nt(k, mask_half(q, j))
                m = jnp.max(s, axis=0, keepdims=True)
                e = jnp.exp2((s - m) * EXP_SCALE)
                l = jnp.sum(e, axis=0, keepdims=True)
                p = e * (1.0 / l)
                dp = dot_nt(v, mask_half(d_o, j)).astype(HALF).astype(WIDE)
                delta = jnp.sum(dp * p, axis=0, keepdims=True)
                ds = (p * ((dp - delta) * 0.125)).astype(HALF)
                probs.append(p.astype(HALF))
                dscores.append(ds)
            dv = dot_nn(jnp.concatenate(probs, axis=1), jnp.concatenate([mask_half(d_o, 0), mask_half(d_o, 1)], axis=0))
            dk = dot_nn(jnp.concatenate(dscores, axis=1), jnp.concatenate([mask_half(q, 0), mask_half(q, 1)], axis=0))
            dq = dot_tn(jnp.concatenate(dscores, axis=0), jnp.concatenate([mask_half(k, 0), mask_half(k, 1)], axis=0))
            dqkv[rows, 128 * pr:128 * pr + 128] = dq.astype(HALF)
            dqkv[rows, DIM + 128 * pr:DIM + 128 * pr + 128] = dk.astype(HALF)
            dqkv[rows, 2 * DIM + 128 * pr:2 * DIM + 128 * pr + 128] = dv.astype(HALF)
    e_f = jnp.concatenate([e_ref[g] for g in range(GROUP)], axis=0).astype(WIDE)
    xhat, inv = normalize(e_f)
    h1 = (xhat * vec[1:2] + vec[2:3]).astype(HALF)
    dh1 = None
    for s in range(3):
        part = dqkv[:, DIM * s:DIM * s + DIM]
        dbqkv_ref[s:s + 1] += col_sum(part.astype(WIDE))
        dwqkv[s] += dot_tn(part, h1)
        term = dot_nn(part, stack_rows((wq0, wq1, wq2, wq3), s))
        dh1 = term if dh1 is None else dh1 + term
    dh1 = dh1.astype(HALF).astype(WIDE)
    dx1 = jnp.concatenate([dx1_ref[g] for g in range(GROUP)], axis=0).astype(WIDE)
    de = (dx1 + norm_back(dh1, xhat, inv, vec[1:2])).astype(HALF)
    de_f = de.astype(WIDE)
    dvec_ref[0:1] += col_sum(dh1 * xhat)
    dvec_ref[1:2] += col_sum(dh1)
    acc = de_f[0:TOK]
    for g in range(1, GROUP):
        acc = acc + de_f[TOK * g:TOK * g + TOK]
    dpos_ref[...] += acc
    x = rows_of((p0, p1, p2, p3))
    dwp[...] += dot_tn(x, de)

    @pl.when(step == STEPS - 1)
    def _():
        copies = [pltpu.make_async_copy(src, dst, sems.at[n]) for n, (src, dst) in enumerate(((dwqkv, dwqkv_out), (dwp, dwp_out)))]
        for c in copies:
            c.start()
        for c in copies:
            c.wait()


def attn_bwd(e, qkv, d_o, dx1, p, wqkv, vec):
    any_spec = pl.BlockSpec(memory_space=pl.ANY)
    return pl.pallas_call(
        attn_bwd_kernel,
        grid=(STEPS,),
        in_specs=[image_spec(DIM), image_spec(3 * DIM), image_spec(DIM), image_spec(DIM)] + [slot_spec()] * 4 + [fixed((3, 192, DIM))] * 4 + [fixed((8, DIM))],
        out_specs=[any_spec, any_spec, pl.BlockSpec((TOK, DIM), lambda i: (0, 0)), pl.BlockSpec((8, DIM), lambda i: (0, 0)), pl.BlockSpec((8, DIM), lambda i: (0, 0))],
        out_shape=[jax.ShapeDtypeStruct((3, DIM, DIM), WIDE), jax.ShapeDtypeStruct((DIM, DIM), WIDE), jax.ShapeDtypeStruct((TOK, DIM), WIDE), jax.ShapeDtypeStruct((8, DIM), WIDE), jax.ShapeDtypeStruct((8, DIM), WIDE)],
        scratch_shapes=[pltpu.VMEM((ROWS, 3 * DIM), HALF), pltpu.VMEM((3, DIM, DIM), WIDE), pltpu.VMEM((DIM, DIM), WIDE), pltpu.SemaphoreType.DMA((2,))],
        compiler_params=params(),
        cost_estimate=pl.CostEstimate(flops=100_000_000_000, bytes_accessed=80_000_000, transcendentals=12_000_000),
        name='attn_bwd',
    )(e, qkv, d_o, dx1, *p, *wqkv, vec)


def permute_xor(x, k):
    return lax.ppermute(x, 'tp', [(i, i ^ k) for i in range(TP)])


def exchange(x, me):
    blocks = x.reshape(TP, IMAGES, PART, DIM)
    picks = [lax.dynamic_index_in_dim(blocks, me ^ k, 0, keepdims=False) for k in range(TP)]
    return [picks[0]] + [permute_xor(picks[k], k) for k in range(1, TP)]


def give_back(slots, me):
    out = jnp.zeros((TP, IMAGES, PART, DIM), HALF)
    for k in range(TP):
        block = slots[k] if k == 0 else permute_xor(slots[k], k)
        out = lax.dynamic_update_index_in_dim(out, block, me ^ k, 0)
    return out.reshape(TP * IMAGES, PART, DIM)


def gather(w):
    w2 = permute_xor(w, 2)
    return [w, permute_xor(w, 1), w2, permute_xor(w2, 1)]


def reduce_slots(g):
    r1 = permute_xor(g[1], 1)
    r3 = permute_xor(g[3], 1)
    return (g[0] + r1) + permute_xor(g[2] + r3, 2)


def pad_rows(rows):
    rows = [r.astype(WIDE).reshape(-1, DIM) for r in rows]
    n = sum(r.shape[0] for r in rows)
    return jnp.concatenate(rows + [jnp.zeros((8 - n, DIM), WIDE)], axis=0)


def group_step(patches, patch_w, patch_b, pos_emb, ln_scale, ln_bias, qkv_w, qkv_b, out_w, out_b, fc1_w, fc1_b, fc2_w, fc2_b, d_out):
    me = lax.axis_index('tp')
    p = exchange(patches, me)
    wqkv = gather(qkv_w.transpose(0, 2, 3, 1).reshape(3, 192, DIM))
    small = jnp.concatenate([pos_emb, jnp.pad(qkv_b.reshape(3, 192), ((0, 0), (0, DIM - 192))), fc1_b.reshape(1, DIM), jnp.zeros((12, DIM), HALF)], axis=0)
    small = gather(small)
    wo = gather(out_w.reshape(192, DIM))
    w1 = gather(fc1_w)
    w2 = gather(fc2_w)
    dout = exchange(d_out, me)
    pos = jnp.concatenate([s[0:PART] for s in small], axis=0)
    bqkv = pad_rows([jnp.concatenate([s[PART:PART + 3, :192] for s in small], axis=1)])
    b1 = pad_rows([s[PART + 3] for s in small])
    vec1 = pad_rows([patch_b, ln_scale[0], ln_bias[0], out_b])
    vec2 = pad_rows([ln_scale[1], ln_bias[1], fc2_b])
    e, qkv, o, x1 = attn_fwd(p, pos, patch_w, vec1, wqkv, bqkv, wo)
    y0, y1, y2, y3, dx1, d_o, dw1, dw2, dwo, dvec2, db1 = mlp(x1, o, dout, w1, b1, w2, wo, vec2)
    x_two = give_back([y0, y1, y2, y3], me)
    d_fc2_w = reduce_slots([dw2[k] for k in range(TP)]).T
    d_fc1_w = reduce_slots([dw1[k] for k in range(TP)])
    d_out_w = reduce_slots([dwo[192 * k:192 * k + 192] for k in range(TP)])
    dwqkv, dwp, dpos, dvec1, dbqkv = attn_bwd(e, qkv, d_o, dx1, p, wqkv, vec1)
    d_qkv_w = reduce_slots([dwqkv[:, 192 * k:192 * k + 192] for k in range(TP)])
    d_qkv_w = d_qkv_w.astype(HALF).reshape(3, 3, 64, DIM).transpose(0, 3, 1, 2)
    small = reduce_slots([jnp.concatenate([dpos[PART * k:PART * k + PART], jnp.pad(dbqkv[0:3, 192 * k:192 * k + 192], ((0, 0), (0, DIM - 192))), db1[k:k + 1], jnp.zeros((4, DIM), WIDE)], axis=0) for k in range(TP)])
    d_pos = small[0:PART]
    d_qkv_b = small[PART:PART + 3, :192].reshape(3, 3, 64)
    d_fc1_b = small[PART + 3]
    d_patch_b = jnp.sum(dpos, axis=0)
    vec = pad_rows([d_patch_b, dvec1[0], dvec2[0], dvec1[1], dvec2[1], dvec2[3], dvec2[2]])
    vec = vec + permute_xor(vec, 1)
    vec = (vec + permute_xor(vec, 2)).astype(HALF)
    core = me % 2
    halves = dwp.reshape(2, 384, DIM)
    mine = lax.dynamic_index_in_dim(halves, core, 0, keepdims=False)
    other = lax.dynamic_index_in_dim(halves, 1 - core, 0, keepdims=False)
    mine = mine + permute_xor(other, 1)
    mine = (mine + permute_xor(mine, 2)).astype(HALF)
    theirs = permute_xor(mine, 1)
    first = core == 0
    d_patch_w = jnp.concatenate([jnp.where(first, mine, theirs), jnp.where(first, theirs, mine)], axis=0)
    return (x_two, d_patch_w, vec[0], d_pos.astype(HALF), vec[1:3], vec[3:5], d_qkv_w, d_qkv_b.astype(HALF), d_out_w.astype(HALF).reshape(3, 64, DIM), vec[5], d_fc1_w.astype(HALF), d_fc1_b.astype(HALF), d_fc2_w.astype(HALF), vec[6])


def solution(mesh):
    in_specs = (P('dp', 'tp', None), P(), P(), P('tp', None), P(), P(), P(None, None, 'tp', None), P(None, 'tp', None), P('tp', None, None), P(), P(None, 'tp'), P('tp'), P('tp', None), P(), P('dp', 'tp', None))
    out_specs = (P('dp', 'tp', None), P('dp', None), P('dp'), P(('dp', 'tp'), None), P('dp', None), P('dp', None), P('dp', None, 'tp', None), P('dp', 'tp', None), P(('dp', 'tp'), None, None), P('dp'), P('dp', 'tp'), P(('dp', 'tp')), P(('dp', 'tp'), None), P('dp'))
    return jax.shard_map(group_step, mesh=mesh, in_specs=in_specs, out_specs=out_specs, check_vma=False)
```

```python
import functools
import jax
import jax.numpy as jnp
from jax import lax
from jax.experimental import pallas as pl
from jax.experimental.pallas import tpu as pltpu
from jax.sharding import PartitionSpec as P

LN_EPS = 1e-6
TP = 4
WIDE = jnp.float32
HALF = jnp.bfloat16
IMAGES = 16
TOK = 256
PART = 64
DIM = 768
GROUP = 2
ROWS = GROUP * TOK
STEPS = IMAGES // GROUP
PAIRS = 6
EXP_SCALE = 0.125 * 1.4426950408889634
GELU_C = 0.7978845608028654
GELU_A = 0.044715
AHEAD = 3
PACK = 2 * DIM + 192


def dot_nn(a, b):
    return lax.dot_general(a, b, (((1,), (0,)), ((), ())), preferred_element_type=WIDE)


def dot_nt(a, b):
    return lax.dot_general(a, b, (((1,), (1,)), ((), ())), preferred_element_type=WIDE)


def dot_tn(a, b):
    return lax.dot_general(a, b, (((0,), (0,)), ((), ())), preferred_element_type=WIDE)


def normalize(x_f):
    mean = jnp.sum(x_f, axis=-1, keepdims=True) * (1.0 / DIM)
    centered = x_f - mean
    var = jnp.sum(centered * centered, axis=-1, keepdims=True) * (1.0 / DIM)
    inv = lax.rsqrt(var + LN_EPS)
    return centered * inv, inv


def norm_back(d_out_f, xhat, inv, scale):
    d_hat = d_out_f * scale
    m1 = jnp.sum(d_hat, axis=-1, keepdims=True) * (1.0 / DIM)
    m2 = jnp.sum(d_hat * xhat, axis=-1, keepdims=True) * (1.0 / DIM)
    return (d_hat - m1 - xhat * m2) * inv


def lane_half(j):
    lane = lax.broadcasted_iota(jnp.int32, (1, 128), 1)
    return (lane < 64) if j == 0 else (lane >= 64)


def mask_half(x, j):
    return jnp.where(lane_half(j), x, jnp.zeros_like(x))


def col_sum(x):
    return jnp.sum(x, axis=0, keepdims=True)


def peers():
    me = lax.axis_index('tp')
    core = lax.rem(me, 2)
    chip = lax.div(me, 2)
    return me, core, (me, me + 1 - 2 * core, me + 2 - 4 * chip, 3 - me)


def meet(others):
    barrier = pltpu.get_barrier_semaphore()
    for k in range(1, TP):
        pl.semaphore_signal(barrier, inc=1, device_id={'tp': others[k]}, device_id_type=pl.DeviceIdType.MESH)
    pl.semaphore_wait(barrier, TP - 1)


def push(src, dst, send, recv, peer):
    return pltpu.make_async_remote_copy(src_ref=src, dst_ref=dst, send_sem=send, recv_sem=recv, device_id={'tp': peer}, device_id_type=pl.DeviceIdType.MESH)


def image_rows(owner, group):
    return pl.ds(owner * IMAGES + group * GROUP, GROUP)


def group_sends(src, buf, send, recv, others, group):
    return [push(src.at[image_rows(others[k], group)], buf.at[k, pl.ds(group * GROUP, GROUP)], send.at[k - 1, group], recv.at[k - 1, group], others[k]) for k in (2, 3, 1)]


def slot_rows(buf, group):
    base = group * GROUP
    return jnp.concatenate([buf[k, base + g] for g in range(GROUP) for k in range(TP)], axis=0)


def attn_fwd_kernel(patches, wq_own, wop_own, bias_own, w1_own, w2_own, wp, vec, e_ref, qkv_ref, o_ref, x1_ref, x_ref, wq_out, wop_out, bias_out, w1_out, w2_out, xbuf, wq, wop, bias, x_send, x_recv, w_send, w_recv, local):
    step = pl.program_id(0)
    me, core, others = peers()
    small = []
    for n, (src, buf) in enumerate(((wq_own, wq), (wop_own, wop))):
        small.append((push(src, buf.at[2], w_send.at[n, 1], w_recv.at[n, 1], others[2]), push(src, buf.at[1], w_send.at[n, 0], w_recv.at[n, 0], others[1]), push(buf.at[2], buf.at[3], w_send.at[n, 2], w_recv.at[n, 2], others[1])))
    large = []
    for n, (src, out) in enumerate(((w1_own, w1_out), (w2_own, w2_out))):
        large.append((push(src, out.at[1], w_send.at[n + 2, 1], w_recv.at[n + 2, 1], others[2]), push(src, out.at[0], w_send.at[n + 2, 0], w_recv.at[n + 2, 0], others[1]), push(out.at[1], out.at[2], w_send.at[n + 2, 2], w_recv.at[n + 2, 2], others[1])))
    biases = [push(bias_own.at[k], bias.at[k], w_send.at[4, k - 1], w_recv.at[4, k - 1], others[k]) for k in range(1, TP)]
    own = [pltpu.make_async_copy(wq_own, wq.at[0], local.at[0]), pltpu.make_async_copy(wop_own, wop.at[0], local.at[1]), pltpu.make_async_copy(bias_own.at[0], bias.at[0], local.at[2]), pltpu.make_async_copy(patches.at[pl.ds(me * IMAGES, IMAGES)], xbuf.at[0], local.at[3])]
    flush = [pltpu.make_async_copy(wq, wq_out, local.at[4]), pltpu.make_async_copy(wop, wop_out, local.at[5]), pltpu.make_async_copy(bias, bias_out, local.at[6])]

    @pl.when(step == 0)
    def _():
        meet(others)
        small[0][0].start()
        small[1][0].start()
        for c in biases:
            c.start()
        small[0][1].start()
        small[1][1].start()
        for g in range(AHEAD):
            for c in group_sends(patches, xbuf, x_send, x_recv, others, g):
                c.start()
        for c in own:
            c.start()
        for n in range(2):
            small[n][0].wait_recv()
            small[n][2].start()
        for n in range(2):
            large[n][1].start()
        for c in own:
            c.wait()
        for n in range(2):
            small[n][1].wait_recv()
            small[n][2].wait_recv()
        for c in biases:
            c.wait_recv()
        for c in flush:
            c.start()

    @pl.when(step + AHEAD < STEPS)
    def _():
        for c in group_sends(patches, xbuf, x_send, x_recv, others, step + AHEAD):
            c.start()

    @pl.when(step == STEPS - AHEAD)
    def _():
        large[0][0].start()
        large[1][0].start()

    for c in group_sends(patches, xbuf, x_send, x_recv, others, step):
        c.wait_recv()
    x = slot_rows(xbuf, step)
    posb = jnp.concatenate([wop[k, 192:192 + PART] for k in range(TP)], axis=0).astype(WIDE) + vec[0:1]
    emb = dot_nn(x, wp[...]) + jnp.concatenate([posb] * GROUP, axis=0)
    e_h = emb.astype(HALF)
    for g in range(GROUP):
        x_ref[g] = x[TOK * g:TOK * g + TOK]
        e_ref[g] = e_h[TOK * g:TOK * g + TOK]
    e_f = e_h.astype(WIDE)
    xhat, _ = normalize(e_f)
    h1 = (xhat * vec[1:2] + vec[2:3]).astype(HALF)
    bqkv = bias[0].astype(WIDE) + bias[1].astype(WIDE) + bias[2].astype(WIDE) + bias[3].astype(WIDE)
    for s in range(3):
        part = (dot_nt(h1, jnp.concatenate([wq[k, s] for k in range(TP)], axis=0)) + bqkv[s:s + 1]).astype(HALF)
        for g in range(GROUP):
            qkv_ref[g, :, DIM * s:DIM * s + DIM] = part[TOK * g:TOK * g + TOK]
    for g in range(GROUP):
        for pr in range(PAIRS):
            q = qkv_ref[g, :, 128 * pr:128 * pr + 128]
            k = qkv_ref[g, :, DIM + 128 * pr:DIM + 128 * pr + 128]
            v = qkv_ref[g, :, 2 * DIM + 128 * pr:2 * DIM + 128 * pr + 128]
            probs = []
            for j in range(2):
                s = dot_nt(mask_half(q, j), k)
                m = jnp.max(s, axis=-1, keepdims=True)
                e = jnp.exp2((s - m) * EXP_SCALE)
                l = jnp.sum(e, axis=-1, keepdims=True)
                probs.append((e * (1.0 / l)).astype(HALF))
            pv = dot_nn(jnp.concatenate(probs, axis=1), jnp.concatenate([mask_half(v, 0), mask_half(v, 1)], axis=0))
            o_ref[g, :, 128 * pr:128 * pr + 128] = pv.astype(HALF)
    o = jnp.concatenate([o_ref[g] for g in range(GROUP)], axis=0)
    e_f = jnp.concatenate([e_ref[g] for g in range(GROUP)], axis=0).astype(WIDE)
    x1 = (e_f + (dot_nn(o, jnp.concatenate([wop[k, 0:192] for k in range(TP)], axis=0)) + vec[3:4])).astype(HALF)
    for g in range(GROUP):
        x1_ref[g] = x1[TOK * g:TOK * g + TOK]

    @pl.when(step == STEPS - 1)
    def _():
        for n in range(2):
            large[n][0].wait_recv()
            large[n][2].start()
        for n in range(2):
            large[n][1].wait_recv()
            large[n][2].wait_recv()
            for c in small[n] + large[n]:
                c.wait_send()
        for c in biases:
            c.wait_send()
        for c in flush:
            c.wait()
        for g in range(STEPS):
            for c in group_sends(patches, xbuf, x_send, x_recv, others, g):
                c.wait_send()


def fixed(shape):
    return pl.BlockSpec(shape, lambda i: (0,) * len(shape), pipeline_mode=pl.Buffered(1))


def image_spec(width):
    return pl.BlockSpec((GROUP, TOK, width), lambda i: (i, 0, 0))


def any_spec():
    return pl.BlockSpec(memory_space=pl.ANY)


def params(cid):
    return pltpu.CompilerParams(dimension_semantics=('arbitrary',), vmem_limit_bytes=67043328, collective_id=cid, has_side_effects=True)


def image_shape(width):
    return jax.ShapeDtypeStruct((IMAGES, TOK, width), HALF)


def half_shape(*shape):
    return jax.ShapeDtypeStruct(shape, HALF)


def wide_shape(*shape):
    return jax.ShapeDtypeStruct(shape, WIDE)


def attn_fwd(patches, wq, wop, bias, w1, w2, wp, vec):
    dma = pltpu.SemaphoreType.DMA
    return pl.pallas_call(
        attn_fwd_kernel,
        grid=(STEPS,),
        in_specs=[any_spec()] * 6 + [fixed((DIM, DIM)), fixed((8, DIM))],
        out_specs=[image_spec(DIM), image_spec(3 * DIM), image_spec(DIM), image_spec(DIM), image_spec(DIM)] + [any_spec()] * 5,
        out_shape=[image_shape(DIM), image_shape(3 * DIM), image_shape(DIM), image_shape(DIM), image_shape(DIM), half_shape(TP, 3, 192, DIM), half_shape(TP, 256, DIM), half_shape(TP, 16, DIM), half_shape(3, DIM, DIM), half_shape(3, DIM, DIM)],
        scratch_shapes=[pltpu.VMEM((TP, IMAGES, PART, DIM), HALF), pltpu.VMEM((TP, 3, 192, DIM), HALF), pltpu.VMEM((TP, 256, DIM), HALF), pltpu.VMEM((TP, 16, DIM), HALF), dma((3, STEPS)), dma((3, STEPS)), dma((5, 3)), dma((5, 3)), dma((7,))],
        compiler_params=params(0),
        cost_estimate=pl.CostEstimate(flops=60_000_000_000, bytes_accessed=50_000_000, transcendentals=12_000_000),
        name='attn_fwd',
    )(patches, wq, wop, bias, w1, w2, wp, vec)


def mlp_kernel(d_out, x1_ref, o_ref, w1_own, w1_rest, w2_own, w2_rest, wop, bias, vec, x2_out, dx1_ref, do_ref, keep_out, recv_out, dvec_ref, db1_ref, dbuf, ybuf, dw1, dw2, dwo, d_send, d_recv, y_send, y_recv, y_own, g_send, g_recv, local):
    step = pl.program_id(0)
    me, core, others = peers()
    slot = lax.rem(step, 2)

    def y_sends(at, group):
        return [push(ybuf.at[at, k], x2_out.at[image_rows(me, group)], y_send.at[k - 1, at], y_recv.at[k - 1, group], others[k]) for k in (2, 3, 1)]

    def y_keep(at, group):
        return pltpu.make_async_copy(ybuf.at[at, 0], x2_out.at[image_rows(me, group)], y_own.at[at])

    def y_wait(at, group):
        for c in y_sends(at, group):
            c.wait_send()
        y_keep(at, group).wait()

    own = pltpu.make_async_copy(d_out.at[pl.ds(me * IMAGES, IMAGES)], dbuf.at[0], local.at[6])
    grads = []
    for n in range(2):
        grads.append(push(dw1.at[2 * n + 1], recv_out.at[n, 0:DIM], g_send.at[n, 0], g_recv.at[n, 0], others[1]))
        grads.append(push(dw2.at[2 * n + 1], recv_out.at[n, DIM:2 * DIM], g_send.at[n, 1], g_recv.at[n, 1], others[1]))
        grads.append(push(dwo.at[192 * (2 * n + 1):192 * (2 * n + 2)], recv_out.at[n, 2 * DIM:PACK], g_send.at[n, 2], g_recv.at[n, 2], others[1]))
    keeps = []
    for n in range(2):
        keeps.append(pltpu.make_async_copy(dw1.at[2 * n], keep_out.at[n, 0:DIM], local.at[3 * n]))
        keeps.append(pltpu.make_async_copy(dw2.at[2 * n], keep_out.at[n, DIM:2 * DIM], local.at[3 * n + 1]))
        keeps.append(pltpu.make_async_copy(dwo.at[192 * (2 * n):192 * (2 * n + 1)], keep_out.at[n, 2 * DIM:PACK], local.at[3 * n + 2]))

    @pl.when(step == 0)
    def _():
        meet(others)
        for g in range(AHEAD):
            for c in group_sends(d_out, dbuf, d_send, d_recv, others, g):
                c.start()
        own.start()
        dw1[...] = jnp.zeros_like(dw1)
        dw2[...] = jnp.zeros_like(dw2)
        dwo[...] = jnp.zeros_like(dwo)
        dvec_ref[...] = jnp.zeros_like(dvec_ref)
        db1_ref[...] = jnp.zeros_like(db1_ref)
        own.wait()

    @pl.when(step + AHEAD < STEPS)
    def _():
        for c in group_sends(d_out, dbuf, d_send, d_recv, others, step + AHEAD):
            c.start()

    x1 = jnp.concatenate([x1_ref[g] for g in range(GROUP)], axis=0)
    xhat, inv = normalize(x1.astype(WIDE))
    h2 = (xhat * vec[0:1] + vec[1:2]).astype(HALF)
    for c in group_sends(d_out, dbuf, d_send, d_recv, others, step):
        c.wait_recv()
    dout = slot_rows(dbuf, step)
    y = None
    dh2 = None
    for f in range(TP):
        w1 = w1_own[...] if f == 0 else w1_rest[f - 1]
        w2 = w2_own[...] if f == 0 else w2_rest[f - 1]
        pre = dot_nn(h2, w1) + bias[f, 3:4].astype(WIDE)
        sq = pre * pre
        t = jnp.tanh(pre * (GELU_C + (GELU_C * GELU_A) * sq))
        half_pre = 0.5 * pre
        hid = (half_pre + half_pre * t).astype(HALF)
        slope = (0.5 + 0.5 * t) + (half_pre * (1.0 - t * t)) * (GELU_C + (3.0 * GELU_C * GELU_A) * sq)
        dhid = dot_nt(dout, w2).astype(HALF).astype(WIDE)
        dpre = dhid * slope
        db1_ref[f:f + 1] += col_sum(dpre)
        dpre_h = dpre.astype(HALF)
        part_y = dot_nn(hid, w2)
        part_h = dot_nt(dpre_h, w1)
        y = part_y if y is None else y + part_y
        dh2 = part_h if dh2 is None else dh2 + part_h
        dw1[f] += dot_tn(h2, dpre_h)
        dw2[f] += dot_tn(dout, hid)
    x2 = (x1.astype(WIDE) + (y + vec[2:3])).astype(HALF)

    @pl.when(step >= 2)
    def _():
        y_wait(slot, step - 2)

    for g in range(GROUP):
        for k in range(TP):
            ybuf[slot, k, g] = x2[TOK * g + PART * k:TOK * g + PART * k + PART]
    dh2 = dh2.astype(HALF).astype(WIDE)
    xhat, inv = normalize(x1.astype(WIDE))
    dout_f = dout.astype(WIDE)
    dx1 = (dout_f + norm_back(dh2, xhat, inv, vec[0:1])).astype(HALF)
    dvec_ref[0:1] += col_sum(dh2 * xhat)
    dvec_ref[1:2] += col_sum(dh2)
    dvec_ref[2:3] += col_sum(dout_f)
    dvec_ref[3:4] += col_sum(dx1.astype(WIDE))
    d_o = dot_nt(dx1, jnp.concatenate([wop[k, 0:192] for k in range(TP)], axis=0)).astype(HALF)
    for g in range(GROUP):
        dx1_ref[g] = dx1[TOK * g:TOK * g + TOK]
        do_ref[g] = d_o[TOK * g:TOK * g + TOK]
    o = jnp.concatenate([o_ref[g] for g in range(GROUP)], axis=0)
    dwo[...] += dot_tn(o, dx1)

    for c in y_sends(slot, step):
        c.start()
    y_keep(slot, step).start()

    @pl.when(step == STEPS - 1)
    def _():
        for c in grads + keeps:
            c.start()
        for c in keeps:
            c.wait()
        for c in grads:
            c.wait()
        for g in range(STEPS):
            for c in group_sends(d_out, dbuf, d_send, d_recv, others, g):
                c.wait_send()
            for c in y_sends(g % 2, g):
                c.wait_recv()
        for g in (STEPS - 2, STEPS - 1):
            y_wait(g % 2, g)


def mlp(d_out, x1, o, w1, w1_rest, w2, w2_rest, wop, bias, vec):
    dma = pltpu.SemaphoreType.DMA
    vec_spec = pl.BlockSpec((8, DIM), lambda i: (0, 0))
    return pl.pallas_call(
        mlp_kernel,
        grid=(STEPS,),
        in_specs=[any_spec(), image_spec(DIM), image_spec(DIM), fixed((DIM, DIM)), fixed((3, DIM, DIM)), fixed((DIM, DIM)), fixed((3, DIM, DIM)), fixed((TP, 256, DIM)), fixed((TP, 16, DIM)), fixed((8, DIM))],
        out_specs=[any_spec(), image_spec(DIM), image_spec(DIM), any_spec(), any_spec(), vec_spec, vec_spec],
        out_shape=[half_shape(TP * IMAGES, PART, DIM), image_shape(DIM), image_shape(DIM), wide_shape(2, PACK, DIM), wide_shape(2, PACK, DIM), wide_shape(8, DIM), wide_shape(8, DIM)],
        scratch_shapes=[pltpu.VMEM((TP, IMAGES, PART, DIM), HALF), pltpu.VMEM((2, TP, GROUP, PART, DIM), HALF), pltpu.VMEM((TP, DIM, DIM), WIDE), pltpu.VMEM((TP, DIM, DIM), WIDE), pltpu.VMEM((DIM, DIM), WIDE), dma((3, STEPS)), dma((3, STEPS)), dma((3, 2)), dma((3, STEPS)), dma((2,)), dma((2, 3)), dma((2, 3)), dma((7,))],
        compiler_params=params(1),
        cost_estimate=pl.CostEstimate(flops=130_000_000_000, bytes_accessed=80_000_000, transcendentals=12_000_000),
        name='mlp',
    )(d_out, x1, o, w1, w1_rest, w2, w2_rest, wop, bias, vec)


def attn_bwd_kernel(pair, e_ref, qkv_ref, do_ref, dx1_ref, x_ref, wq, vec, dvec2_ref, db1_ref, cross_out, dqkv_out, dwp_out, dpos_out, tiny_out, dqkv, dwq, dwp, dpos, tiny, near_q, near_p, near_pos, far_q, far_p, far_pos, half_q, half_p, half_pos, p_send, p_recv, t_send, t_recv, n_send, n_recv, f_send, f_recv, h_send, h_recv, local):
    step = pl.program_id(0)
    me, core, others = peers()
    cuts = (0, DIM, 2 * DIM, PACK)
    pairs = [push(pair.at[cuts[n]:cuts[n + 1]], cross_out.at[cuts[n]:cuts[n + 1]], p_send.at[n], p_recv.at[n], others[2]) for n in range(3)]

    @pl.when(step == 0)
    def _():
        meet(others)
        for c in pairs:
            c.start()
        dwq[...] = jnp.zeros_like(dwq)
        dwp[...] = jnp.zeros_like(dwp)
        dpos[...] = jnp.zeros_like(dpos)
        tiny[...] = jnp.zeros_like(tiny)

    for g in range(GROUP):
        rows = slice(TOK * g, TOK * g + TOK)
        for pr in range(PAIRS):
            cols = slice(128 * pr, 128 * pr + 128)
            q = qkv_ref[g, :, 128 * pr:128 * pr + 128]
            k = qkv_ref[g, :, DIM + 128 * pr:DIM + 128 * pr + 128]
            v = qkv_ref[g, :, 2 * DIM + 128 * pr:2 * DIM + 128 * pr + 128]
            d_o = do_ref[g, :, 128 * pr:128 * pr + 128]
            probs = []
            dscores = []
            for j in range(2):
                s = dot_nt(k, mask_half(q, j))
                m = jnp.max(s, axis=0, keepdims=True)
                e = jnp.exp2((s - m) * EXP_SCALE)
                l = jnp.sum(e, axis=0, keepdims=True)
                p = e * (1.0 / l)
                dp = dot_nt(v, mask_half(d_o, j)).astype(HALF).astype(WIDE)
                delta = jnp.sum(dp * p, axis=0, keepdims=True)
                ds = (p * ((dp - delta) * 0.125)).astype(HALF)
                probs.append(p.astype(HALF))
                dscores.append(ds)
            dv = dot_nn(jnp.concatenate(probs, axis=1), jnp.concatenate([mask_half(d_o, 0), mask_half(d_o, 1)], axis=0))
            dk = dot_nn(jnp.concatenate(dscores, axis=1), jnp.concatenate([mask_half(q, 0), mask_half(q, 1)], axis=0))
            dq = dot_tn(jnp.concatenate(dscores, axis=0), jnp.concatenate([mask_half(k, 0), mask_half(k, 1)], axis=0))
            dqkv[rows, 128 * pr:128 * pr + 128] = dq.astype(HALF)
            dqkv[rows, DIM + 128 * pr:DIM + 128 * pr + 128] = dk.astype(HALF)
            dqkv[rows, 2 * DIM + 128 * pr:2 * DIM + 128 * pr + 128] = dv.astype(HALF)
    e_f = jnp.concatenate([e_ref[g] for g in range(GROUP)], axis=0).astype(WIDE)
    xhat, inv = normalize(e_f)
    h1 = (xhat * vec[1:2] + vec[2:3]).astype(HALF)
    dh1 = None
    for s in range(3):
        part = dqkv[:, DIM * s:DIM * s + DIM]
        tiny[s:s + 1] += col_sum(part.astype(WIDE))
        grad = dot_tn(part, h1)
        for k in range(TP):
            dwq[k, s] += grad[192 * k:192 * k + 192]
        term = dot_nn(part, jnp.concatenate([wq[k, s] for k in range(TP)], axis=0))
        dh1 = term if dh1 is None else dh1 + term
    dh1 = dh1.astype(HALF).astype(WIDE)
    dx1 = jnp.concatenate([dx1_ref[g] for g in range(GROUP)], axis=0).astype(WIDE)
    de = (dx1 + norm_back(dh1, xhat, inv, vec[1:2])).astype(HALF)
    de_f = de.astype(WIDE)
    tiny[16:17] += col_sum(dh1 * xhat)
    tiny[17:18] += col_sum(dh1)
    acc = de_f[0:TOK]
    for g in range(1, GROUP):
        acc = acc + de_f[TOK * g:TOK * g + TOK]
    dpos[...] += acc
    x = jnp.concatenate([x_ref[g] for g in range(GROUP)], axis=0)
    dwp[...] += dot_tn(x, de)

    @pl.when(step == STEPS - 1)
    def _():
        tiny[8:16] = db1_ref[...]
        tiny[18:19] = col_sum(dpos[...])
        tiny[24:32] = dvec2_ref[...]
        other_half = pl.ds(384 * (1 - core), 384)
        my_half = pl.ds(384 * core, 384)
        near = [push(dwq.at[3], near_q.at[1], n_send.at[0], n_recv.at[0], others[1]), push(dwq.at[1], near_q.at[0], n_send.at[1], n_recv.at[1], others[1]), push(dpos.at[3 * PART:4 * PART], near_pos.at[1], n_send.at[2], n_recv.at[2], others[1]), push(dpos.at[PART:2 * PART], near_pos.at[0], n_send.at[3], n_recv.at[3], others[1]), push(dwp.at[other_half], near_p, n_send.at[4], n_recv.at[4], others[1])]
        tinies = [push(tiny, tiny_out.at[k - 1], t_send.at[k - 1], t_recv.at[k - 1], others[k]) for k in range(1, TP)]
        far = [push(dwq.at[2], far_q, f_send.at[0], f_recv.at[0], others[2]), push(dwp.at[my_half], far_p, f_send.at[1], f_recv.at[1], others[2]), push(dpos.at[2 * PART:3 * PART], far_pos, f_send.at[2], f_recv.at[2], others[2])]
        for c in near + tinies:
            c.start()
        near[0].wait_recv()
        for s in range(3):
            dwq[2, s] += near_q[1, s]
        far[0].start()
        near[4].wait_recv()
        dwp[my_half] += near_p[...]
        far[1].start()
        near[2].wait_recv()
        dpos[2 * PART:3 * PART] += near_pos[1]
        far[2].start()
        near[1].wait_recv()
        near[3].wait_recv()
        for c in pairs:
            c.wait()
        far[0].wait_recv()
        for s in range(3):
            half_q[s] = ((dwq[0, s] + near_q[0, s]) + far_q[s]).astype(HALF)
        q_copy = pltpu.make_async_copy(half_q, dqkv_out, local.at[0])
        q_copy.start()
        far[1].wait()
        half_p[...] = (dwp[my_half] + far_p[...]).astype(HALF)
        swap = push(half_p, dwp_out.at[my_half], h_send, h_recv, others[1])
        swap.start()
        p_copy = pltpu.make_async_copy(half_p, dwp_out.at[my_half], local.at[1])
        p_copy.start()
        far[2].wait_recv()
        half_pos[...] = ((dpos[0:PART] + near_pos[0]) + far_pos[...]).astype(HALF)
        pos_copy = pltpu.make_async_copy(half_pos, dpos_out, local.at[2])
        pos_copy.start()
        for c in near:
            c.wait_send()
        for c in tinies:
            c.wait()
        far[0].wait_send()
        far[2].wait_send()
        tiny_copy = pltpu.make_async_copy(tiny, tiny_out.at[3], local.at[3])
        tiny_copy.start()
        q_copy.wait()
        p_copy.wait()
        pos_copy.wait()
        tiny_copy.wait()
        swap.wait()


def attn_bwd(pair, e, qkv, d_o, dx1, x, wq, vec, dvec2, db1):
    dma = pltpu.SemaphoreType.DMA
    return pl.pallas_call(
        attn_bwd_kernel,
        grid=(STEPS,),
        in_specs=[any_spec(), image_spec(DIM), image_spec(3 * DIM), image_spec(DIM), image_spec(DIM), image_spec(DIM), fixed((TP, 3, 192, DIM)), fixed((8, DIM)), fixed((8, DIM)), fixed((8, DIM))],
        out_specs=[any_spec()] * 5,
        out_shape=[wide_shape(PACK, DIM), half_shape(3, 192, DIM), half_shape(DIM, DIM), half_shape(PART, DIM), wide_shape(TP, 32, DIM)],
        scratch_shapes=[pltpu.VMEM((ROWS, 3 * DIM), HALF), pltpu.VMEM((TP, 3, 192, DIM), WIDE), pltpu.VMEM((DIM, DIM), WIDE), pltpu.VMEM((TOK, DIM), WIDE), pltpu.VMEM((32, DIM), WIDE), pltpu.VMEM((2, 3, 192, DIM), WIDE), pltpu.VMEM((384, DIM), WIDE), pltpu.VMEM((2, PART, DIM), WIDE), pltpu.VMEM((3, 192, DIM), WIDE), pltpu.VMEM((384, DIM), WIDE), pltpu.VMEM((PART, DIM), WIDE), pltpu.VMEM((3, 192, DIM), HALF), pltpu.VMEM((384, DIM), HALF), pltpu.VMEM((PART, DIM), HALF), dma((3,)), dma((3,)), dma((3,)), dma((3,)), dma((5,)), dma((5,)), dma((3,)), dma((3,)), dma, dma, dma((4,))],
        compiler_params=params(2),
        cost_estimate=pl.CostEstimate(flops=100_000_000_000, bytes_accessed=80_000_000, transcendentals=12_000_000),
        name='attn_bwd',
    )(pair, e, qkv, d_o, dx1, x, wq, vec, dvec2, db1)


def pad_rows(rows):
    rows = [r.astype(WIDE).reshape(-1, DIM) for r in rows]
    n = sum(r.shape[0] for r in rows)
    return jnp.concatenate(rows + [jnp.zeros((8 - n, DIM), WIDE)], axis=0)


def group_step(patches, patch_w, patch_b, pos_emb, ln_scale, ln_bias, qkv_w, qkv_b, out_w, out_b, fc1_w, fc1_b, fc2_w, fc2_b, d_out):
    wq = qkv_w.transpose(0, 2, 3, 1).reshape(3, 192, DIM)
    wop = jnp.concatenate([out_w.reshape(192, DIM), pos_emb], axis=0)
    qb = qkv_b.reshape(3, 192)
    bias = jnp.stack([jnp.concatenate([jnp.pad(qb, ((0, 0), (192 * k, DIM - 192 - 192 * k))), fc1_b.reshape(1, DIM), jnp.zeros((12, DIM), HALF)], axis=0) for k in range(TP)])
    vec1 = pad_rows([patch_b, ln_scale[0], ln_bias[0], out_b])
    vec2 = pad_rows([ln_scale[1], ln_bias[1], fc2_b])
    e, qkv, o, x1, x, wq_all, wop_all, bias_all, w1_rest, w2_rest = attn_fwd(patches, wq, wop, bias, fc1_w, fc2_w, patch_w, vec1)
    x_two, dx1, d_o, keep, near, dvec2, db1 = mlp(d_out, x1, o, fc1_w, w1_rest, fc2_w, w2_rest, wop_all, bias_all, vec2)
    pair = keep[1] + near[1]
    cross, d_qkv, d_patch_w, d_pos, tiny = attn_bwd(pair, e, qkv, d_o, dx1, x, wq_all, vec1, dvec2, db1)
    total = ((keep[0] + near[0]) + cross).astype(HALF)
    d_fc1_w = total[0:DIM]
    d_fc2_w = total[DIM:2 * DIM].T
    d_out_w = total[2 * DIM:].reshape(3, 64, DIM)
    d_qkv_w = d_qkv.reshape(3, 3, 64, DIM).transpose(0, 3, 1, 2)
    vec = ((tiny[3] + tiny[0]) + (tiny[1] + tiny[2])).astype(HALF)
    d_qkv_b = (tiny[3, 0:3, 0:192] + tiny[0, 0:3, 192:384]) + (tiny[1, 0:3, 384:576] + tiny[2, 0:3, 576:768])
    d_fc1_b = (tiny[3, 8] + tiny[0, 9]) + (tiny[1, 10] + tiny[2, 11])
    d_ln_scale = jnp.stack([vec[16], vec[24]])
    d_ln_bias = jnp.stack([vec[17], vec[25]])
    return (x_two, d_patch_w, vec[18], d_pos, d_ln_scale, d_ln_bias, d_qkv_w, d_qkv_b.astype(HALF).reshape(3, 3, 64), d_out_w, vec[27], d_fc1_w, d_fc1_b.astype(HALF), d_fc2_w, vec[26])


def solution(mesh):
    in_specs = (P('dp', 'tp', None), P(), P(), P('tp', None), P(), P(), P(None, None, 'tp', None), P(None, 'tp', None), P('tp', None, None), P(), P(None, 'tp'), P('tp'), P('tp', None), P(), P('dp', 'tp', None))
    out_specs = (P('dp', 'tp', None), P('dp', None), P('dp'), P(('dp', 'tp'), None), P('dp', None), P('dp', None), P('dp', None, 'tp', None), P('dp', 'tp', None), P(('dp', 'tp'), None, None), P('dp'), P('dp', 'tp'), P(('dp', 'tp')), P(('dp', 'tp'), None), P('dp'))
    return jax.shard_map(group_step, mesh=mesh, in_specs=in_specs, out_specs=out_specs, check_vma=False)
```

```python
import functools
import jax
import jax.numpy as jnp
from jax import lax
from jax.experimental import pallas as pl
from jax.experimental.pallas import tpu as pltpu
from jax.sharding import PartitionSpec as P

LN_EPS = 1e-6
TP = 4
WIDE = jnp.float32
HALF = jnp.bfloat16
IMAGES = 16
TOK = 256
PART = 64
DIM = 768
GROUP = 2
ROWS = GROUP * TOK
STEPS = IMAGES // GROUP
PAIRS = 6
EXP_SCALE = 0.125 * 1.4426950408889634
GELU_C = 0.7978845608028654
GELU_A = 0.044715
AHEAD = 3
PACK = 2 * DIM + 192
CHUNKS = 6
CHUNK = PACK // CHUNKS


def dot_nn(a, b):
    return lax.dot_general(a, b, (((1,), (0,)), ((), ())), preferred_element_type=WIDE)


def dot_nt(a, b):
    return lax.dot_general(a, b, (((1,), (1,)), ((), ())), preferred_element_type=WIDE)


def dot_tn(a, b):
    return lax.dot_general(a, b, (((0,), (0,)), ((), ())), preferred_element_type=WIDE)


def normalize(x_f):
    mean = jnp.sum(x_f, axis=-1, keepdims=True) * (1.0 / DIM)
    centered = x_f - mean
    var = jnp.sum(centered * centered, axis=-1, keepdims=True) * (1.0 / DIM)
    inv = lax.rsqrt(var + LN_EPS)
    return centered * inv, inv


def norm_back(d_out_f, xhat, inv, scale):
    d_hat = d_out_f * scale
    m1 = jnp.sum(d_hat, axis=-1, keepdims=True) * (1.0 / DIM)
    m2 = jnp.sum(d_hat * xhat, axis=-1, keepdims=True) * (1.0 / DIM)
    return (d_hat - m1 - xhat * m2) * inv


def lane_half(j):
    lane = lax.broadcasted_iota(jnp.int32, (1, 128), 1)
    return (lane < 64) if j == 0 else (lane >= 64)


def mask_half(x, j):
    return jnp.where(lane_half(j), x, jnp.zeros_like(x))


def col_sum(x):
    return jnp.sum(x, axis=0, keepdims=True)


def row(ref):
    return ref[...].reshape(1, DIM).astype(WIDE)


def peers():
    me = lax.axis_index('tp')
    core = lax.rem(me, 2)
    chip = lax.div(me, 2)
    return me, core, (me, me + 1 - 2 * core, me + 2 - 4 * chip, 3 - me)


def meet(others):
    barrier = pltpu.get_barrier_semaphore()
    for k in range(1, TP):
        pl.semaphore_signal(barrier, inc=1, device_id={'tp': others[k]}, device_id_type=pl.DeviceIdType.MESH)
    pl.semaphore_wait(barrier, TP - 1)


def push(src, dst, send, recv, peer):
    return pltpu.make_async_remote_copy(src_ref=src, dst_ref=dst, send_sem=send, recv_sem=recv, device_id={'tp': peer}, device_id_type=pl.DeviceIdType.MESH)


def image_rows(owner, group):
    return pl.ds(owner * IMAGES + group * GROUP, GROUP)


def group_sends(src, buf, send, recv, others, group):
    return [push(src.at[image_rows(others[k], group)], buf.at[k, pl.ds(group * GROUP, GROUP)], send.at[k - 1, group], recv.at[k - 1, group], others[k]) for k in (2, 3, 1)]


def slot_rows(buf, group):
    base = group * GROUP
    return jnp.concatenate([buf[k, base + g] for g in range(GROUP) for k in range(TP)], axis=0)


def attn_fwd_kernel(patches, wq_own, wo_own, pos_own, w1_own, w2_own, wp, patch_b, qkv_b, fc1_b, out_b, ln_scale, ln_bias, e_ref, qkv_ref, o_ref, x1_ref, x_ref, wq_out, wop_out, bias_out, w1_out, w2_near, xbuf, wq, wop, bias, bias_own, bqkv, x_send, x_recv, w_send, w_recv, local):
    step = pl.program_id(0)
    me, core, others = peers()
    small = []
    for n, (src, cut) in enumerate(((wq_own, None), (wo_own, (0, 192)), (pos_own, (192, 256)))):
        at = [wq.at[k] if cut is None else wop.at[k, cut[0]:cut[1]] for k in range(TP)]
        small.append((push(src, at[2], w_send.at[n, 1], w_recv.at[n, 1], others[2]), push(src, at[1], w_send.at[n, 0], w_recv.at[n, 0], others[1]), push(at[2], at[3], w_send.at[n, 2], w_recv.at[n, 2], others[1])))
    large = (push(w1_own, w1_out.at[1], w_send.at[3, 1], w_recv.at[3, 1], others[2]), push(w1_own, w1_out.at[0], w_send.at[3, 0], w_recv.at[3, 0], others[1]), push(w1_out.at[1], w1_out.at[2], w_send.at[3, 2], w_recv.at[3, 2], others[1]), push(w2_own, w2_near, w_send.at[4, 0], w_recv.at[4, 0], others[1]))
    biases = [push(bias_own, bias.at[k], w_send.at[5, k - 1], w_recv.at[5, k - 1], others[k]) for k in range(1, TP)]
    own = [pltpu.make_async_copy(wq_own, wq.at[0], local.at[0]), pltpu.make_async_copy(wo_own, wop.at[0, 0:192], local.at[1]), pltpu.make_async_copy(pos_own, wop.at[0, 192:256], local.at[2]), pltpu.make_async_copy(patches.at[pl.ds(me * IMAGES, IMAGES)], xbuf.at[0], local.at[3])]
    flush = [pltpu.make_async_copy(wq, wq_out, local.at[4]), pltpu.make_async_copy(wop, wop_out, local.at[5]), pltpu.make_async_copy(bias, bias_out, local.at[6])]

    @pl.when(step == 0)
    def _():
        bias_own[...] = jnp.zeros_like(bias_own)
        for s in range(3):
            for h in range(3):
                bias_own[s:s + 1, 64 * h:64 * h + 64] = qkv_b[s, h:h + 1]
        bias_own[3:4] = fc1_b[...].reshape(1, DIM)
        bias[0] = bias_own[...]
        meet(others)
        for n in range(3):
            small[n][0].start()
        for c in biases:
            c.start()
        for n in range(3):
            small[n][1].start()
        for g in range(AHEAD):
            for c in group_sends(patches, xbuf, x_send, x_recv, others, g):
                c.start()
        for c in own:
            c.start()
        for n in range(3):
            small[n][0].wait_recv()
            small[n][2].start()
        large[1].start()
        large[3].start()
        for c in own:
            c.wait()
        for n in range(3):
            small[n][1].wait_recv()
            small[n][2].wait_recv()
        for c in biases:
            c.wait_recv()
        for s in range(3):
            for k in range(TP):
                bqkv[s:s + 1, 192 * k:192 * k + 192] = bias[k, s:s + 1, 0:192].astype(WIDE)
        for c in flush:
            c.start()

    @pl.when(step + AHEAD < STEPS)
    def _():
        for c in group_sends(patches, xbuf, x_send, x_recv, others, step + AHEAD):
            c.start()

    @pl.when(step == STEPS - AHEAD)
    def _():
        large[0].start()

    for c in group_sends(patches, xbuf, x_send, x_recv, others, step):
        c.wait_recv()
    x = slot_rows(xbuf, step)
    posb = jnp.concatenate([wop[k, 192:192 + PART] for k in range(TP)], axis=0).astype(WIDE) + row(patch_b)
    emb = dot_nn(x, wp[...]) + jnp.concatenate([posb] * GROUP, axis=0)
    e_h = emb.astype(HALF)
    for g in range(GROUP):
        x_ref[g] = x[TOK * g:TOK * g + TOK]
        e_ref[g] = e_h[TOK * g:TOK * g + TOK]
    e_f = e_h.astype(WIDE)
    xhat, _ = normalize(e_f)
    h1 = (xhat * ln_scale[0:1].astype(WIDE) + ln_bias[0:1].astype(WIDE)).astype(HALF)
    for s in range(3):
        part = (dot_nt(h1, jnp.concatenate([wq[k, s] for k in range(TP)], axis=0)) + bqkv[s:s + 1]).astype(HALF)
        for g in range(GROUP):
            qkv_ref[g, :, DIM * s:DIM * s + DIM] = part[TOK * g:TOK * g + TOK]
    for g in range(GROUP):
        for pr in range(PAIRS):
            q = qkv_ref[g, :, 128 * pr:128 * pr + 128]
            k = qkv_ref[g, :, DIM + 128 * pr:DIM + 128 * pr + 128]
            v = qkv_ref[g, :, 2 * DIM + 128 * pr:2 * DIM + 128 * pr + 128]
            probs = []
            for j in range(2):
                s = dot_nt(mask_half(q, j), k)
                m = jnp.max(s, axis=-1, keepdims=True)
                e = jnp.exp2((s - m) * EXP_SCALE)
                l = jnp.sum(e, axis=-1, keepdims=True)
                probs.append((e * (1.0 / l)).astype(HALF))
            pv = dot_nn(jnp.concatenate(probs, axis=1), jnp.concatenate([mask_half(v, 0), mask_half(v, 1)], axis=0))
            o_ref[g, :, 128 * pr:128 * pr + 128] = pv.astype(HALF)
    o = jnp.concatenate([o_ref[g] for g in range(GROUP)], axis=0)
    e_f = jnp.concatenate([e_ref[g] for g in range(GROUP)], axis=0).astype(WIDE)
    x1 = (e_f + (dot_nn(o, jnp.concatenate([wop[k, 0:192] for k in range(TP)], axis=0)) + row(out_b))).astype(HALF)
    for g in range(GROUP):
        x1_ref[g] = x1[TOK * g:TOK * g + TOK]

    @pl.when(step == STEPS - 1)
    def _():
        large[0].wait_recv()
        large[2].start()
        for c in large[1:]:
            c.wait_recv()
        for c in small[0] + small[1] + small[2] + large:
            c.wait_send()
        for c in biases:
            c.wait_send()
        for c in flush:
            c.wait()
        for g in range(STEPS):
            for c in group_sends(patches, xbuf, x_send, x_recv, others, g):
                c.wait_send()


def fixed(shape):
    return pl.BlockSpec(shape, lambda i: (0,) * len(shape), pipeline_mode=pl.Buffered(1))


def image_spec(width):
    return pl.BlockSpec((GROUP, TOK, width), lambda i: (i, 0, 0))


def any_spec():
    return pl.BlockSpec(memory_space=pl.ANY)


def params(cid):
    return pltpu.CompilerParams(dimension_semantics=('arbitrary',), vmem_limit_bytes=67043328, collective_id=cid, has_side_effects=True)


def image_shape(width):
    return jax.ShapeDtypeStruct((IMAGES, TOK, width), HALF)


def half_shape(*shape):
    return jax.ShapeDtypeStruct(shape, HALF)


def wide_shape(*shape):
    return jax.ShapeDtypeStruct(shape, WIDE)


def vec_spec(*shape):
    return pl.BlockSpec(shape, lambda i: (0,) * len(shape))


def attn_fwd(patches, wq, wo, pos, w1, w2, wp, patch_b, qkv_b, fc1_b, out_b, ln_scale, ln_bias):
    dma = pltpu.SemaphoreType.DMA
    return pl.pallas_call(
        attn_fwd_kernel,
        grid=(STEPS,),
        in_specs=[any_spec()] * 6 + [fixed((DIM, DIM)), vec_spec(DIM), vec_spec(3, 3, 64), vec_spec(DIM), vec_spec(DIM), vec_spec(2, DIM), vec_spec(2, DIM)],
        out_specs=[image_spec(DIM), image_spec(3 * DIM), image_spec(DIM), image_spec(DIM), image_spec(DIM)] + [any_spec()] * 5,
        out_shape=[image_shape(DIM), image_shape(3 * DIM), image_shape(DIM), image_shape(DIM), image_shape(DIM), half_shape(TP, 3, 192, DIM), half_shape(TP, 256, DIM), half_shape(TP, 16, DIM), half_shape(3, DIM, DIM), half_shape(DIM, DIM)],
        scratch_shapes=[pltpu.VMEM((TP, IMAGES, PART, DIM), HALF), pltpu.VMEM((TP, 3, 192, DIM), HALF), pltpu.VMEM((TP, 256, DIM), HALF), pltpu.VMEM((TP, 16, DIM), HALF), pltpu.VMEM((16, DIM), HALF), pltpu.VMEM((8, DIM), WIDE), dma((3, STEPS)), dma((3, STEPS)), dma((6, 3)), dma((6, 3)), dma((7,))],
        compiler_params=params(0),
        cost_estimate=pl.CostEstimate(flops=60_000_000_000, bytes_accessed=50_000_000, transcendentals=12_000_000),
        name='attn_fwd',
    )(patches, wq, wo, pos, w1, w2, wp, patch_b, qkv_b, fc1_b, out_b, ln_scale, ln_bias)


def mlp_slot(n, f, h2, dout, w1, w2, b1, y, dh2, dw1, dw2, db1_ref):
    pre = dot_nn(h2, w1) + b1
    sq = pre * pre
    t = jnp.tanh(pre * (GELU_C + (GELU_C * GELU_A) * sq))
    half_pre = 0.5 * pre
    hid = (half_pre + half_pre * t).astype(HALF)
    slope = (0.5 + 0.5 * t) + (half_pre * (1.0 - t * t)) * (GELU_C + (3.0 * GELU_C * GELU_A) * sq)
    dhid = dot_nt(dout, w2).astype(HALF).astype(WIDE)
    dpre = dhid * slope
    db1_ref[f:f + 1] += col_sum(dpre)
    dpre_h = dpre.astype(HALF)
    part_y = dot_nn(hid, w2)
    part_h = dot_nt(dpre_h, w1)
    y = part_y if y is None else y + part_y
    dh2 = part_h if dh2 is None else dh2 + part_h
    dw1[n] += dot_tn(h2, dpre_h)
    dw2[n] += dot_tn(dout, hid)
    return y, dh2


def mlp_near_kernel(d_out, w2_push, x1_ref, w1_own, w1_near, w2_own, w2_near, bias, ln_scale, ln_bias, dout_ref, y_ref, dh_ref, w2_far, keep_out, give_out, dvec_ref, db1_ref, dbuf, dw1, dw2, d_send, d_recv, w_send, w_recv, local):
    step = pl.program_id(0)
    me, core, others = peers()
    own = pltpu.make_async_copy(d_out.at[pl.ds(me * IMAGES, IMAGES)], dbuf.at[0], local.at[4])
    far = push(w2_push, w2_far.at[0], w_send.at[0], w_recv.at[0], others[2])
    relay = push(w2_far.at[0], w2_far.at[1], w_send.at[1], w_recv.at[1], others[1])

    @pl.when(step == 0)
    def _():
        meet(others)
        for g in range(AHEAD):
            for c in group_sends(d_out, dbuf, d_send, d_recv, others, g):
                c.start()
        own.start()
        dw1[...] = jnp.zeros_like(dw1)
        dw2[...] = jnp.zeros_like(dw2)
        dvec_ref[...] = jnp.zeros_like(dvec_ref)
        db1_ref[...] = jnp.zeros_like(db1_ref)
        own.wait()

    @pl.when(step + AHEAD < STEPS)
    def _():
        for c in group_sends(d_out, dbuf, d_send, d_recv, others, step + AHEAD):
            c.start()

    @pl.when(step == STEPS - AHEAD)
    def _():
        far.start()

    x1 = jnp.concatenate([x1_ref[g] for g in range(GROUP)], axis=0)
    xhat, inv = normalize(x1.astype(WIDE))
    h2 = (xhat * ln_scale[1:2].astype(WIDE) + ln_bias[1:2].astype(WIDE)).astype(HALF)
    for c in group_sends(d_out, dbuf, d_send, d_recv, others, step):
        c.wait_recv()
    dout = slot_rows(dbuf, step)
    dvec_ref[2:3] += col_sum(dout.astype(WIDE))
    y = None
    dh2 = None
    for f, (w1, w2) in enumerate(((w1_own, w2_own), (w1_near, w2_near))):
        y, dh2 = mlp_slot(f, f, h2, dout, w1[...], w2[...], bias[f, 3:4].astype(WIDE), y, dh2, dw1, dw2, db1_ref)
    for g in range(GROUP):
        rows = slice(TOK * g, TOK * g + TOK)
        dout_ref[g] = dout[rows]
        y_ref[g] = y[rows]
        dh_ref[g] = dh2[rows]

    @pl.when(step == STEPS - 1)
    def _():
        copies = []
        for n, out in enumerate((keep_out, give_out)):
            copies.append(pltpu.make_async_copy(dw1.at[n], out.at[0:DIM], local.at[2 * n]))
            copies.append(pltpu.make_async_copy(dw2.at[n], out.at[DIM:2 * DIM], local.at[2 * n + 1]))
        for c in copies:
            c.start()
        far.wait_recv()
        relay.start()
        for g in range(STEPS):
            for c in group_sends(d_out, dbuf, d_send, d_recv, others, g):
                c.wait_send()
        for c in copies:
            c.wait()
        far.wait_send()
        relay.wait()


def mlp_near(d_out, x1, w1, w1_near, w2, w2_near, bias, ln_scale, ln_bias):
    dma = pltpu.SemaphoreType.DMA
    wide_image = jax.ShapeDtypeStruct((IMAGES, TOK, DIM), WIDE)
    return pl.pallas_call(
        mlp_near_kernel,
        grid=(STEPS,),
        in_specs=[any_spec(), any_spec(), image_spec(DIM), fixed((DIM, DIM)), pl.BlockSpec((None, DIM, DIM), lambda i: (0, 0, 0), pipeline_mode=pl.Buffered(1)), fixed((DIM, DIM)), fixed((DIM, DIM)), fixed((TP, 16, DIM)), vec_spec(2, DIM), vec_spec(2, DIM)],
        out_specs=[image_spec(DIM)] * 3 + [any_spec()] * 3 + [vec_spec(8, DIM), vec_spec(8, DIM)],
        out_shape=[image_shape(DIM), wide_image, wide_image, half_shape(2, DIM, DIM), wide_shape(2 * DIM, DIM), wide_shape(2 * DIM, DIM), wide_shape(8, DIM), wide_shape(8, DIM)],
        scratch_shapes=[pltpu.VMEM((TP, IMAGES, PART, DIM), HALF), pltpu.VMEM((2, DIM, DIM), WIDE), pltpu.VMEM((2, DIM, DIM), WIDE), dma((3, STEPS)), dma((3, STEPS)), dma((2,)), dma((2,)), dma((5,))],
        compiler_params=params(1),
        cost_estimate=pl.CostEstimate(flops=60_000_000_000, bytes_accessed=80_000_000, transcendentals=6_000_000),
        name='mlp_near',
    )(d_out, w2, x1, w1, w1_near, w2, w2_near, bias, ln_scale, ln_bias)


def mlp_far_kernel(give, x1_ref, o_ref, dout_ref, y_ref, dh_ref, w1_rest, w2_far, wop, bias, ln_scale, ln_bias, fc2_b, dvec_near, db1_near, x2_out, dx1_ref, do_ref, near_a, keep_o, near_o, keep_b, near_b, dvec_ref, db1_ref, ybuf, dw1, dw2, dwo, y_send, y_recv, y_own, g_send, g_recv, local):
    step = pl.program_id(0)
    me, core, others = peers()
    slot = lax.rem(step, 2)

    def y_sends(at, group):
        return [push(ybuf.at[at, k], x2_out.at[image_rows(me, group)], y_send.at[k - 1, at], y_recv.at[k - 1, group], others[k]) for k in (2, 3, 1)]

    def y_keep(at, group):
        return pltpu.make_async_copy(ybuf.at[at, 0], x2_out.at[image_rows(me, group)], y_own.at[at])

    def y_wait(at, group):
        for c in y_sends(at, group):
            c.wait_send()
        y_keep(at, group).wait()

    early = push(give, near_a, g_send.at[0], g_recv.at[0], others[1])
    grads = [push(dw1.at[1], near_b.at[0:DIM], g_send.at[1], g_recv.at[1], others[1]), push(dw2.at[1], near_b.at[DIM:2 * DIM], g_send.at[2], g_recv.at[2], others[1]), push(dwo.at[576:768], near_b.at[2 * DIM:PACK], g_send.at[3], g_recv.at[3], others[1]), push(dwo.at[192:384], near_o, g_send.at[4], g_recv.at[4], others[1])]
    keeps = [pltpu.make_async_copy(dw1.at[0], keep_b.at[0:DIM], local.at[0]), pltpu.make_async_copy(dw2.at[0], keep_b.at[DIM:2 * DIM], local.at[1]), pltpu.make_async_copy(dwo.at[384:576], keep_b.at[2 * DIM:PACK], local.at[2]), pltpu.make_async_copy(dwo.at[0:192], keep_o, local.at[3])]

    @pl.when(step == 0)
    def _():
        meet(others)
        early.start()
        dw1[...] = jnp.zeros_like(dw1)
        dw2[...] = jnp.zeros_like(dw2)
        dwo[...] = jnp.zeros_like(dwo)
        dvec_ref[...] = dvec_near[...]
        db1_ref[...] = db1_near[...]

    x1 = jnp.concatenate([x1_ref[g] for g in range(GROUP)], axis=0)
    dout = jnp.concatenate([dout_ref[g] for g in range(GROUP)], axis=0)
    xhat, inv = normalize(x1.astype(WIDE))
    h2 = (xhat * ln_scale[1:2].astype(WIDE) + ln_bias[1:2].astype(WIDE)).astype(HALF)
    y = jnp.concatenate([y_ref[g] for g in range(GROUP)], axis=0)
    dh2 = jnp.concatenate([dh_ref[g] for g in range(GROUP)], axis=0)
    for f in range(2):
        y, dh2 = mlp_slot(f, f + 2, h2, dout, w1_rest[f + 1], w2_far[f], bias[f + 2, 3:4].astype(WIDE), y, dh2, dw1, dw2, db1_ref)
    x2 = (x1.astype(WIDE) + (y + row(fc2_b))).astype(HALF)

    @pl.when(step >= 2)
    def _():
        y_wait(slot, step - 2)

    for g in range(GROUP):
        for k in range(TP):
            ybuf[slot, k, g] = x2[TOK * g + PART * k:TOK * g + PART * k + PART]
    dh2 = dh2.astype(HALF).astype(WIDE)
    xhat, inv = normalize(x1.astype(WIDE))
    dout_f = dout.astype(WIDE)
    dx1 = (dout_f + norm_back(dh2, xhat, inv, ln_scale[1:2].astype(WIDE))).astype(HALF)
    dvec_ref[0:1] += col_sum(dh2 * xhat)
    dvec_ref[1:2] += col_sum(dh2)
    dvec_ref[3:4] += col_sum(dx1.astype(WIDE))
    d_o = dot_nt(dx1, jnp.concatenate([wop[k, 0:192] for k in range(TP)], axis=0)).astype(HALF)
    for g in range(GROUP):
        dx1_ref[g] = dx1[TOK * g:TOK * g + TOK]
        do_ref[g] = d_o[TOK * g:TOK * g + TOK]
    o = jnp.concatenate([o_ref[g] for g in range(GROUP)], axis=0)
    dwo[...] += dot_tn(o, dx1)

    for c in y_sends(slot, step):
        c.start()
    y_keep(slot, step).start()

    @pl.when(step == STEPS - 1)
    def _():
        for c in grads + keeps:
            c.start()
        for c in keeps:
            c.wait()
        early.wait()
        for c in grads:
            c.wait()
        for g in range(STEPS):
            for c in y_sends(g % 2, g):
                c.wait_recv()
        for g in (STEPS - 2, STEPS - 1):
            y_wait(g % 2, g)


def mlp_far(give, x1, o, dout, y, dh, w1_rest, w2_far, wop, bias, ln_scale, ln_bias, fc2_b, dvec_near, db1_near):
    dma = pltpu.SemaphoreType.DMA
    return pl.pallas_call(
        mlp_far_kernel,
        grid=(STEPS,),
        in_specs=[any_spec()] + [image_spec(DIM)] * 5 + [fixed((3, DIM, DIM)), fixed((2, DIM, DIM)), fixed((TP, 256, DIM)), fixed((TP, 16, DIM)), vec_spec(2, DIM), vec_spec(2, DIM), vec_spec(DIM), vec_spec(8, DIM), vec_spec(8, DIM)],
        out_specs=[any_spec(), image_spec(DIM), image_spec(DIM)] + [any_spec()] * 5 + [vec_spec(8, DIM), vec_spec(8, DIM)],
        out_shape=[half_shape(TP * IMAGES, PART, DIM), image_shape(DIM), image_shape(DIM), wide_shape(2 * DIM, DIM), wide_shape(192, DIM), wide_shape(192, DIM), wide_shape(PACK, DIM), wide_shape(PACK, DIM), wide_shape(8, DIM), wide_shape(8, DIM)],
        scratch_shapes=[pltpu.VMEM((2, TP, GROUP, PART, DIM), HALF), pltpu.VMEM((2, DIM, DIM), WIDE), pltpu.VMEM((2, DIM, DIM), WIDE), pltpu.VMEM((DIM, DIM), WIDE), dma((3, 2)), dma((3, STEPS)), dma((2,)), dma((5,)), dma((5,)), dma((4,))],
        compiler_params=params(2),
        cost_estimate=pl.CostEstimate(flops=70_000_000_000, bytes_accessed=80_000_000, transcendentals=6_000_000),
        name='mlp_far',
    )(give, x1, o, dout, y, dh, w1_rest, w2_far, wop, bias, ln_scale, ln_bias, fc2_b, dvec_near, db1_near)


def attn_bwd_kernel(keep_b, near_b, keep_a, near_a, keep_o, near_o, e_ref, qkv_ref, do_ref, dx1_ref, x_ref, wq, ln_scale, ln_bias, dvec2_ref, db1_ref, cross_out, dfc1_out, dfc2_out, dwo_out, dqkv_out, dwp_out, dpos_out, tiny_out, fetch_k, fetch_n, sums, dqkv, dwq, dwp, dpos, tiny, near_q, near_p, near_pos, far_q, far_p, far_pos, half_q, half_p, half_pos, p_send, p_recv, t_send, t_recv, n_send, n_recv, f_send, f_recv, h_send, h_recv, c_sem, o_sem, total1, total2, total3, local):
    step = pl.program_id(0)
    me, core, others = peers()
    pairs = [push(sums.at[n], cross_out.at[CHUNK * n:CHUNK * n + CHUNK], p_send.at[n], p_recv.at[n], others[2]) for n in range(CHUNKS)]

    def fetch(n):
        rows = pl.ds(n * CHUNK, CHUNK)
        at = lax.rem(n, 2)
        return (pltpu.make_async_copy(keep_b.at[rows], fetch_k.at[at], c_sem.at[0, at]), pltpu.make_async_copy(near_b.at[rows], fetch_n.at[at], c_sem.at[1, at]))

    @pl.when(step == 0)
    def _():
        meet(others)
        for c in fetch(0):
            c.start()

    @pl.when(step < CHUNKS)
    def _():
        @pl.when(step + 1 < CHUNKS)
        def _():
            for c in fetch(step + 1):
                c.start()
        for c in fetch(step):
            c.wait()
        at = lax.rem(step, 2)
        sums[step] = fetch_k[at] + fetch_n[at]

    @pl.when(step == 0)
    def _():
        dwq[...] = jnp.zeros_like(dwq)
        dwp[...] = jnp.zeros_like(dwp)
        dpos[...] = jnp.zeros_like(dpos)
        tiny[...] = jnp.zeros_like(tiny)

    @pl.when(step < CHUNKS)
    def _():
        push(sums.at[step], cross_out.at[pl.ds(step * CHUNK, CHUNK)], p_send.at[step], p_recv.at[step], others[2]).start()

    for g in range(GROUP):
        rows = slice(TOK * g, TOK * g + TOK)
        for pr in range(PAIRS):
            cols = slice(128 * pr, 128 * pr + 128)
            q = qkv_ref[g, :, 128 * pr:128 * pr + 128]
            k = qkv_ref[g, :, DIM + 128 * pr:DIM + 128 * pr + 128]
            v = qkv_ref[g, :, 2 * DIM + 128 * pr:2 * DIM + 128 * pr + 128]
            d_o = do_ref[g, :, 128 * pr:128 * pr + 128]
            probs = []
            dscores = []
            for j in range(2):
                s = dot_nt(k, mask_half(q, j))
                m = jnp.max(s, axis=0, keepdims=True)
                e = jnp.exp2((s - m) * EXP_SCALE)
                l = jnp.sum(e, axis=0, keepdims=True)
                p = e * (1.0 / l)
                dp = dot_nt(v, mask_half(d_o, j)).astype(HALF).astype(WIDE)
                delta = jnp.sum(dp * p, axis=0, keepdims=True)
                ds = (p * ((dp - delta) * 0.125)).astype(HALF)
                probs.append(p.astype(HALF))
                dscores.append(ds)
            dv = dot_nn(jnp.concatenate(probs, axis=1), jnp.concatenate([mask_half(d_o, 0), mask_half(d_o, 1)], axis=0))
            dk = dot_nn(jnp.concatenate(dscores, axis=1), jnp.concatenate([mask_half(q, 0), mask_half(q, 1)], axis=0))
            dq = dot_tn(jnp.concatenate(dscores, axis=0), jnp.concatenate([mask_half(k, 0), mask_half(k, 1)], axis=0))
            dqkv[rows, 128 * pr:128 * pr + 128] = dq.astype(HALF)
            dqkv[rows, DIM + 128 * pr:DIM + 128 * pr + 128] = dk.astype(HALF)
            dqkv[rows, 2 * DIM + 128 * pr:2 * DIM + 128 * pr + 128] = dv.astype(HALF)
    e_f = jnp.concatenate([e_ref[g] for g in range(GROUP)], axis=0).astype(WIDE)
    xhat, inv = normalize(e_f)
    h1 = (xhat * ln_scale[0:1].astype(WIDE) + ln_bias[0:1].astype(WIDE)).astype(HALF)
    dh1 = None
    for s in range(3):
        part = dqkv[:, DIM * s:DIM * s + DIM]
        tiny[s:s + 1] += col_sum(part.astype(WIDE))
        grad = dot_tn(part, h1)
        for k in range(TP):
            dwq[k, s] += grad[192 * k:192 * k + 192]
        term = dot_nn(part, jnp.concatenate([wq[k, s] for k in range(TP)], axis=0))
        dh1 = term if dh1 is None else dh1 + term
    dh1 = dh1.astype(HALF).astype(WIDE)
    dx1 = jnp.concatenate([dx1_ref[g] for g in range(GROUP)], axis=0).astype(WIDE)
    de = (dx1 + norm_back(dh1, xhat, inv, ln_scale[0:1].astype(WIDE))).astype(HALF)
    de_f = de.astype(WIDE)
    tiny[8:9] += col_sum(dh1 * xhat)
    tiny[9:10] += col_sum(dh1)
    acc = de_f[0:TOK]
    for g in range(1, GROUP):
        acc = acc + de_f[TOK * g:TOK * g + TOK]
    dpos[...] += acc
    x = jnp.concatenate([x_ref[g] for g in range(GROUP)], axis=0)
    dwp[...] += dot_tn(x, de)

    @pl.when(step == STEPS - 1)
    def _():
        tiny[4:8] = db1_ref[0:4]
        tiny[10:11] = col_sum(dpos[...])
        tiny[12:16] = dvec2_ref[0:4]
        chip = lax.div(me, 2)
        my_quarter = pl.ds(384 * core + 192 * chip, 192)
        far_quarter = pl.ds(384 * core + 192 * (1 - chip), 192)
        my_part = pl.ds(192 * chip, 192)
        other_half = pl.ds(384 * (1 - core), 384)
        my_half = pl.ds(384 * core, 384)
        near = [push(dwq.at[3], near_q.at[1], n_send.at[0], n_recv.at[0], others[1]), push(dwq.at[1], near_q.at[0], n_send.at[1], n_recv.at[1], others[1]), push(dpos.at[3 * PART:4 * PART], near_pos.at[1], n_send.at[2], n_recv.at[2], others[1]), push(dpos.at[PART:2 * PART], near_pos.at[0], n_send.at[3], n_recv.at[3], others[1]), push(dwp.at[other_half], near_p, n_send.at[4], n_recv.at[4], others[1])]
        tinies = [push(tiny, tiny_out.at[k - 1], t_send.at[k - 1], t_recv.at[k - 1], others[k]) for k in range(1, TP)]
        far = [push(dwq.at[2], far_q, f_send.at[0], f_recv.at[0], others[2]), push(dwp.at[far_quarter], far_p, f_send.at[1], f_recv.at[1], others[2]), push(dpos.at[2 * PART:3 * PART], far_pos, f_send.at[2], f_recv.at[2], others[2])]
        near[4].start()
        near[0].start()
        for c in near[1:4] + tinies:
            c.start()
        near[4].wait_recv()
        dwp[my_half] += near_p[...]
        far[1].start()
        near[0].wait_recv()
        for s in range(3):
            dwq[2, s] += near_q[1, s]
        far[0].start()
        near[2].wait_recv()
        dpos[2 * PART:3 * PART] += near_pos[1]
        far[2].start()
        near[1].wait_recv()
        near[3].wait_recv()
        far[1].wait()
        half_p[my_part] = (dwp[my_quarter] + far_p[...]).astype(HALF)
        spread = push(half_p.at[my_part], half_p.at[my_part], h_send.at[1], h_recv.at[1], others[2])
        spread.start()
        for c in pairs:
            c.wait()
        outs = []

        def total(keep_ref, near_ref, cross_ref, rows):
            copies = [pltpu.make_async_copy(r, sums.at[n, 0:rows], c_sem.at[n, 0]) for n, r in enumerate((keep_ref, near_ref, cross_ref))]
            for c in copies:
                c.start()
            for c in copies:
                c.wait()
            return (sums[0, 0:rows] + sums[1, 0:rows]) + sums[2, 0:rows]

        for n in range(3):
            rows = slice(256 * n, 256 * n + 256)
            total1[rows] = total(keep_a.at[rows], near_a.at[rows], cross_out.at[rows], 256).astype(HALF)
        outs.append(pltpu.make_async_copy(total1, dfc1_out, o_sem.at[0]))
        outs[0].start()
        for n in range(3):
            rows = slice(DIM + 256 * n, DIM + 256 * n + 256)
            part = total(keep_a.at[rows], near_a.at[rows], cross_out.at[rows], 256)
            total2[:, 256 * n:256 * n + 256] = part.T.astype(HALF)
        outs.append(pltpu.make_async_copy(total2, dfc2_out, o_sem.at[1]))
        outs[1].start()
        total3[...] = total(keep_o, near_o, cross_out.at[2 * DIM:PACK], 192).astype(HALF)
        outs.append(pltpu.make_async_copy(total3, dwo_out, o_sem.at[2]))
        outs[2].start()
        far[0].wait_recv()
        for s in range(3):
            half_q[s] = ((dwq[0, s] + near_q[0, s]) + far_q[s]).astype(HALF)
        q_copy = pltpu.make_async_copy(half_q, dqkv_out, local.at[0])
        q_copy.start()
        spread.wait()
        swap = push(half_p, dwp_out.at[my_half], h_send.at[0], h_recv.at[0], others[1])
        swap.start()
        p_copy = pltpu.make_async_copy(half_p, dwp_out.at[my_half], local.at[1])
        p_copy.start()
        far[2].wait_recv()
        half_pos[...] = ((dpos[0:PART] + near_pos[0]) + far_pos[...]).astype(HALF)
        pos_copy = pltpu.make_async_copy(half_pos, dpos_out, local.at[2])
        pos_copy.start()
        for c in near:
            c.wait_send()
        for c in tinies:
            c.wait()
        far[0].wait_send()
        far[2].wait_send()
        tiny_copy = pltpu.make_async_copy(tiny, tiny_out.at[3], local.at[3])
        tiny_copy.start()
        for c in outs:
            c.wait()
        q_copy.wait()
        p_copy.wait()
        pos_copy.wait()
        tiny_copy.wait()
        swap.wait()


def attn_bwd(keep_b, near_b, keep_a, near_a, keep_o, near_o, e, qkv, d_o, dx1, x, wq, ln_scale, ln_bias, dvec2, db1):
    dma = pltpu.SemaphoreType.DMA
    return pl.pallas_call(
        attn_bwd_kernel,
        grid=(STEPS,),
        in_specs=[any_spec()] * 6 + [image_spec(DIM), image_spec(3 * DIM), image_spec(DIM), image_spec(DIM), image_spec(DIM), fixed((TP, 3, 192, DIM)), vec_spec(2, DIM), vec_spec(2, DIM), vec_spec(8, DIM), vec_spec(8, DIM)],
        out_specs=[any_spec()] * 8,
        out_shape=[wide_shape(PACK, DIM), half_shape(DIM, DIM), half_shape(DIM, DIM), half_shape(192, DIM), half_shape(3, 192, DIM), half_shape(DIM, DIM), half_shape(PART, DIM), wide_shape(TP, 16, DIM)],
        scratch_shapes=[pltpu.VMEM((2, CHUNK, DIM), WIDE), pltpu.VMEM((2, CHUNK, DIM), WIDE), pltpu.VMEM((CHUNKS, CHUNK, DIM), WIDE), pltpu.VMEM((ROWS, 3 * DIM), HALF), pltpu.VMEM((TP, 3, 192, DIM), WIDE), pltpu.VMEM((DIM, DIM), WIDE), pltpu.VMEM((TOK, DIM), WIDE), pltpu.VMEM((16, DIM), WIDE), pltpu.VMEM((2, 3, 192, DIM), WIDE), pltpu.VMEM((384, DIM), WIDE), pltpu.VMEM((2, PART, DIM), WIDE), pltpu.VMEM((3, 192, DIM), WIDE), pltpu.VMEM((192, DIM), WIDE), pltpu.VMEM((PART, DIM), WIDE), pltpu.VMEM((3, 192, DIM), HALF), pltpu.VMEM((384, DIM), HALF), pltpu.VMEM((PART, DIM), HALF), dma((CHUNKS,)), dma((CHUNKS,)), dma((3,)), dma((3,)), dma((5,)), dma((5,)), dma((3,)), dma((3,)), dma((2,)), dma((2,)), dma((3, 2)), dma((3,)), pltpu.VMEM((DIM, DIM), HALF), pltpu.VMEM((DIM, DIM), HALF), pltpu.VMEM((192, DIM), HALF), dma((4,))],
        compiler_params=params(3),
        cost_estimate=pl.CostEstimate(flops=100_000_000_000, bytes_accessed=80_000_000, transcendentals=12_000_000),
        name='attn_bwd',
    )(keep_b, near_b, keep_a, near_a, keep_o, near_o, e, qkv, d_o, dx1, x, wq, ln_scale, ln_bias, dvec2, db1)


def finish_kernel(x2, fc1, fc2, wo, qkv, wp, pos, tiny, x2_out, fc1_out, fc2_out, wo_out, qkv_out, wp_out, pos_out, patch_b, ln_scale, ln_bias, qkv_b, out_b, fc1_b, fc2_b):
    for src, dst in ((x2, x2_out), (fc1, fc1_out), (fc2, fc2_out), (wo, wo_out), (qkv, qkv_out), (wp, wp_out), (pos, pos_out)):
        dst[...] = src[...]

    @pl.when(pl.program_id(0) == 0)
    def _():
        vec = ((tiny[3] + tiny[0]) + (tiny[1] + tiny[2])).astype(HALF)
        patch_b[...] = vec[10:11].reshape(DIM)
        ln_scale[0:1] = vec[8:9]
        ln_scale[1:2] = vec[12:13]
        ln_bias[0:1] = vec[9:10]
        ln_bias[1:2] = vec[13:14]
        fc2_b[...] = vec[14:15].reshape(DIM)
        out_b[...] = vec[15:16].reshape(DIM)
        fc1_b[...] = ((tiny[3, 4:5] + tiny[0, 5:6]) + (tiny[1, 6:7] + tiny[2, 7:8])).astype(HALF).reshape(DIM)
        for s in range(3):
            for h in range(3):
                at = [tiny[j, s:s + 1, 192 * k + 64 * h:192 * k + 64 * h + 64] for k, j in enumerate((3, 0, 1, 2))]
                qkv_b[s, h:h + 1] = ((at[0] + at[1]) + (at[2] + at[3])).astype(HALF)


def finish(x2, fc1, fc2, wo, qkv, wp, pos, tiny):
    arrays = (x2, fc1, fc2, wo, qkv, wp, pos)
    specs = [pl.BlockSpec((a.shape[0] // 4,) + a.shape[1:], lambda i, n=a.ndim: (i,) + (0,) * (n - 1)) for a in arrays]
    smalls = [(DIM,), (2, DIM), (2, DIM), (3, 3, 64), (DIM,), (DIM,), (DIM,)]
    return pl.pallas_call(
        finish_kernel,
        grid=(4,),
        in_specs=specs + [vec_spec(TP, 16, DIM)],
        out_specs=specs + [vec_spec(*shape) for shape in smalls],
        out_shape=[jax.ShapeDtypeStruct(a.shape, a.dtype) for a in arrays] + [half_shape(*shape) for shape in smalls],
        compiler_params=pltpu.CompilerParams(dimension_semantics=('arbitrary',), vmem_limit_bytes=67043328),
        name='finish',
    )(*arrays, tiny)


def group_step(patches, patch_w, patch_b, pos_emb, ln_scale, ln_bias, qkv_w, qkv_b, out_w, out_b, fc1_w, fc1_b, fc2_w, fc2_b, d_out):
    wq = qkv_w.transpose(0, 2, 3, 1).reshape(3, 192, DIM)
    wo = out_w.reshape(192, DIM)
    e, qkv, o, x1, x, wq_all, wop_all, bias_all, w1_rest, w2_near = attn_fwd(patches, wq, wo, pos_emb, fc1_w, fc2_w, patch_w, patch_b, qkv_b, fc1_b, out_b, ln_scale, ln_bias)
    dout, y, dh, w2_far, keep_a, give_a, dvec_n, db1_n = mlp_near(d_out, x1, fc1_w, w1_rest, fc2_w, w2_near, bias_all, ln_scale, ln_bias)
    x_two, dx1, d_o, near_a, keep_o, near_o, keep_b, near_b, dvec2, db1 = mlp_far(give_a, x1, o, dout, y, dh, w1_rest, w2_far, wop_all, bias_all, ln_scale, ln_bias, fc2_b, dvec_n, db1_n)
    _, d_fc1_w, d_fc2_w, d_out_w, d_qkv, d_patch_w, d_pos, tiny = attn_bwd(keep_b, near_b, keep_a, near_a, keep_o, near_o, e, qkv, d_o, dx1, x, wq_all, ln_scale, ln_bias, dvec2, db1)
    x_two, d_fc1_w, d_fc2_w, d_out_w, d_qkv, d_patch_w, d_pos, d_patch_b, d_ln_scale, d_ln_bias, d_qkv_b, d_out_b, d_fc1_b, d_fc2_b = finish(x_two, d_fc1_w, d_fc2_w, d_out_w, d_qkv.reshape(576, DIM), d_patch_w, d_pos, tiny)
    d_qkv_w = d_qkv.reshape(3, 3, 64, DIM).transpose(0, 3, 1, 2)
    return (x_two, d_patch_w, d_patch_b, d_pos, d_ln_scale, d_ln_bias, d_qkv_w, d_qkv_b, d_out_w.reshape(3, 64, DIM), d_out_b, d_fc1_w, d_fc1_b, d_fc2_w, d_fc2_b)


def solution(mesh):
    in_specs = (P('dp', 'tp', None), P(), P(), P('tp', None), P(), P(), P(None, None, 'tp', None), P(None, 'tp', None), P('tp', None, None), P(), P(None, 'tp'), P('tp'), P('tp', None), P(), P('dp', 'tp', None))
    out_specs = (P('dp', 'tp', None), P('dp', None), P('dp'), P(('dp', 'tp'), None), P('dp', None), P('dp', None), P('dp', None, 'tp', None), P('dp', 'tp', None), P(('dp', 'tp'), None, None), P('dp'), P('dp', 'tp'), P(('dp', 'tp')), P(('dp', 'tp'), None), P('dp'))
    return jax.shard_map(group_step, mesh=mesh, in_specs=in_specs, out_specs=out_specs, check_vma=False)
```

```python
import functools
import jax
import jax.numpy as jnp
from jax import lax
from jax.experimental import pallas as pl
from jax.experimental.pallas import tpu as pltpu
from jax.sharding import PartitionSpec as P

LN_EPS = 1e-6
TP = 4
WIDE = jnp.float32
HALF = jnp.bfloat16
IMAGES = 16
TOK = 256
PART = 64
DIM = 768
GROUP = 1
ROWS = GROUP * TOK
STEPS = IMAGES // GROUP
FRONT = 2
FRONT_STEPS = IMAGES // FRONT
PAIRS = 6
EXP_SCALE = 0.125 * 1.4426950408889634
GELU_C = 0.7978845608028654
GELU_A = 0.044715
AHEAD = 6 // FRONT
PACK = 2 * DIM + 192
EARLY = 256
LATE = DIM - EARLY
CHUNKS = 6
CHUNK = PACK // CHUNKS


def dot_nn(a, b):
    return lax.dot_general(a, b, (((1,), (0,)), ((), ())), preferred_element_type=WIDE)


def dot_nt(a, b):
    return lax.dot_general(a, b, (((1,), (1,)), ((), ())), preferred_element_type=WIDE)


def dot_tn(a, b):
    return lax.dot_general(a, b, (((0,), (0,)), ((), ())), preferred_element_type=WIDE)


def normalize(x_f):
    mean = jnp.sum(x_f, axis=-1, keepdims=True) * (1.0 / DIM)
    centered = x_f - mean
    var = jnp.sum(centered * centered, axis=-1, keepdims=True) * (1.0 / DIM)
    inv = lax.rsqrt(var + LN_EPS)
    return centered * inv, inv


def norm_back(d_out_f, xhat, inv, scale):
    d_hat = d_out_f * scale
    m1 = jnp.sum(d_hat, axis=-1, keepdims=True) * (1.0 / DIM)
    m2 = jnp.sum(d_hat * xhat, axis=-1, keepdims=True) * (1.0 / DIM)
    return (d_hat - m1 - xhat * m2) * inv


def lane_half(j):
    lane = lax.broadcasted_iota(jnp.int32, (1, 128), 1)
    return (lane < 64) if j == 0 else (lane >= 64)


def mask_half(x, j):
    return jnp.where(lane_half(j), x, jnp.zeros_like(x))


def col_sum(x):
    return jnp.sum(x, axis=0, keepdims=True)


def row(ref):
    return ref[...].reshape(1, DIM).astype(WIDE)


def peers():
    me = lax.axis_index('tp')
    core = lax.rem(me, 2)
    chip = lax.div(me, 2)
    return me, core, (me, me + 1 - 2 * core, me + 2 - 4 * chip, 3 - me)


def meet(others):
    barrier = pltpu.get_barrier_semaphore()
    for k in range(1, TP):
        pl.semaphore_signal(barrier, inc=1, device_id={'tp': others[k]}, device_id_type=pl.DeviceIdType.MESH)
    pl.semaphore_wait(barrier, TP - 1)


def push(src, dst, send, recv, peer):
    return pltpu.make_async_remote_copy(src_ref=src, dst_ref=dst, send_sem=send, recv_sem=recv, device_id={'tp': peer}, device_id_type=pl.DeviceIdType.MESH)


def image_rows(owner, group, size):
    return pl.ds(owner * IMAGES + group * size, size)


def group_sends(src, buf, send, recv, others, group):
    return [push(src.at[image_rows(others[k], group, FRONT)], buf.at[k, pl.ds(group * FRONT, FRONT)], send.at[k - 1, group], recv.at[k - 1, group], others[k]) for k in (2, 3, 1)]


def slot_rows(buf, group):
    base = group * FRONT
    return jnp.concatenate([buf[k, base + g] for g in range(FRONT) for k in range(TP)], axis=0)


def mlp_slot(f, base, h2, dout, w1, w2, bias, y, dh2, dw1, dw2, db1_ref):
    hids = []
    dpres = []
    for c in range(w1.shape[1] // 256):
        cols = slice(256 * c, 256 * c + 256)
        units = slice(base + 256 * c, base + 256 * c + 256)
        pre = dot_nn(h2, w1[:, cols]) + bias[f, 3:4, units].astype(WIDE)
        sq = pre * pre
        t = jnp.tanh(pre * (GELU_C + (GELU_C * GELU_A) * sq))
        half_pre = 0.5 * pre
        hids.append((half_pre + half_pre * t).astype(HALF))
        slope = (0.5 + 0.5 * t) + (half_pre * (1.0 - t * t)) * (GELU_C + (3.0 * GELU_C * GELU_A) * sq)
        dpre = dot_nt(dout, w2[cols]).astype(HALF).astype(WIDE) * slope
        db1_ref[f:f + 1, units] += col_sum(dpre)
        dpres.append(dpre.astype(HALF))
    hid = jnp.concatenate(hids, axis=1)
    dpre_h = jnp.concatenate(dpres, axis=1)
    part_y = dot_nn(hid, w2)
    part_h = dot_nt(dpre_h, w1)
    y = part_y if y is None else y + part_y
    dh2 = part_h if dh2 is None else dh2 + part_h
    dw1[...] += dot_tn(h2, dpre_h)
    dw2[...] += dot_tn(dout, hid)
    return y, dh2


def front_kernel(patches, d_out, wq_own, wo_own, pos_own, w1_own, w2_own, wp, patch_b, qkv_b, fc1_b, out_b, ln_scale, ln_bias, e_ref, qkv_ref, o_ref, x1_ref, x_ref, dout_ref, y_ref, dh_ref, wq_out, wop_out, bias_out, w1_far, w2_far, keep_out, give_out, part1_out, part2_out, dvec_ref, db1_ref, xbuf, dbuf, wq, wop, w1, w2, wa1, wa2, bias, bias_own, bqkv, dw1, dw2, dwa1, dwa2, x_send, x_recv, d_send, d_recv, w_send, w_recv, local, done):
    step = pl.program_id(0)
    me, core, others = peers()
    small = []
    for n, (src, cut) in enumerate(((wq_own, None), (wo_own, (0, 192)), (pos_own, (192, 256)))):
        at = [wq.at[k] if cut is None else wop.at[k, cut[0]:cut[1]] for k in range(TP)]
        small.append((push(src, at[2], w_send.at[n, 1], w_recv.at[n, 1], others[2]), push(src, at[1], w_send.at[n, 0], w_recv.at[n, 0], others[1]), push(at[2], at[3], w_send.at[n, 2], w_recv.at[n, 2], others[1])))
    near = [push(w1_own, w1.at[1], w_send.at[3, 0], w_recv.at[3, 0], others[1]), push(w2_own, w2.at[1], w_send.at[4, 0], w_recv.at[4, 0], others[1])]
    early = [push(w1_own.at[:, 0:EARLY], wa1.at[0], w_send.at[6, 0], w_recv.at[6, 0], others[2]), push(w2_own.at[0:EARLY], wa2.at[0], w_send.at[7, 0], w_recv.at[7, 0], others[2])]
    early_relay = [push(wa1.at[0], wa1.at[1], w_send.at[6, 1], w_recv.at[6, 1], others[1]), push(wa2.at[0], wa2.at[1], w_send.at[7, 1], w_recv.at[7, 1], others[1])]
    far = [push(w1_own.at[:, EARLY:DIM], w1_far.at[0], w_send.at[3, 1], w_recv.at[3, 1], others[2]), push(w2_own.at[EARLY:DIM], w2_far.at[0], w_send.at[4, 1], w_recv.at[4, 1], others[2])]
    relay = [push(w1_far.at[0], w1_far.at[1], w_send.at[3, 2], w_recv.at[3, 2], others[1]), push(w2_far.at[0], w2_far.at[1], w_send.at[4, 2], w_recv.at[4, 2], others[1])]
    biases = [push(bias_own, bias.at[k], w_send.at[5, k - 1], w_recv.at[5, k - 1], others[k]) for k in range(1, TP)]
    own = [pltpu.make_async_copy(wq_own, wq.at[0], local.at[0]), pltpu.make_async_copy(wo_own, wop.at[0, 0:192], local.at[1]), pltpu.make_async_copy(pos_own, wop.at[0, 192:256], local.at[2]), pltpu.make_async_copy(patches.at[pl.ds(me * IMAGES, IMAGES)], xbuf.at[0], local.at[3]), pltpu.make_async_copy(d_out.at[pl.ds(me * IMAGES, IMAGES)], dbuf.at[0], local.at[7]), pltpu.make_async_copy(w1_own, w1.at[0], local.at[8]), pltpu.make_async_copy(w2_own, w2.at[0], local.at[9])]
    flush = [pltpu.make_async_copy(wq, wq_out, local.at[4]), pltpu.make_async_copy(wop, wop_out, local.at[5]), pltpu.make_async_copy(bias, bias_out, local.at[6])]

    def arrivals(group):
        return group_sends(patches, xbuf, x_send, x_recv, others, group) + group_sends(d_out, dbuf, d_send, d_recv, others, group)

    @pl.when(step == 0)
    def _():
        bias_own[...] = jnp.zeros_like(bias_own)
        for s in range(3):
            for h in range(3):
                bias_own[s:s + 1, 64 * h:64 * h + 64] = qkv_b[s, h:h + 1]
        bias_own[3:4] = fc1_b[...].reshape(1, DIM)
        bias[0] = bias_own[...]
        meet(others)
        for n in range(3):
            small[n][0].start()
        for c in biases:
            c.start()
        for n in range(3):
            small[n][1].start()
        for g in range(AHEAD):
            for c in arrivals(g) + (early if g == 0 else []):
                c.start()
        for c in own + near:
            c.start()
        dw1[...] = jnp.zeros_like(dw1)
        dw2[...] = jnp.zeros_like(dw2)
        dwa1[...] = jnp.zeros_like(dwa1)
        dwa2[...] = jnp.zeros_like(dwa2)
        dvec_ref[...] = jnp.zeros_like(dvec_ref)
        db1_ref[...] = jnp.zeros_like(db1_ref)
        for n in range(3):
            small[n][0].wait_recv()
            small[n][2].start()
        for c in own:
            c.wait()
        for n in range(3):
            small[n][1].wait_recv()
            small[n][2].wait_recv()
        for c in biases + near:
            c.wait_recv()
        for s in range(3):
            for k in range(TP):
                bqkv[s:s + 1, 192 * k:192 * k + 192] = bias[k, s:s + 1, 0:192].astype(WIDE)
        for c in flush:
            c.start()

    @pl.when(step + AHEAD < FRONT_STEPS)
    def _():
        for c in arrivals(step + AHEAD):
            c.start()

    @pl.when(step == FRONT_STEPS - AHEAD)
    def _():
        far[0].start()
        far[1].start()

    for c in group_sends(patches, xbuf, x_send, x_recv, others, step):
        c.wait_recv()
    x = slot_rows(xbuf, step)
    posb = jnp.concatenate([wop[k, 192:192 + PART] for k in range(TP)], axis=0).astype(WIDE) + row(patch_b)
    emb = dot_nn(x, wp[...]) + jnp.concatenate([posb] * FRONT, axis=0)
    e_h = emb.astype(HALF)
    for g in range(FRONT):
        x_ref[g] = x[TOK * g:TOK * g + TOK]
        e_ref[g] = e_h[TOK * g:TOK * g + TOK]
    e_f = e_h.astype(WIDE)
    xhat, _ = normalize(e_f)
    h1 = (xhat * ln_scale[0:1].astype(WIDE) + ln_bias[0:1].astype(WIDE)).astype(HALF)
    for s in range(3):
        part = (dot_nt(h1, jnp.concatenate([wq[k, s] for k in range(TP)], axis=0)) + bqkv[s:s + 1]).astype(HALF)
        for g in range(FRONT):
            qkv_ref[g, :, DIM * s:DIM * s + DIM] = part[TOK * g:TOK * g + TOK]
    for g in range(FRONT):
        for pr in range(PAIRS):
            q = qkv_ref[g, :, 128 * pr:128 * pr + 128]
            k = qkv_ref[g, :, DIM + 128 * pr:DIM + 128 * pr + 128]
            v = qkv_ref[g, :, 2 * DIM + 128 * pr:2 * DIM + 128 * pr + 128]
            probs = []
            for j in range(2):
                s = dot_nt(mask_half(q, j), k)
                m = jnp.max(s, axis=-1, keepdims=True)
                e = jnp.exp2((s - m) * EXP_SCALE)
                l = jnp.sum(e, axis=-1, keepdims=True)
                probs.append((e * (1.0 / l)).astype(HALF))
            pv = dot_nn(jnp.concatenate(probs, axis=1), jnp.concatenate([mask_half(v, 0), mask_half(v, 1)], axis=0))
            o_ref[g, :, 128 * pr:128 * pr + 128] = pv.astype(HALF)
    o = jnp.concatenate([o_ref[g] for g in range(FRONT)], axis=0)
    e_f = jnp.concatenate([e_ref[g] for g in range(FRONT)], axis=0).astype(WIDE)
    x1 = (e_f + (dot_nn(o, jnp.concatenate([wop[k, 0:192] for k in range(TP)], axis=0)) + row(out_b))).astype(HALF)
    for g in range(FRONT):
        x1_ref[g] = x1[TOK * g:TOK * g + TOK]

    xhat, _ = normalize(x1.astype(WIDE))
    h2 = (xhat * ln_scale[1:2].astype(WIDE) + ln_bias[1:2].astype(WIDE)).astype(HALF)
    for c in group_sends(d_out, dbuf, d_send, d_recv, others, step):
        c.wait_recv()
    dout = slot_rows(dbuf, step)
    dvec_ref[2:3] += col_sum(dout.astype(WIDE))
    y = None
    dh2 = None
    for f in range(2):
        y, dh2 = mlp_slot(f, 0, h2, dout, w1[f], w2[f], bias, y, dh2, dw1.at[f], dw2.at[f], db1_ref)

    @pl.when(step == 0)
    def _():
        for n in range(2):
            early[n].wait_recv()
            early_relay[n].start()
        for c in early_relay:
            c.wait_recv()

    for f in range(2):
        y, dh2 = mlp_slot(f + 2, 0, h2, dout, wa1[f], wa2[f], bias, y, dh2, dwa1.at[f], dwa2.at[f], db1_ref)
    for g in range(FRONT):
        rows = slice(TOK * g, TOK * g + TOK)
        dout_ref[g] = dout[rows]
        y_ref[g] = y[rows]
        dh_ref[g] = dh2[rows]

    @pl.when(step == FRONT_STEPS - 1)
    def _():
        copies = []
        for n, out in enumerate((keep_out, give_out)):
            copies.append(pltpu.make_async_copy(dw1.at[n], out.at[0:DIM], done.at[2 * n]))
            copies.append(pltpu.make_async_copy(dw2.at[n], out.at[DIM:2 * DIM], done.at[2 * n + 1]))
        copies.append(pltpu.make_async_copy(dwa1, part1_out, done.at[4]))
        copies.append(pltpu.make_async_copy(dwa2, part2_out, done.at[5]))
        for c in copies:
            c.start()
        for n in range(2):
            far[n].wait_recv()
            relay[n].start()
        for c in relay:
            c.wait_recv()
        for c in small[0] + small[1] + small[2] + tuple(near + early + early_relay + far + relay + biases):
            c.wait_send()
        for c in copies + flush:
            c.wait()
        for g in range(FRONT_STEPS):
            for c in arrivals(g):
                c.wait_send()


def fixed(shape):
    return pl.BlockSpec(shape, lambda i: (0,) * len(shape), pipeline_mode=pl.Buffered(1))


def image_spec(width, size=GROUP):
    return pl.BlockSpec((size, TOK, width), lambda i: (i, 0, 0))


def any_spec():
    return pl.BlockSpec(memory_space=pl.ANY)


def params(cid):
    return pltpu.CompilerParams(dimension_semantics=('arbitrary',), vmem_limit_bytes=67043328, collective_id=cid, has_side_effects=True)


def image_shape(width):
    return jax.ShapeDtypeStruct((IMAGES, TOK, width), HALF)


def half_shape(*shape):
    return jax.ShapeDtypeStruct(shape, HALF)


def wide_shape(*shape):
    return jax.ShapeDtypeStruct(shape, WIDE)


def vec_spec(*shape):
    return pl.BlockSpec(shape, lambda i: (0,) * len(shape))


def front(patches, d_out, wq, wo, pos, w1, w2, wp, patch_b, qkv_b, fc1_b, out_b, ln_scale, ln_bias):
    dma = pltpu.SemaphoreType.DMA
    wide_image = jax.ShapeDtypeStruct((IMAGES, TOK, DIM), WIDE)
    return pl.pallas_call(
        front_kernel,
        grid=(FRONT_STEPS,),
        in_specs=[any_spec()] * 7 + [fixed((DIM, DIM)), vec_spec(DIM), vec_spec(3, 3, 64), vec_spec(DIM), vec_spec(DIM), vec_spec(2, DIM), vec_spec(2, DIM)],
        out_specs=[image_spec(DIM, FRONT), image_spec(3 * DIM, FRONT)] + [image_spec(DIM, FRONT)] * 6 + [any_spec()] * 9 + [vec_spec(8, DIM), vec_spec(8, DIM)],
        out_shape=[image_shape(DIM), image_shape(3 * DIM), image_shape(DIM), image_shape(DIM), image_shape(DIM), image_shape(DIM), wide_image, wide_image, half_shape(TP, 3, 192, DIM), half_shape(TP, 256, DIM), half_shape(TP, 16, DIM), half_shape(2, DIM, LATE), half_shape(2, LATE, DIM), wide_shape(2 * DIM, DIM), wide_shape(2 * DIM, DIM), wide_shape(2, DIM, EARLY), wide_shape(2, DIM, EARLY), wide_shape(8, DIM), wide_shape(8, DIM)],
        scratch_shapes=[pltpu.VMEM((TP, IMAGES, PART, DIM), HALF), pltpu.VMEM((TP, IMAGES, PART, DIM), HALF), pltpu.VMEM((TP, 3, 192, DIM), HALF), pltpu.VMEM((TP, 256, DIM), HALF), pltpu.VMEM((2, DIM, DIM), HALF), pltpu.VMEM((2, DIM, DIM), HALF), pltpu.VMEM((2, DIM, EARLY), HALF), pltpu.VMEM((2, EARLY, DIM), HALF), pltpu.VMEM((TP, 16, DIM), HALF), pltpu.VMEM((16, DIM), HALF), pltpu.VMEM((8, DIM), WIDE), pltpu.VMEM((2, DIM, DIM), WIDE), pltpu.VMEM((2, DIM, DIM), WIDE), pltpu.VMEM((2, DIM, EARLY), WIDE), pltpu.VMEM((2, DIM, EARLY), WIDE), dma((3, FRONT_STEPS)), dma((3, FRONT_STEPS)), dma((3, FRONT_STEPS)), dma((3, FRONT_STEPS)), dma((8, 3)), dma((8, 3)), dma((10,)), dma((6,))],
        compiler_params=params(0),
        cost_estimate=pl.CostEstimate(flops=120_000_000_000, bytes_accessed=120_000_000, transcendentals=18_000_000),
        name='front',
    )(patches, d_out, wq, wo, pos, w1, w2, wp, patch_b, qkv_b, fc1_b, out_b, ln_scale, ln_bias)


def mlp_far_kernel(give, part1, part2, x1_ref, o_ref, dout_ref, y_ref, dh_ref, w1_far, w2_far, wop, bias, ln_scale, ln_bias, fc2_b, dvec_near, db1_near, x2_out, dx1_ref, do_ref, near_a, keep_o, near_o, keep_b, near_b, dvec_ref, db1_ref, ybuf, dw1, dw2, dwo, y_send, y_recv, y_own, g_send, g_recv, local):
    step = pl.program_id(0)
    me, core, others = peers()
    slot = lax.rem(step, 2)

    def y_sends(at, group):
        return [push(ybuf.at[at, k], x2_out.at[image_rows(me, group, GROUP)], y_send.at[k - 1, at], y_recv.at[k - 1, group], others[k]) for k in (2, 3, 1)]

    def y_keep(at, group):
        return pltpu.make_async_copy(ybuf.at[at, 0], x2_out.at[image_rows(me, group, GROUP)], y_own.at[at])

    def y_wait(at, group):
        for c in y_sends(at, group):
            c.wait_send()
        y_keep(at, group).wait()

    early = push(give, near_a, g_send.at[0], g_recv.at[0], others[1])
    grads = [push(dw1.at[1], near_b.at[0:DIM], g_send.at[1], g_recv.at[1], others[1]), push(dw2.at[1], near_b.at[DIM:2 * DIM], g_send.at[2], g_recv.at[2], others[1]), push(dwo.at[576:768], near_b.at[2 * DIM:PACK], g_send.at[3], g_recv.at[3], others[1]), push(dwo.at[192:384], near_o, g_send.at[4], g_recv.at[4], others[1])]
    keeps = [pltpu.make_async_copy(dw1.at[0], keep_b.at[0:DIM], local.at[0]), pltpu.make_async_copy(dw2.at[0], keep_b.at[DIM:2 * DIM], local.at[1]), pltpu.make_async_copy(dwo.at[384:576], keep_b.at[2 * DIM:PACK], local.at[2]), pltpu.make_async_copy(dwo.at[0:192], keep_o, local.at[3])]

    @pl.when(step == 0)
    def _():
        meet(others)
        early.start()
        loads = [pltpu.make_async_copy(part1, dw1.at[:, :, 0:EARLY], local.at[4]), pltpu.make_async_copy(part2, dw2.at[:, :, 0:EARLY], local.at[5])]
        for c in loads:
            c.start()
        for acc in (dw1, dw2):
            for n in range(2):
                acc[n, :, EARLY:DIM] = jnp.zeros((DIM, LATE), WIDE)
        for c in loads:
            c.wait()
        dwo[...] = jnp.zeros_like(dwo)
        dvec_ref[...] = dvec_near[...]
        db1_ref[...] = db1_near[...]

    x1 = jnp.concatenate([x1_ref[g] for g in range(GROUP)], axis=0)
    dout = jnp.concatenate([dout_ref[g] for g in range(GROUP)], axis=0)
    xhat, inv = normalize(x1.astype(WIDE))
    h2 = (xhat * ln_scale[1:2].astype(WIDE) + ln_bias[1:2].astype(WIDE)).astype(HALF)
    y = jnp.concatenate([y_ref[g] for g in range(GROUP)], axis=0)
    dh2 = jnp.concatenate([dh_ref[g] for g in range(GROUP)], axis=0)
    for f in range(2):
        y, dh2 = mlp_slot(f + 2, EARLY, h2, dout, w1_far[f], w2_far[f], bias, y, dh2, dw1.at[f, :, EARLY:DIM], dw2.at[f, :, EARLY:DIM], db1_ref)
    x2 = (x1.astype(WIDE) + (y + row(fc2_b))).astype(HALF)

    @pl.when(step >= 2)
    def _():
        y_wait(slot, step - 2)

    for g in range(GROUP):
        for k in range(TP):
            ybuf[slot, k, g] = x2[TOK * g + PART * k:TOK * g + PART * k + PART]
    dh2 = dh2.astype(HALF).astype(WIDE)
    xhat, inv = normalize(x1.astype(WIDE))
    dout_f = dout.astype(WIDE)
    dx1 = (dout_f + norm_back(dh2, xhat, inv, ln_scale[1:2].astype(WIDE))).astype(HALF)
    dvec_ref[0:1] += col_sum(dh2 * xhat)
    dvec_ref[1:2] += col_sum(dh2)
    dvec_ref[3:4] += col_sum(dx1.astype(WIDE))
    d_o = dot_nt(dx1, jnp.concatenate([wop[k, 0:192] for k in range(TP)], axis=0)).astype(HALF)
    for g in range(GROUP):
        dx1_ref[g] = dx1[TOK * g:TOK * g + TOK]
        do_ref[g] = d_o[TOK * g:TOK * g + TOK]
    o = jnp.concatenate([o_ref[g] for g in range(GROUP)], axis=0)
    dwo[...] += dot_tn(o, dx1)

    for c in y_sends(slot, step):
        c.start()
    y_keep(slot, step).start()

    @pl.when(step == STEPS - 1)
    def _():
        for c in grads + keeps:
            c.start()
        for c in keeps:
            c.wait()
        early.wait()
        for c in grads:
            c.wait()
        for g in range(STEPS):
            for c in y_sends(g % 2, g):
                c.wait_recv()
        for g in (STEPS - 2, STEPS - 1):
            y_wait(g % 2, g)


def mlp_far(give, part1, part2, x1, o, dout, y, dh, w1_far, w2_far, wop, bias, ln_scale, ln_bias, fc2_b, dvec_near, db1_near):
    dma = pltpu.SemaphoreType.DMA
    return pl.pallas_call(
        mlp_far_kernel,
        grid=(STEPS,),
        in_specs=[any_spec()] * 3 + [image_spec(DIM)] * 5 + [fixed((2, DIM, LATE)), fixed((2, LATE, DIM)), fixed((TP, 256, DIM)), fixed((TP, 16, DIM)), vec_spec(2, DIM), vec_spec(2, DIM), vec_spec(DIM), vec_spec(8, DIM), vec_spec(8, DIM)],
        out_specs=[any_spec(), image_spec(DIM), image_spec(DIM)] + [any_spec()] * 5 + [vec_spec(8, DIM), vec_spec(8, DIM)],
        out_shape=[half_shape(TP * IMAGES, PART, DIM), image_shape(DIM), image_shape(DIM), wide_shape(2 * DIM, DIM), wide_shape(192, DIM), wide_shape(192, DIM), wide_shape(PACK, DIM), wide_shape(PACK, DIM), wide_shape(8, DIM), wide_shape(8, DIM)],
        scratch_shapes=[pltpu.VMEM((2, TP, GROUP, PART, DIM), HALF), pltpu.VMEM((2, DIM, DIM), WIDE), pltpu.VMEM((2, DIM, DIM), WIDE), pltpu.VMEM((DIM, DIM), WIDE), dma((3, 2)), dma((3, STEPS)), dma((2,)), dma((5,)), dma((5,)), dma((6,))],
        compiler_params=params(2),
        cost_estimate=pl.CostEstimate(flops=70_000_000_000, bytes_accessed=80_000_000, transcendentals=6_000_000),
        name='mlp_far',
    )(give, part1, part2, x1, o, dout, y, dh, w1_far, w2_far, wop, bias, ln_scale, ln_bias, fc2_b, dvec_near, db1_near)


def attn_bwd_kernel(keep_b, near_b, keep_a, near_a, keep_o, near_o, e_ref, qkv_ref, do_ref, dx1_ref, x_ref, wq, ln_scale, ln_bias, dvec2_ref, db1_ref, cross_out, dfc1_out, dfc2_out, dwo_out, dqkv_out, dwp_out, dpos_out, tiny_out, fetch_k, fetch_n, sums, dqkv, dwq, dwp, dpos, tiny, near_q, near_p, near_pos, far_q, far_p, far_pos, half_q, half_p, half_pos, p_send, p_recv, t_send, t_recv, n_send, n_recv, f_send, f_recv, h_send, h_recv, c_sem, o_sem, total1, total2, total3, local):
    step = pl.program_id(0)
    me, core, others = peers()
    pairs = [push(sums.at[n], cross_out.at[CHUNK * n:CHUNK * n + CHUNK], p_send.at[n], p_recv.at[n], others[2]) for n in range(CHUNKS)]

    def fetch(n):
        rows = pl.ds(n * CHUNK, CHUNK)
        at = lax.rem(n, 2)
        return (pltpu.make_async_copy(keep_b.at[rows], fetch_k.at[at], c_sem.at[0, at]), pltpu.make_async_copy(near_b.at[rows], fetch_n.at[at], c_sem.at[1, at]))

    @pl.when(step == 0)
    def _():
        meet(others)
        for c in fetch(0):
            c.start()

    @pl.when(step < CHUNKS)
    def _():
        @pl.when(step + 1 < CHUNKS)
        def _():
            for c in fetch(step + 1):
                c.start()
        for c in fetch(step):
            c.wait()
        at = lax.rem(step, 2)
        sums[step] = fetch_k[at] + fetch_n[at]

    @pl.when(step == 0)
    def _():
        dwq[...] = jnp.zeros_like(dwq)
        dwp[...] = jnp.zeros_like(dwp)
        dpos[...] = jnp.zeros_like(dpos)
        tiny[...] = jnp.zeros_like(tiny)

    @pl.when(step < CHUNKS)
    def _():
        push(sums.at[step], cross_out.at[pl.ds(step * CHUNK, CHUNK)], p_send.at[step], p_recv.at[step], others[2]).start()

    for g in range(GROUP):
        rows = slice(TOK * g, TOK * g + TOK)
        for pr in range(PAIRS):
            cols = slice(128 * pr, 128 * pr + 128)
            q = qkv_ref[g, :, 128 * pr:128 * pr + 128]
            k = qkv_ref[g, :, DIM + 128 * pr:DIM + 128 * pr + 128]
            v = qkv_ref[g, :, 2 * DIM + 128 * pr:2 * DIM + 128 * pr + 128]
            d_o = do_ref[g, :, 128 * pr:128 * pr + 128]
            probs = []
            dscores = []
            for j in range(2):
                s = dot_nt(k, mask_half(q, j))
                m = jnp.max(s, axis=0, keepdims=True)
                e = jnp.exp2((s - m) * EXP_SCALE)
                l = jnp.sum(e, axis=0, keepdims=True)
                p = e * (1.0 / l)
                dp = dot_nt(v, mask_half(d_o, j)).astype(HALF).astype(WIDE)
                delta = jnp.sum(dp * p, axis=0, keepdims=True)
                ds = (p * ((dp - delta) * 0.125)).astype(HALF)
                probs.append(p.astype(HALF))
                dscores.append(ds)
            dv = dot_nn(jnp.concatenate(probs, axis=1), jnp.concatenate([mask_half(d_o, 0), mask_half(d_o, 1)], axis=0))
            dk = dot_nn(jnp.concatenate(dscores, axis=1), jnp.concatenate([mask_half(q, 0), mask_half(q, 1)], axis=0))
            dq = dot_tn(jnp.concatenate(dscores, axis=0), jnp.concatenate([mask_half(k, 0), mask_half(k, 1)], axis=0))
            dqkv[rows, 128 * pr:128 * pr + 128] = dq.astype(HALF)
            dqkv[rows, DIM + 128 * pr:DIM + 128 * pr + 128] = dk.astype(HALF)
            dqkv[rows, 2 * DIM + 128 * pr:2 * DIM + 128 * pr + 128] = dv.astype(HALF)
    e_f = jnp.concatenate([e_ref[g] for g in range(GROUP)], axis=0).astype(WIDE)
    xhat, inv = normalize(e_f)
    h1 = (xhat * ln_scale[0:1].astype(WIDE) + ln_bias[0:1].astype(WIDE)).astype(HALF)
    dh1 = None
    for s in range(3):
        part = dqkv[:, DIM * s:DIM * s + DIM]
        tiny[s:s + 1] += col_sum(part.astype(WIDE))
        grad = dot_tn(part, h1)
        for k in range(TP):
            dwq[k, s] += grad[192 * k:192 * k + 192]
        term = dot_nn(part, jnp.concatenate([wq[k, s] for k in range(TP)], axis=0))
        dh1 = term if dh1 is None else dh1 + term
    dh1 = dh1.astype(HALF).astype(WIDE)
    dx1 = jnp.concatenate([dx1_ref[g] for g in range(GROUP)], axis=0).astype(WIDE)
    de = (dx1 + norm_back(dh1, xhat, inv, ln_scale[0:1].astype(WIDE))).astype(HALF)
    de_f = de.astype(WIDE)
    tiny[8:9] += col_sum(dh1 * xhat)
    tiny[9:10] += col_sum(dh1)
    acc = de_f[0:TOK]
    for g in range(1, GROUP):
        acc = acc + de_f[TOK * g:TOK * g + TOK]
    dpos[...] += acc
    x = jnp.concatenate([x_ref[g] for g in range(GROUP)], axis=0)
    dwp[...] += dot_tn(x, de)

    @pl.when(step == STEPS - 1)
    def _():
        tiny[4:8] = db1_ref[0:4]
        tiny[10:11] = col_sum(dpos[...])
        tiny[12:16] = dvec2_ref[0:4]
        chip = lax.div(me, 2)
        my_quarter = pl.ds(384 * core + 192 * chip, 192)
        far_quarter = pl.ds(384 * core + 192 * (1 - chip), 192)
        my_part = pl.ds(192 * chip, 192)
        other_half = pl.ds(384 * (1 - core), 384)
        my_half = pl.ds(384 * core, 384)
        near = [push(dwq.at[3], near_q.at[1], n_send.at[0], n_recv.at[0], others[1]), push(dwq.at[1], near_q.at[0], n_send.at[1], n_recv.at[1], others[1]), push(dpos.at[3 * PART:4 * PART], near_pos.at[1], n_send.at[2], n_recv.at[2], others[1]), push(dpos.at[PART:2 * PART], near_pos.at[0], n_send.at[3], n_recv.at[3], others[1]), push(dwp.at[other_half], near_p, n_send.at[4], n_recv.at[4], others[1])]
        tinies = [push(tiny, tiny_out.at[k - 1], t_send.at[k - 1], t_recv.at[k - 1], others[k]) for k in range(1, TP)]
        far = [push(dwq.at[2], far_q, f_send.at[0], f_recv.at[0], others[2]), push(dwp.at[far_quarter], far_p, f_send.at[1], f_recv.at[1], others[2]), push(dpos.at[2 * PART:3 * PART], far_pos, f_send.at[2], f_recv.at[2], others[2])]
        near[4].start()
        near[0].start()
        for c in near[1:4] + tinies:
            c.start()
        near[4].wait_recv()
        dwp[my_half] += near_p[...]
        far[1].start()
        near[0].wait_recv()
        for s in range(3):
            dwq[2, s] += near_q[1, s]
        far[0].start()
        near[2].wait_recv()
        dpos[2 * PART:3 * PART] += near_pos[1]
        far[2].start()
        near[1].wait_recv()
        near[3].wait_recv()
        far[1].wait()
        half_p[my_part] = (dwp[my_quarter] + far_p[...]).astype(HALF)
        spread = push(half_p.at[my_part], half_p.at[my_part], h_send.at[1], h_recv.at[1], others[2])
        spread.start()
        for c in pairs:
            c.wait()
        outs = []

        def total(keep_ref, near_ref, cross_ref, rows):
            copies = [pltpu.make_async_copy(r, sums.at[n, 0:rows], c_sem.at[n, 0]) for n, r in enumerate((keep_ref, near_ref, cross_ref))]
            for c in copies:
                c.start()
            for c in copies:
                c.wait()
            return (sums[0, 0:rows] + sums[1, 0:rows]) + sums[2, 0:rows]

        for n in range(3):
            rows = slice(256 * n, 256 * n + 256)
            total1[rows] = total(keep_a.at[rows], near_a.at[rows], cross_out.at[rows], 256).astype(HALF)
        outs.append(pltpu.make_async_copy(total1, dfc1_out, o_sem.at[0]))
        outs[0].start()
        for n in range(3):
            rows = slice(DIM + 256 * n, DIM + 256 * n + 256)
            part = total(keep_a.at[rows], near_a.at[rows], cross_out.at[rows], 256)
            total2[:, 256 * n:256 * n + 256] = part.T.astype(HALF)
        outs.append(pltpu.make_async_copy(total2, dfc2_out, o_sem.at[1]))
        outs[1].start()
        total3[...] = total(keep_o, near_o, cross_out.at[2 * DIM:PACK], 192).astype(HALF)
        outs.append(pltpu.make_async_copy(total3, dwo_out, o_sem.at[2]))
        outs[2].start()
        far[0].wait_recv()
        for s in range(3):
            half_q[s] = ((dwq[0, s] + near_q[0, s]) + far_q[s]).astype(HALF)
        q_copy = pltpu.make_async_copy(half_q, dqkv_out, local.at[0])
        q_copy.start()
        spread.wait()
        swap = push(half_p, dwp_out.at[my_half], h_send.at[0], h_recv.at[0], others[1])
        swap.start()
        p_copy = pltpu.make_async_copy(half_p, dwp_out.at[my_half], local.at[1])
        p_copy.start()
        far[2].wait_recv()
        half_pos[...] = ((dpos[0:PART] + near_pos[0]) + far_pos[...]).astype(HALF)
        pos_copy = pltpu.make_async_copy(half_pos, dpos_out, local.at[2])
        pos_copy.start()
        for c in near:
            c.wait_send()
        for c in tinies:
            c.wait()
        far[0].wait_send()
        far[2].wait_send()
        tiny_copy = pltpu.make_async_copy(tiny, tiny_out.at[3], local.at[3])
        tiny_copy.start()
        for c in outs:
            c.wait()
        q_copy.wait()
        p_copy.wait()
        pos_copy.wait()
        tiny_copy.wait()
        swap.wait()


def attn_bwd(keep_b, near_b, keep_a, near_a, keep_o, near_o, e, qkv, d_o, dx1, x, wq, ln_scale, ln_bias, dvec2, db1):
    dma = pltpu.SemaphoreType.DMA
    return pl.pallas_call(
        attn_bwd_kernel,
        grid=(STEPS,),
        in_specs=[any_spec()] * 6 + [image_spec(DIM), image_spec(3 * DIM), image_spec(DIM), image_spec(DIM), image_spec(DIM), fixed((TP, 3, 192, DIM)), vec_spec(2, DIM), vec_spec(2, DIM), vec_spec(8, DIM), vec_spec(8, DIM)],
        out_specs=[any_spec()] * 8,
        out_shape=[wide_shape(PACK, DIM), half_shape(DIM, DIM), half_shape(DIM, DIM), half_shape(192, DIM), half_shape(3, 192, DIM), half_shape(DIM, DIM), half_shape(PART, DIM), wide_shape(TP, 16, DIM)],
        scratch_shapes=[pltpu.VMEM((2, CHUNK, DIM), WIDE), pltpu.VMEM((2, CHUNK, DIM), WIDE), pltpu.VMEM((CHUNKS, CHUNK, DIM), WIDE), pltpu.VMEM((ROWS, 3 * DIM), HALF), pltpu.VMEM((TP, 3, 192, DIM), WIDE), pltpu.VMEM((DIM, DIM), WIDE), pltpu.VMEM((TOK, DIM), WIDE), pltpu.VMEM((16, DIM), WIDE), pltpu.VMEM((2, 3, 192, DIM), WIDE), pltpu.VMEM((384, DIM), WIDE), pltpu.VMEM((2, PART, DIM), WIDE), pltpu.VMEM((3, 192, DIM), WIDE), pltpu.VMEM((192, DIM), WIDE), pltpu.VMEM((PART, DIM), WIDE), pltpu.VMEM((3, 192, DIM), HALF), pltpu.VMEM((384, DIM), HALF), pltpu.VMEM((PART, DIM), HALF), dma((CHUNKS,)), dma((CHUNKS,)), dma((3,)), dma((3,)), dma((5,)), dma((5,)), dma((3,)), dma((3,)), dma((2,)), dma((2,)), dma((3, 2)), dma((3,)), pltpu.VMEM((DIM, DIM), HALF), pltpu.VMEM((DIM, DIM), HALF), pltpu.VMEM((192, DIM), HALF), dma((4,))],
        compiler_params=params(3),
        cost_estimate=pl.CostEstimate(flops=100_000_000_000, bytes_accessed=80_000_000, transcendentals=12_000_000),
        name='attn_bwd',
    )(keep_b, near_b, keep_a, near_a, keep_o, near_o, e, qkv, d_o, dx1, x, wq, ln_scale, ln_bias, dvec2, db1)


def finish_kernel(x2, fc1, fc2, wo, qkv, wp, pos, tiny, x2_out, fc1_out, fc2_out, wo_out, qkv_out, wp_out, pos_out, patch_b, ln_scale, ln_bias, qkv_b, out_b, fc1_b, fc2_b):
    for src, dst in ((x2, x2_out), (fc1, fc1_out), (fc2, fc2_out), (wo, wo_out), (qkv, qkv_out), (wp, wp_out), (pos, pos_out)):
        dst[...] = src[...]

    @pl.when(pl.program_id(0) == 0)
    def _():
        vec = ((tiny[3] + tiny[0]) + (tiny[1] + tiny[2])).astype(HALF)
        patch_b[...] = vec[10:11].reshape(DIM)
        ln_scale[0:1] = vec[8:9]
        ln_scale[1:2] = vec[12:13]
        ln_bias[0:1] = vec[9:10]
        ln_bias[1:2] = vec[13:14]
        fc2_b[...] = vec[14:15].reshape(DIM)
        out_b[...] = vec[15:16].reshape(DIM)
        fc1_b[...] = ((tiny[3, 4:5] + tiny[0, 5:6]) + (tiny[1, 6:7] + tiny[2, 7:8])).astype(HALF).reshape(DIM)
        for s in range(3):
            for h in range(3):
                at = [tiny[j, s:s + 1, 192 * k + 64 * h:192 * k + 64 * h + 64] for k, j in enumerate((3, 0, 1, 2))]
                qkv_b[s, h:h + 1] = ((at[0] + at[1]) + (at[2] + at[3])).astype(HALF)


def finish(x2, fc1, fc2, wo, qkv, wp, pos, tiny):
    arrays = (x2, fc1, fc2, wo, qkv, wp, pos)
    specs = [pl.BlockSpec((a.shape[0] // 4,) + a.shape[1:], lambda i, n=a.ndim: (i,) + (0,) * (n - 1)) for a in arrays]
    smalls = [(DIM,), (2, DIM), (2, DIM), (3, 3, 64), (DIM,), (DIM,), (DIM,)]
    return pl.pallas_call(
        finish_kernel,
        grid=(4,),
        in_specs=specs + [vec_spec(TP, 16, DIM)],
        out_specs=specs + [vec_spec(*shape) for shape in smalls],
        out_shape=[jax.ShapeDtypeStruct(a.shape, a.dtype) for a in arrays] + [half_shape(*shape) for shape in smalls],
        compiler_params=pltpu.CompilerParams(dimension_semantics=('arbitrary',), vmem_limit_bytes=67043328),
        name='finish',
    )(*arrays, tiny)


def group_step(patches, patch_w, patch_b, pos_emb, ln_scale, ln_bias, qkv_w, qkv_b, out_w, out_b, fc1_w, fc1_b, fc2_w, fc2_b, d_out):
    wq = qkv_w.transpose(0, 2, 3, 1).reshape(3, 192, DIM)
    wo = out_w.reshape(192, DIM)
    e, qkv, o, x1, x, dout, y, dh, wq_all, wop_all, bias_all, w1_far, w2_far, keep_a, give_a, part1, part2, dvec_n, db1_n = front(patches, d_out, wq, wo, pos_emb, fc1_w, fc2_w, patch_w, patch_b, qkv_b, fc1_b, out_b, ln_scale, ln_bias)
    x_two, dx1, d_o, near_a, keep_o, near_o, keep_b, near_b, dvec2, db1 = mlp_far(give_a, part1, part2, x1, o, dout, y, dh, w1_far, w2_far, wop_all, bias_all, ln_scale, ln_bias, fc2_b, dvec_n, db1_n)
    _, d_fc1_w, d_fc2_w, d_out_w, d_qkv, d_patch_w, d_pos, tiny = attn_bwd(keep_b, near_b, keep_a, near_a, keep_o, near_o, e, qkv, d_o, dx1, x, wq_all, ln_scale, ln_bias, dvec2, db1)
    x_two, d_fc1_w, d_fc2_w, d_out_w, d_qkv, d_patch_w, d_pos, d_patch_b, d_ln_scale, d_ln_bias, d_qkv_b, d_out_b, d_fc1_b, d_fc2_b = finish(x_two, d_fc1_w, d_fc2_w, d_out_w, d_qkv.reshape(576, DIM), d_patch_w, d_pos, tiny)
    d_qkv_w = d_qkv.reshape(3, 3, 64, DIM).transpose(0, 3, 1, 2)
    return (x_two, d_patch_w, d_patch_b, d_pos, d_ln_scale, d_ln_bias, d_qkv_w, d_qkv_b, d_out_w.reshape(3, 64, DIM), d_out_b, d_fc1_w, d_fc1_b, d_fc2_w, d_fc2_b)


def solution(mesh):
    in_specs = (P('dp', 'tp', None), P(), P(), P('tp', None), P(), P(), P(None, None, 'tp', None), P(None, 'tp', None), P('tp', None, None), P(), P(None, 'tp'), P('tp'), P('tp', None), P(), P('dp', 'tp', None))
    out_specs = (P('dp', 'tp', None), P('dp', None), P('dp'), P(('dp', 'tp'), None), P('dp', None), P('dp', None), P('dp', None, 'tp', None), P('dp', 'tp', None), P(('dp', 'tp'), None, None), P('dp'), P('dp', 'tp'), P(('dp', 'tp')), P(('dp', 'tp'), None), P('dp'))
    return jax.shard_map(group_step, mesh=mesh, in_specs=in_specs, out_specs=out_specs, check_vma=False)
```

```python
import functools
import jax
import jax.numpy as jnp
from jax import lax
from jax.experimental import pallas as pl
from jax.experimental.pallas import tpu as pltpu
from jax.sharding import PartitionSpec as P

LN_EPS = 1e-6
TP = 4
WIDE = jnp.float32
HALF = jnp.bfloat16
IMAGES = 16
TOK = 256
PART = 64
DIM = 768
GROUP = 1
ROWS = GROUP * TOK
STEPS = IMAGES // GROUP
FRONT = 2
FRONT_STEPS = IMAGES // FRONT
PAIRS = 6
EXP_SCALE = 0.125 * 1.4426950408889634
GELU_C = 0.7978845608028654
GELU_A = 0.044715
AHEAD = 6 // FRONT
PACK = 2 * DIM + 192
EARLY = 256
LATE = DIM - EARLY
CHUNKS = 6
CHUNK = PACK // CHUNKS


def dot_nn(a, b):
    return lax.dot_general(a, b, (((1,), (0,)), ((), ())), preferred_element_type=WIDE)


def dot_nt(a, b):
    return lax.dot_general(a, b, (((1,), (1,)), ((), ())), preferred_element_type=WIDE)


def dot_tn(a, b):
    return lax.dot_general(a, b, (((0,), (0,)), ((), ())), preferred_element_type=WIDE)


def normalize(x_f):
    mean = jnp.sum(x_f, axis=-1, keepdims=True) * (1.0 / DIM)
    centered = x_f - mean
    var = jnp.sum(centered * centered, axis=-1, keepdims=True) * (1.0 / DIM)
    inv = lax.rsqrt(var + LN_EPS)
    return centered * inv, inv


def norm_back(d_out_f, xhat, inv, scale):
    d_hat = d_out_f * scale
    m1 = jnp.sum(d_hat, axis=-1, keepdims=True) * (1.0 / DIM)
    m2 = jnp.sum(d_hat * xhat, axis=-1, keepdims=True) * (1.0 / DIM)
    return (d_hat - m1 - xhat * m2) * inv


def lane_half(j):
    lane = lax.broadcasted_iota(jnp.int32, (1, 128), 1)
    return (lane < 64) if j == 0 else (lane >= 64)


def mask_half(x, j):
    return jnp.where(lane_half(j), x, jnp.zeros_like(x))


def col_sum(x):
    return jnp.sum(x, axis=0, keepdims=True)


def row(ref):
    return ref[...].reshape(1, DIM).astype(WIDE)


def peers():
    me = lax.axis_index('tp')
    core = lax.rem(me, 2)
    chip = lax.div(me, 2)
    return me, core, (me, me + 1 - 2 * core, me + 2 - 4 * chip, 3 - me)


def meet(others):
    barrier = pltpu.get_barrier_semaphore()
    for k in range(1, TP):
        pl.semaphore_signal(barrier, inc=1, device_id={'tp': others[k]}, device_id_type=pl.DeviceIdType.MESH)
    pl.semaphore_wait(barrier, TP - 1)


def push(src, dst, send, recv, peer):
    return pltpu.make_async_remote_copy(src_ref=src, dst_ref=dst, send_sem=send, recv_sem=recv, device_id={'tp': peer}, device_id_type=pl.DeviceIdType.MESH)


def image_rows(owner, group, size):
    return pl.ds(owner * IMAGES + group * size, size)


def group_sends(src, buf, send, recv, others, group):
    return [push(src.at[image_rows(others[k], group, FRONT)], buf.at[k, pl.ds(group * FRONT, FRONT)], send.at[k - 1, group], recv.at[k - 1, group], others[k]) for k in (2, 3, 1)]


def slot_rows(buf, group):
    base = group * FRONT
    return jnp.concatenate([buf[k, base + g] for g in range(FRONT) for k in range(TP)], axis=0)


def mlp_slot(f, base, h2, dout, w1, w2, bias, y, dh2, dw1, dw2, db1_ref):
    hids = []
    dpres = []
    for c in range(w1.shape[1] // 256):
        cols = slice(256 * c, 256 * c + 256)
        units = slice(base + 256 * c, base + 256 * c + 256)
        pre = dot_nn(h2, w1[:, cols]) + bias[f, 3:4, units].astype(WIDE)
        sq = pre * pre
        t = jnp.tanh(pre * (GELU_C + (GELU_C * GELU_A) * sq))
        half_pre = 0.5 * pre
        hids.append((half_pre + half_pre * t).astype(HALF))
        slope = (0.5 + 0.5 * t) + (half_pre * (1.0 - t * t)) * (GELU_C + (3.0 * GELU_C * GELU_A) * sq)
        dpre = dot_nt(dout, w2[cols]).astype(HALF).astype(WIDE) * slope
        db1_ref[f:f + 1, units] += col_sum(dpre)
        dpres.append(dpre.astype(HALF))
    hid = jnp.concatenate(hids, axis=1)
    dpre_h = jnp.concatenate(dpres, axis=1)
    part_y = dot_nn(hid, w2)
    part_h = dot_nt(dpre_h, w1)
    y = part_y if y is None else y + part_y
    dh2 = part_h if dh2 is None else dh2 + part_h

    def grads():
        dw1[...] += dot_tn(h2, dpre_h)
        dw2[...] += dot_tn(dout, hid)

    return y, dh2, grads


def front_kernel(patches, d_out, wq_own, wo_own, pos_own, w1_own, w2_own, wp, patch_b, qkv_b, fc1_b, out_b, ln_scale, ln_bias, e_ref, qkv_ref, o_ref, x1_ref, x_ref, lse_ref, dout_ref, y_ref, dh_ref, wq_out, wop_out, bias_out, w1_far, w2_far, keep_out, give_out, part1_out, part2_out, dvec_ref, db1_ref, xbuf, dbuf, wq, wop, w1, w2, wa1, wa2, bias, bias_own, bqkv, dw1, dw2, dwa1, dwa2, x_send, x_recv, d_send, d_recv, w_send, w_recv, local, done):
    step = pl.program_id(0)
    me, core, others = peers()
    small = []
    for n, (src, cut) in enumerate(((wq_own, None), (wo_own, (0, 192)), (pos_own, (192, 256)))):
        at = [wq.at[k] if cut is None else wop.at[k, cut[0]:cut[1]] for k in range(TP)]
        small.append((push(src, at[2], w_send.at[n, 1], w_recv.at[n, 1], others[2]), push(src, at[1], w_send.at[n, 0], w_recv.at[n, 0], others[1]), push(at[2], at[3], w_send.at[n, 2], w_recv.at[n, 2], others[1])))
    near = [push(w1_own, w1.at[1], w_send.at[3, 0], w_recv.at[3, 0], others[1]), push(w2_own, w2.at[1], w_send.at[4, 0], w_recv.at[4, 0], others[1])]
    early = [push(w1_own.at[:, 0:EARLY], wa1.at[0], w_send.at[6, 0], w_recv.at[6, 0], others[2]), push(w2_own.at[0:EARLY], wa2.at[0], w_send.at[7, 0], w_recv.at[7, 0], others[2])]
    early_relay = [push(wa1.at[0], wa1.at[1], w_send.at[6, 1], w_recv.at[6, 1], others[1]), push(wa2.at[0], wa2.at[1], w_send.at[7, 1], w_recv.at[7, 1], others[1])]
    far = [push(w1_own.at[:, EARLY:DIM], w1_far.at[0], w_send.at[3, 1], w_recv.at[3, 1], others[2]), push(w2_own.at[EARLY:DIM - 256], w2_far.at[0, 0:256], w_send.at[4, 1], w_recv.at[4, 1], others[2]), push(w2_own.at[DIM - 256:DIM], w2_far.at[0, 256:512], w_send.at[8, 0], w_recv.at[8, 0], others[2])]
    relay = [push(w1_far.at[0], w1_far.at[1], w_send.at[3, 2], w_recv.at[3, 2], others[1]), push(w2_far.at[0, 0:256], w2_far.at[1, 0:256], w_send.at[4, 2], w_recv.at[4, 2], others[1]), push(w2_far.at[0, 256:512], w2_far.at[1, 256:512], w_send.at[8, 1], w_recv.at[8, 1], others[1])]
    biases = [push(bias_own, bias.at[k], w_send.at[5, k - 1], w_recv.at[5, k - 1], others[k]) for k in range(1, TP)]
    own = [pltpu.make_async_copy(wq_own, wq.at[0], local.at[0]), pltpu.make_async_copy(wo_own, wop.at[0, 0:192], local.at[1]), pltpu.make_async_copy(pos_own, wop.at[0, 192:256], local.at[2]), pltpu.make_async_copy(patches.at[pl.ds(me * IMAGES, IMAGES)], xbuf.at[0], local.at[3]), pltpu.make_async_copy(d_out.at[pl.ds(me * IMAGES, IMAGES)], dbuf.at[0], local.at[7]), pltpu.make_async_copy(w1_own, w1.at[0], local.at[8]), pltpu.make_async_copy(w2_own, w2.at[0], local.at[9])]
    flush = [pltpu.make_async_copy(wq, wq_out, local.at[4]), pltpu.make_async_copy(wop, wop_out, local.at[5]), pltpu.make_async_copy(bias, bias_out, local.at[6])]

    def arrivals(group):
        return group_sends(patches, xbuf, x_send, x_recv, others, group) + group_sends(d_out, dbuf, d_send, d_recv, others, group)

    @pl.when(step == 0)
    def _():
        bias_own[...] = jnp.zeros_like(bias_own)
        for s in range(3):
            for h in range(3):
                bias_own[s:s + 1, 64 * h:64 * h + 64] = qkv_b[s, h:h + 1]
        bias_own[3:4] = fc1_b[...].reshape(1, DIM)
        bias[0] = bias_own[...]
        meet(others)
        for n in range(3):
            small[n][0].start()
        for c in biases:
            c.start()
        for n in range(3):
            small[n][1].start()
        for g in range(AHEAD):
            for c in arrivals(g) + (early if g == 0 else []):
                c.start()
        for c in own + near:
            c.start()
        dw1[...] = jnp.zeros_like(dw1)
        dw2[...] = jnp.zeros_like(dw2)
        dwa1[...] = jnp.zeros_like(dwa1)
        dwa2[...] = jnp.zeros_like(dwa2)
        dvec_ref[...] = jnp.zeros_like(dvec_ref)
        db1_ref[...] = jnp.zeros_like(db1_ref)
        for n in range(3):
            small[n][0].wait_recv()
            small[n][2].start()
        for c in own:
            c.wait()
        for n in range(3):
            small[n][1].wait_recv()
            small[n][2].wait_recv()
        for c in biases + near:
            c.wait_recv()
        for s in range(3):
            for k in range(TP):
                bqkv[s:s + 1, 192 * k:192 * k + 192] = bias[k, s:s + 1, 0:192].astype(WIDE)
        for c in flush:
            c.start()

    @pl.when(step + AHEAD < FRONT_STEPS)
    def _():
        for c in arrivals(step + AHEAD):
            c.start()

    @pl.when(step == FRONT_STEPS - AHEAD)
    def _():
        for c in far:
            c.start()

    for c in group_sends(patches, xbuf, x_send, x_recv, others, step):
        c.wait_recv()
    x = slot_rows(xbuf, step)
    posb = jnp.concatenate([wop[k, 192:192 + PART] for k in range(TP)], axis=0).astype(WIDE) + row(patch_b)
    emb = dot_nn(x, wp[...]) + jnp.concatenate([posb] * FRONT, axis=0)
    e_h = emb.astype(HALF)
    for g in range(FRONT):
        x_ref[g] = x[TOK * g:TOK * g + TOK]
        e_ref[g] = e_h[TOK * g:TOK * g + TOK]
    e_f = e_h.astype(WIDE)
    xhat, _ = normalize(e_f)
    h1 = (xhat * ln_scale[0:1].astype(WIDE) + ln_bias[0:1].astype(WIDE)).astype(HALF)
    for s in range(3):
        part = (dot_nt(h1, jnp.concatenate([wq[k, s] for k in range(TP)], axis=0)) + bqkv[s:s + 1]).astype(HALF)
        for g in range(FRONT):
            qkv_ref[g, :, DIM * s:DIM * s + DIM] = part[TOK * g:TOK * g + TOK]
    for g in range(FRONT):
        for pr in range(PAIRS):
            q = qkv_ref[g, :, 128 * pr:128 * pr + 128]
            k = qkv_ref[g, :, DIM + 128 * pr:DIM + 128 * pr + 128]
            v = qkv_ref[g, :, 2 * DIM + 128 * pr:2 * DIM + 128 * pr + 128]
            probs = []
            for j in range(2):
                s = dot_nt(k, mask_half(q, j))
                m = jnp.max(s, axis=0, keepdims=True)
                e = jnp.exp2((s - m) * EXP_SCALE)
                l = jnp.sum(e, axis=0, keepdims=True)
                lse_ref[g, 2 * pr + j:2 * pr + j + 1] = m * EXP_SCALE + jnp.log2(l)
                probs.append((e * (1.0 / l)).astype(HALF))
            pv = dot_tn(jnp.concatenate(probs, axis=0), jnp.concatenate([mask_half(v, 0), mask_half(v, 1)], axis=0))
            o_ref[g, :, 128 * pr:128 * pr + 128] = pv.astype(HALF)
    o = jnp.concatenate([o_ref[g] for g in range(FRONT)], axis=0)
    e_f = jnp.concatenate([e_ref[g] for g in range(FRONT)], axis=0).astype(WIDE)
    x1 = (e_f + (dot_nn(o, jnp.concatenate([wop[k, 0:192] for k in range(TP)], axis=0)) + row(out_b))).astype(HALF)
    for g in range(FRONT):
        x1_ref[g] = x1[TOK * g:TOK * g + TOK]

    xhat, _ = normalize(x1.astype(WIDE))
    h2 = (xhat * ln_scale[1:2].astype(WIDE) + ln_bias[1:2].astype(WIDE)).astype(HALF)
    for c in group_sends(d_out, dbuf, d_send, d_recv, others, step):
        c.wait_recv()
    dout = slot_rows(dbuf, step)
    dvec_ref[2:3] += col_sum(dout.astype(WIDE))
    y = None
    dh2 = None
    for f in range(2):
        y, dh2, grads = mlp_slot(f, 0, h2, dout, w1[f], w2[f], bias, y, dh2, dw1.at[f], dw2.at[f], db1_ref)
        grads()

    @pl.when(step == 0)
    def _():
        for n in range(2):
            early[n].wait_recv()
            early_relay[n].start()
        for c in early_relay:
            c.wait_recv()

    for f in range(2):
        y, dh2, grads = mlp_slot(f + 2, 0, h2, dout, wa1[f], wa2[f], bias, y, dh2, dwa1.at[f], dwa2.at[f], db1_ref)
        grads()
    for g in range(FRONT):
        rows = slice(TOK * g, TOK * g + TOK)
        dout_ref[g] = dout[rows]
        y_ref[g] = y[rows]
        dh_ref[g] = dh2[rows]

    @pl.when(step == FRONT_STEPS - 1)
    def _():
        copies = []
        for n, out in enumerate((keep_out, give_out)):
            copies.append(pltpu.make_async_copy(dw1.at[n], out.at[0:DIM], done.at[2 * n]))
            copies.append(pltpu.make_async_copy(dw2.at[n], out.at[DIM:2 * DIM], done.at[2 * n + 1]))
        copies.append(pltpu.make_async_copy(dwa1, part1_out, done.at[4]))
        copies.append(pltpu.make_async_copy(dwa2, part2_out, done.at[5]))
        for c in copies:
            c.start()
        for n in range(3):
            far[n].wait_recv()
            relay[n].start()
        for c in relay:
            c.wait_recv()
        for c in small[0] + small[1] + small[2] + tuple(near + early + early_relay + far + relay + biases):
            c.wait_send()
        for c in copies + flush:
            c.wait()
        for g in range(FRONT_STEPS):
            for c in arrivals(g):
                c.wait_send()


def fixed(shape):
    return pl.BlockSpec(shape, lambda i: (0,) * len(shape), pipeline_mode=pl.Buffered(1))


def image_spec(width, size=GROUP):
    return pl.BlockSpec((size, TOK, width), lambda i: (i, 0, 0))


def lse_spec(size=GROUP):
    return pl.BlockSpec((size, 16, TOK), lambda i: (i, 0, 0))


def any_spec():
    return pl.BlockSpec(memory_space=pl.ANY)


def params(cid):
    return pltpu.CompilerParams(dimension_semantics=('arbitrary',), vmem_limit_bytes=67043328, collective_id=cid, has_side_effects=True)


def image_shape(width):
    return jax.ShapeDtypeStruct((IMAGES, TOK, width), HALF)


def half_shape(*shape):
    return jax.ShapeDtypeStruct(shape, HALF)


def wide_shape(*shape):
    return jax.ShapeDtypeStruct(shape, WIDE)


def vec_spec(*shape):
    return pl.BlockSpec(shape, lambda i: (0,) * len(shape))


def front(patches, d_out, wq, wo, pos, w1, w2, wp, patch_b, qkv_b, fc1_b, out_b, ln_scale, ln_bias):
    dma = pltpu.SemaphoreType.DMA
    wide_image = jax.ShapeDtypeStruct((IMAGES, TOK, DIM), WIDE)
    return pl.pallas_call(
        front_kernel,
        grid=(FRONT_STEPS,),
        in_specs=[any_spec()] * 7 + [fixed((DIM, DIM)), vec_spec(DIM), vec_spec(3, 3, 64), vec_spec(DIM), vec_spec(DIM), vec_spec(2, DIM), vec_spec(2, DIM)],
        out_specs=[image_spec(DIM, FRONT), image_spec(3 * DIM, FRONT)] + [image_spec(DIM, FRONT)] * 3 + [lse_spec(FRONT)] + [image_spec(DIM, FRONT)] * 3 + [any_spec()] * 9 + [vec_spec(8, DIM), vec_spec(8, DIM)],
        out_shape=[image_shape(DIM), image_shape(3 * DIM), image_shape(DIM), image_shape(DIM), image_shape(DIM), wide_shape(IMAGES, 16, TOK), image_shape(DIM), wide_image, wide_image, half_shape(TP, 3, 192, DIM), half_shape(TP, 256, DIM), half_shape(TP, 16, DIM), half_shape(2, DIM, LATE), half_shape(2, LATE, DIM), wide_shape(2 * DIM, DIM), wide_shape(2 * DIM, DIM), wide_shape(2, DIM, EARLY), wide_shape(2, DIM, EARLY), wide_shape(8, DIM), wide_shape(8, DIM)],
        scratch_shapes=[pltpu.VMEM((TP, IMAGES, PART, DIM), HALF), pltpu.VMEM((TP, IMAGES, PART, DIM), HALF), pltpu.VMEM((TP, 3, 192, DIM), HALF), pltpu.VMEM((TP, 256, DIM), HALF), pltpu.VMEM((2, DIM, DIM), HALF), pltpu.VMEM((2, DIM, DIM), HALF), pltpu.VMEM((2, DIM, EARLY), HALF), pltpu.VMEM((2, EARLY, DIM), HALF), pltpu.VMEM((TP, 16, DIM), HALF), pltpu.VMEM((16, DIM), HALF), pltpu.VMEM((8, DIM), WIDE), pltpu.VMEM((2, DIM, DIM), WIDE), pltpu.VMEM((2, DIM, DIM), WIDE), pltpu.VMEM((2, DIM, EARLY), WIDE), pltpu.VMEM((2, DIM, EARLY), WIDE), dma((3, FRONT_STEPS)), dma((3, FRONT_STEPS)), dma((3, FRONT_STEPS)), dma((3, FRONT_STEPS)), dma((9, 3)), dma((9, 3)), dma((10,)), dma((6,))],
        compiler_params=params(0),
        cost_estimate=pl.CostEstimate(flops=120_000_000_000, bytes_accessed=120_000_000, transcendentals=18_000_000),
        name='front',
    )(patches, d_out, wq, wo, pos, w1, w2, wp, patch_b, qkv_b, fc1_b, out_b, ln_scale, ln_bias)


def mlp_far_kernel(give, part1, part2, x1_ref, o_ref, dout_ref, y_ref, dh_ref, w1_far, w2_far, bias, ln_scale, ln_bias, fc2_b, dvec_near, db1_near, x2_out, dx1_ref, near_a, keep_o, near_o, keep_b, near_b, dvec_ref, db1_ref, ybuf, stage, dw1, dw2, dwo, y_send, y_recv, y_own, g_send, g_recv, local):
    step = pl.program_id(0)
    me, core, others = peers()
    slot = lax.rem(step, 2)

    def y_sends(at, group):
        return [push(ybuf.at[at, k], x2_out.at[image_rows(me, group, GROUP)], y_send.at[k - 1, at], y_recv.at[k - 1, group], others[k]) for k in (2, 3, 1)]

    def y_keep(at, group):
        return pltpu.make_async_copy(ybuf.at[at, 0], x2_out.at[image_rows(me, group, GROUP)], y_own.at[at])

    def y_wait(at, group):
        for c in y_sends(at, group):
            c.wait_send()
        y_keep(at, group).wait()

    early = [push(give, near_a, g_send.at[0], g_recv.at[0], others[1]), push(part1.at[1], near_b.at[0:DIM, 0:EARLY], g_send.at[5], g_recv.at[5], others[1]), push(part2.at[1], near_b.at[DIM:2 * DIM, 0:EARLY], g_send.at[6], g_recv.at[6], others[1])]
    grads = [push(dw1.at[1], near_b.at[0:DIM, EARLY:DIM], g_send.at[1], g_recv.at[1], others[1]), push(dw2.at[1], near_b.at[DIM:2 * DIM, EARLY:DIM], g_send.at[2], g_recv.at[2], others[1]), push(dwo.at[576:768], near_b.at[2 * DIM:PACK], g_send.at[3], g_recv.at[3], others[1]), push(dwo.at[192:384], near_o, g_send.at[4], g_recv.at[4], others[1])]
    keeps = [pltpu.make_async_copy(dw1.at[0], keep_b.at[0:DIM, EARLY:DIM], local.at[0]), pltpu.make_async_copy(dw2.at[0], keep_b.at[DIM:2 * DIM, EARLY:DIM], local.at[1]), pltpu.make_async_copy(dwo.at[384:576], keep_b.at[2 * DIM:PACK], local.at[2]), pltpu.make_async_copy(dwo.at[0:192], keep_o, local.at[3])]
    moves = [pltpu.make_async_copy(stage.at[0], keep_b.at[0:DIM, 0:EARLY], local.at[6]), pltpu.make_async_copy(stage.at[1], keep_b.at[DIM:2 * DIM, 0:EARLY], local.at[7])]

    @pl.when(step == 0)
    def _():
        meet(others)
        for c in early:
            c.start()
        loads = [pltpu.make_async_copy(part1.at[0], stage.at[0], local.at[4]), pltpu.make_async_copy(part2.at[0], stage.at[1], local.at[5])]
        for c in loads:
            c.start()
        dw1[...] = jnp.zeros_like(dw1)
        dw2[...] = jnp.zeros_like(dw2)
        for c in loads:
            c.wait()
        for c in moves:
            c.start()
        dwo[...] = jnp.zeros_like(dwo)
        dvec_ref[...] = dvec_near[...]
        db1_ref[...] = db1_near[...]

    x1 = jnp.concatenate([x1_ref[g] for g in range(GROUP)], axis=0)
    dout = jnp.concatenate([dout_ref[g] for g in range(GROUP)], axis=0)
    xhat, inv = normalize(x1.astype(WIDE))
    h2 = (xhat * ln_scale[1:2].astype(WIDE) + ln_bias[1:2].astype(WIDE)).astype(HALF)
    y = jnp.concatenate([y_ref[g] for g in range(GROUP)], axis=0)
    dh2 = jnp.concatenate([dh_ref[g] for g in range(GROUP)], axis=0)
    weight_grads = []
    for f in range(2):
        y, dh2, late = mlp_slot(f + 2, EARLY, h2, dout, w1_far[f], w2_far[f], bias, y, dh2, dw1.at[f], dw2.at[f], db1_ref)
        weight_grads.append(late)
    x2 = (x1.astype(WIDE) + (y + row(fc2_b))).astype(HALF)

    @pl.when(step >= 2)
    def _():
        y_wait(slot, step - 2)

    for g in range(GROUP):
        for k in range(TP):
            ybuf[slot, k, g] = x2[TOK * g + PART * k:TOK * g + PART * k + PART]
    weight_grads[1]()

    for c in y_sends(slot, step):
        c.start()
    y_keep(slot, step).start()

    @pl.when(step == STEPS - 1)
    def _():
        grads[0].start()
        grads[1].start()

    weight_grads[0]()
    dh2 = dh2.astype(HALF).astype(WIDE)
    xhat, inv = normalize(x1.astype(WIDE))
    dout_f = dout.astype(WIDE)
    dx1 = (dout_f + norm_back(dh2, xhat, inv, ln_scale[1:2].astype(WIDE))).astype(HALF)
    dvec_ref[0:1] += col_sum(dh2 * xhat)
    dvec_ref[1:2] += col_sum(dh2)
    dvec_ref[3:4] += col_sum(dx1.astype(WIDE))
    for g in range(GROUP):
        dx1_ref[g] = dx1[TOK * g:TOK * g + TOK]
    o = jnp.concatenate([o_ref[g] for g in range(GROUP)], axis=0)
    dwo[...] += dot_tn(o, dx1)


    @pl.when(step == STEPS - 1)
    def _():
        for c in grads[2:] + keeps:
            c.start()
        for c in keeps + moves:
            c.wait()
        for c in early + grads:
            c.wait()
        for g in range(STEPS):
            for c in y_sends(g % 2, g):
                c.wait_recv()
        for g in (STEPS - 2, STEPS - 1):
            y_wait(g % 2, g)


def mlp_far(give, part1, part2, x1, o, dout, y, dh, w1_far, w2_far, bias, ln_scale, ln_bias, fc2_b, dvec_near, db1_near):
    dma = pltpu.SemaphoreType.DMA
    return pl.pallas_call(
        mlp_far_kernel,
        grid=(STEPS,),
        in_specs=[any_spec()] * 3 + [image_spec(DIM)] * 5 + [fixed((2, DIM, LATE)), fixed((2, LATE, DIM)), fixed((TP, 16, DIM)), vec_spec(2, DIM), vec_spec(2, DIM), vec_spec(DIM), vec_spec(8, DIM), vec_spec(8, DIM)],
        out_specs=[any_spec(), image_spec(DIM)] + [any_spec()] * 5 + [vec_spec(8, DIM), vec_spec(8, DIM)],
        out_shape=[half_shape(TP * IMAGES, PART, DIM), image_shape(DIM), wide_shape(2 * DIM, DIM), wide_shape(192, DIM), wide_shape(192, DIM), wide_shape(PACK, DIM), wide_shape(PACK, DIM), wide_shape(8, DIM), wide_shape(8, DIM)],
        scratch_shapes=[pltpu.VMEM((2, TP, GROUP, PART, DIM), HALF), pltpu.VMEM((2, DIM, EARLY), WIDE), pltpu.VMEM((2, DIM, LATE), WIDE), pltpu.VMEM((2, DIM, LATE), WIDE), pltpu.VMEM((DIM, DIM), WIDE), dma((3, 2)), dma((3, STEPS)), dma((2,)), dma((7,)), dma((7,)), dma((8,))],
        compiler_params=params(2),
        cost_estimate=pl.CostEstimate(flops=70_000_000_000, bytes_accessed=80_000_000, transcendentals=6_000_000),
        name='mlp_far',
    )(give, part1, part2, x1, o, dout, y, dh, w1_far, w2_far, bias, ln_scale, ln_bias, fc2_b, dvec_near, db1_near)


def attn_bwd_kernel(keep_b, near_b, keep_a, near_a, keep_o, near_o, e_ref, qkv_ref, lse_ref, dx1_ref, x_ref, wq_all, wop, ln_scale, ln_bias, dvec2_ref, db1_ref, cross_out, dfc1_out, dfc2_out, dwo_out, dqkv_out, dwp_out, dpos_out, tiny_out, fetch_k, fetch_n, sums, do_buf, wq, dqkv, dwq, dwp, dpos, tiny, near_q, near_p, near_pos, far_q, far_p, far_pos, half_q, half_p, half_pos, p_send, p_recv, t_send, t_recv, n_send, n_recv, f_send, f_recv, h_send, h_recv, c_sem, o_sem, total1, total2, total3, fq_send, fq_recv, local):
    step = pl.program_id(0)
    me, core, others = peers()
    pairs = [push(sums.at[n], cross_out.at[CHUNK * n:CHUNK * n + CHUNK], p_send.at[n], p_recv.at[n], others[2]) for n in range(CHUNKS)]

    def fetch(n):
        rows = pl.ds(n * CHUNK, CHUNK)
        at = lax.rem(n, 2)
        return (pltpu.make_async_copy(keep_b.at[rows], fetch_k.at[at], c_sem.at[0, at]), pltpu.make_async_copy(near_b.at[rows], fetch_n.at[at], c_sem.at[1, at]))

    @pl.when(step == 0)
    def _():
        meet(others)
        for c in fetch(0):
            c.start()

    @pl.when(step < CHUNKS)
    def _():
        @pl.when(step + 1 < CHUNKS)
        def _():
            for c in fetch(step + 1):
                c.start()
        for c in fetch(step):
            c.wait()
        at = lax.rem(step, 2)
        sums[step] = fetch_k[at] + fetch_n[at]

    @pl.when(step == 0)
    def _():
        dwq[...] = jnp.zeros_like(dwq)
        dwp[...] = jnp.zeros_like(dwp)
        dpos[...] = jnp.zeros_like(dpos)
        tiny[...] = jnp.zeros_like(tiny)

    @pl.when(step < CHUNKS)
    def _():
        push(sums.at[step], cross_out.at[pl.ds(step * CHUNK, CHUNK)], p_send.at[step], p_recv.at[step], others[2]).start()

    @pl.when(step == 0)
    def _():
        wq_copy = pltpu.make_async_copy(wq_all, wq, local.at[4])
        wq_copy.start()
        wq_copy.wait()

    wo = jnp.concatenate([wop[k, 0:192] for k in range(TP)], axis=0)
    for g in range(GROUP):
        do_buf[g] = dot_nt(dx1_ref[g], wo).astype(HALF)
    for g in range(GROUP):
        rows = slice(TOK * g, TOK * g + TOK)
        for pr in range(PAIRS):
            cols = slice(128 * pr, 128 * pr + 128)
            q = qkv_ref[g, :, 128 * pr:128 * pr + 128]
            k = qkv_ref[g, :, DIM + 128 * pr:DIM + 128 * pr + 128]
            v = qkv_ref[g, :, 2 * DIM + 128 * pr:2 * DIM + 128 * pr + 128]
            d_o = do_buf[g, :, 128 * pr:128 * pr + 128]
            probs = []
            dscores = []
            for j in range(2):
                s = dot_nt(k, mask_half(q, j))
                p = jnp.exp2(s * EXP_SCALE - lse_ref[g, 2 * pr + j:2 * pr + j + 1])
                dp = dot_nt(v, mask_half(d_o, j)).astype(HALF).astype(WIDE)
                delta = jnp.sum(dp * p, axis=0, keepdims=True)
                ds = (p * ((dp - delta) * 0.125)).astype(HALF)
                probs.append(p.astype(HALF))
                dscores.append(ds)
            dv = dot_nn(jnp.concatenate(probs, axis=1), jnp.concatenate([mask_half(d_o, 0), mask_half(d_o, 1)], axis=0))
            dk = dot_nn(jnp.concatenate(dscores, axis=1), jnp.concatenate([mask_half(q, 0), mask_half(q, 1)], axis=0))
            dq = dot_tn(jnp.concatenate(dscores, axis=0), jnp.concatenate([mask_half(k, 0), mask_half(k, 1)], axis=0))
            dqkv[rows, 128 * pr:128 * pr + 128] = dq.astype(HALF)
            dqkv[rows, DIM + 128 * pr:DIM + 128 * pr + 128] = dk.astype(HALF)
            dqkv[rows, 2 * DIM + 128 * pr:2 * DIM + 128 * pr + 128] = dv.astype(HALF)
    e_f = jnp.concatenate([e_ref[g] for g in range(GROUP)], axis=0).astype(WIDE)
    xhat, inv = normalize(e_f)
    h1 = (xhat * ln_scale[0:1].astype(WIDE) + ln_bias[0:1].astype(WIDE)).astype(HALF)
    dh1 = None
    for s in range(3):
        part = dqkv[:, DIM * s:DIM * s + DIM]
        tiny[s:s + 1] += col_sum(part.astype(WIDE))
        grad = dot_tn(part, h1)
        for k in range(TP):
            dwq[k, s] += grad[192 * k:192 * k + 192]
        term = dot_nn(part, jnp.concatenate([wq[k, s] for k in range(TP)], axis=0))
        dh1 = term if dh1 is None else dh1 + term
    dh1 = dh1.astype(HALF).astype(WIDE)
    dx1 = jnp.concatenate([dx1_ref[g] for g in range(GROUP)], axis=0).astype(WIDE)
    de = (dx1 + norm_back(dh1, xhat, inv, ln_scale[0:1].astype(WIDE))).astype(HALF)
    de_f = de.astype(WIDE)
    tiny[8:9] += col_sum(dh1 * xhat)
    tiny[9:10] += col_sum(dh1)
    acc = de_f[0:TOK]
    for g in range(1, GROUP):
        acc = acc + de_f[TOK * g:TOK * g + TOK]
    dpos[...] += acc
    x = jnp.concatenate([x_ref[g] for g in range(GROUP)], axis=0)
    dwp[...] += dot_tn(x, de)

    @pl.when(step == STEPS - 1)
    def _():
        tiny[4:8] = db1_ref[0:4]
        tiny[10:11] = col_sum(dpos[...])
        tiny[12:16] = dvec2_ref[0:4]
        chip = lax.div(me, 2)
        my_quarter = pl.ds(384 * core + 192 * chip, 192)
        far_quarter = pl.ds(384 * core + 192 * (1 - chip), 192)
        my_part = pl.ds(192 * chip, 192)
        other_half = pl.ds(384 * (1 - core), 384)
        my_half = pl.ds(384 * core, 384)
        near = [push(dwq.at[3], near_q.at[1], n_send.at[0], n_recv.at[0], others[1]), push(dwq.at[1], near_q.at[0], n_send.at[1], n_recv.at[1], others[1]), push(dpos.at[3 * PART:4 * PART], near_pos.at[1], n_send.at[2], n_recv.at[2], others[1]), push(dpos.at[PART:2 * PART], near_pos.at[0], n_send.at[3], n_recv.at[3], others[1]), push(dwp.at[other_half], near_p, n_send.at[4], n_recv.at[4], others[1])]
        tinies = [push(tiny, tiny_out.at[k - 1], t_send.at[k - 1], t_recv.at[k - 1], others[k]) for k in range(1, TP)]
        far = [None, push(dwp.at[far_quarter], far_p, f_send.at[1], f_recv.at[1], others[2]), push(dpos.at[2 * PART:3 * PART], far_pos, f_send.at[2], f_recv.at[2], others[2])]
        far_qs = [push(dwq.at[2, s], far_q.at[s], fq_send.at[s], fq_recv.at[s], others[2]) for s in range(3)]
        near[4].start()
        near[0].start()
        for c in near[1:4] + tinies:
            c.start()
        near[4].wait_recv()
        dwp[my_half] += near_p[...]
        far[1].start()
        near[0].wait_recv()
        for s in range(3):
            dwq[2, s] += near_q[1, s]
        for c in far_qs:
            c.start()
        near[2].wait_recv()
        dpos[2 * PART:3 * PART] += near_pos[1]
        far[2].start()
        near[1].wait_recv()
        near[3].wait_recv()
        far[1].wait()
        half_p[my_part] = (dwp[my_quarter] + far_p[...]).astype(HALF)
        spread = push(half_p.at[my_part], half_p.at[my_part], h_send.at[1], h_recv.at[1], others[2])
        spread.start()
        for c in pairs:
            c.wait()
        outs = []

        def total(keep_ref, near_ref, cross_ref, rows):
            copies = [pltpu.make_async_copy(r, sums.at[n, 0:rows], c_sem.at[n, 0]) for n, r in enumerate((keep_ref, near_ref, cross_ref))]
            for c in copies:
                c.start()
            for c in copies:
                c.wait()
            return (sums[0, 0:rows] + sums[1, 0:rows]) + sums[2, 0:rows]

        for n in range(3):
            rows = slice(256 * n, 256 * n + 256)
            total1[rows] = total(keep_a.at[rows], near_a.at[rows], cross_out.at[rows], 256).astype(HALF)
        outs.append(pltpu.make_async_copy(total1, dfc1_out, o_sem.at[0]))
        outs[0].start()
        for n in range(3):
            rows = slice(DIM + 256 * n, DIM + 256 * n + 256)
            part = total(keep_a.at[rows], near_a.at[rows], cross_out.at[rows], 256)
            total2[:, 256 * n:256 * n + 256] = part.T.astype(HALF)
        outs.append(pltpu.make_async_copy(total2, dfc2_out, o_sem.at[1]))
        outs[1].start()
        total3[...] = total(keep_o, near_o, cross_out.at[2 * DIM:PACK], 192).astype(HALF)
        outs.append(pltpu.make_async_copy(total3, dwo_out, o_sem.at[2]))
        outs[2].start()
        for s in range(3):
            far_qs[s].wait_recv()
            half_q[s] = ((dwq[0, s] + near_q[0, s]) + far_q[s]).astype(HALF)
        q_copy = pltpu.make_async_copy(half_q, dqkv_out, local.at[0])
        q_copy.start()
        spread.wait()
        swap = push(half_p, dwp_out.at[my_half], h_send.at[0], h_recv.at[0], others[1])
        swap.start()
        p_copy = pltpu.make_async_copy(half_p, dwp_out.at[my_half], local.at[1])
        p_copy.start()
        far[2].wait_recv()
        half_pos[...] = ((dpos[0:PART] + near_pos[0]) + far_pos[...]).astype(HALF)
        pos_copy = pltpu.make_async_copy(half_pos, dpos_out, local.at[2])
        pos_copy.start()
        for c in near:
            c.wait_send()
        for c in tinies:
            c.wait()
        for c in far_qs:
            c.wait_send()
        far[2].wait_send()
        tiny_copy = pltpu.make_async_copy(tiny, tiny_out.at[3], local.at[3])
        tiny_copy.start()
        for c in outs:
            c.wait()
        q_copy.wait()
        p_copy.wait()
        pos_copy.wait()
        tiny_copy.wait()
        swap.wait()


def attn_bwd(keep_b, near_b, keep_a, near_a, keep_o, near_o, e, qkv, lse, dx1, x, wq, wop, ln_scale, ln_bias, dvec2, db1):
    dma = pltpu.SemaphoreType.DMA
    return pl.pallas_call(
        attn_bwd_kernel,
        grid=(STEPS,),
        in_specs=[any_spec()] * 6 + [image_spec(DIM), image_spec(3 * DIM), lse_spec(), image_spec(DIM), image_spec(DIM), any_spec(), fixed((TP, 256, DIM)), vec_spec(2, DIM), vec_spec(2, DIM), vec_spec(8, DIM), vec_spec(8, DIM)],
        out_specs=[any_spec()] * 8,
        out_shape=[wide_shape(PACK, DIM), half_shape(DIM, DIM), half_shape(DIM, DIM), half_shape(192, DIM), half_shape(3, 192, DIM), half_shape(DIM, DIM), half_shape(PART, DIM), wide_shape(TP, 16, DIM)],
        scratch_shapes=[pltpu.VMEM((2, CHUNK, DIM), WIDE), pltpu.VMEM((2, CHUNK, DIM), WIDE), pltpu.VMEM((CHUNKS, CHUNK, DIM), WIDE), pltpu.VMEM((GROUP, TOK, DIM), HALF), pltpu.VMEM((TP, 3, 192, DIM), HALF), pltpu.VMEM((ROWS, 3 * DIM), HALF), pltpu.VMEM((TP, 3, 192, DIM), WIDE), pltpu.VMEM((DIM, DIM), WIDE), pltpu.VMEM((TOK, DIM), WIDE), pltpu.VMEM((16, DIM), WIDE), pltpu.VMEM((2, 3, 192, DIM), WIDE), pltpu.VMEM((384, DIM), WIDE), pltpu.VMEM((2, PART, DIM), WIDE), pltpu.VMEM((3, 192, DIM), WIDE), pltpu.VMEM((192, DIM), WIDE), pltpu.VMEM((PART, DIM), WIDE), pltpu.VMEM((3, 192, DIM), HALF), pltpu.VMEM((384, DIM), HALF), pltpu.VMEM((PART, DIM), HALF), dma((CHUNKS,)), dma((CHUNKS,)), dma((3,)), dma((3,)), dma((5,)), dma((5,)), dma((3,)), dma((3,)), dma((2,)), dma((2,)), dma((3, 2)), dma((3,)), pltpu.VMEM((DIM, DIM), HALF), pltpu.VMEM((DIM, DIM), HALF), pltpu.VMEM((192, DIM), HALF), dma((3,)), dma((3,)), dma((5,))],
        compiler_params=params(3),
        cost_estimate=pl.CostEstimate(flops=100_000_000_000, bytes_accessed=80_000_000, transcendentals=12_000_000),
        name='attn_bwd',
    )(keep_b, near_b, keep_a, near_a, keep_o, near_o, e, qkv, lse, dx1, x, wq, wop, ln_scale, ln_bias, dvec2, db1)


def finish_kernel(x2, fc1, fc2, wo, qkv, wp, pos, tiny, x2_out, fc1_out, fc2_out, wo_out, qkv_out, wp_out, pos_out, patch_b, ln_scale, ln_bias, qkv_b, out_b, fc1_b, fc2_b):
    for src, dst in ((x2, x2_out), (fc1, fc1_out), (fc2, fc2_out), (wo, wo_out), (qkv, qkv_out), (wp, wp_out), (pos, pos_out)):
        dst[...] = src[...]

    @pl.when(pl.program_id(0) == 0)
    def _():
        vec = ((tiny[3] + tiny[0]) + (tiny[1] + tiny[2])).astype(HALF)
        patch_b[...] = vec[10:11].reshape(DIM)
        ln_scale[0:1] = vec[8:9]
        ln_scale[1:2] = vec[12:13]
        ln_bias[0:1] = vec[9:10]
        ln_bias[1:2] = vec[13:14]
        fc2_b[...] = vec[14:15].reshape(DIM)
        out_b[...] = vec[15:16].reshape(DIM)
        fc1_b[...] = ((tiny[3, 4:5] + tiny[0, 5:6]) + (tiny[1, 6:7] + tiny[2, 7:8])).astype(HALF).reshape(DIM)
        for s in range(3):
            for h in range(3):
                at = [tiny[j, s:s + 1, 192 * k + 64 * h:192 * k + 64 * h + 64] for k, j in enumerate((3, 0, 1, 2))]
                qkv_b[s, h:h + 1] = ((at[0] + at[1]) + (at[2] + at[3])).astype(HALF)


def finish(x2, fc1, fc2, wo, qkv, wp, pos, tiny):
    arrays = (x2, fc1, fc2, wo, qkv, wp, pos)
    specs = [pl.BlockSpec((a.shape[0] // 4,) + a.shape[1:], lambda i, n=a.ndim: (i,) + (0,) * (n - 1)) for a in arrays]
    smalls = [(DIM,), (2, DIM), (2, DIM), (3, 3, 64), (DIM,), (DIM,), (DIM,)]
    return pl.pallas_call(
        finish_kernel,
        grid=(4,),
        in_specs=specs + [vec_spec(TP, 16, DIM)],
        out_specs=specs + [vec_spec(*shape) for shape in smalls],
        out_shape=[jax.ShapeDtypeStruct(a.shape, a.dtype) for a in arrays] + [half_shape(*shape) for shape in smalls],
        compiler_params=pltpu.CompilerParams(dimension_semantics=('arbitrary',), vmem_limit_bytes=67043328),
        name='finish',
    )(*arrays, tiny)


def group_step(patches, patch_w, patch_b, pos_emb, ln_scale, ln_bias, qkv_w, qkv_b, out_w, out_b, fc1_w, fc1_b, fc2_w, fc2_b, d_out):
    wq = qkv_w.transpose(0, 2, 3, 1).reshape(3, 192, DIM)
    wo = out_w.reshape(192, DIM)
    e, qkv, o, x1, x, lse, dout, y, dh, wq_all, wop_all, bias_all, w1_far, w2_far, keep_a, give_a, part1, part2, dvec_n, db1_n = front(patches, d_out, wq, wo, pos_emb, fc1_w, fc2_w, patch_w, patch_b, qkv_b, fc1_b, out_b, ln_scale, ln_bias)
    x_two, dx1, near_a, keep_o, near_o, keep_b, near_b, dvec2, db1 = mlp_far(give_a, part1, part2, x1, o, dout, y, dh, w1_far, w2_far, bias_all, ln_scale, ln_bias, fc2_b, dvec_n, db1_n)
    _, d_fc1_w, d_fc2_w, d_out_w, d_qkv, d_patch_w, d_pos, tiny = attn_bwd(keep_b, near_b, keep_a, near_a, keep_o, near_o, e, qkv, lse, dx1, x, wq_all, wop_all, ln_scale, ln_bias, dvec2, db1)
    x_two, d_fc1_w, d_fc2_w, d_out_w, d_qkv, d_patch_w, d_pos, d_patch_b, d_ln_scale, d_ln_bias, d_qkv_b, d_out_b, d_fc1_b, d_fc2_b = finish(x_two, d_fc1_w, d_fc2_w, d_out_w, d_qkv.reshape(576, DIM), d_patch_w, d_pos, tiny)
    d_qkv_w = d_qkv.reshape(3, 3, 64, DIM).transpose(0, 3, 1, 2)
    return (x_two, d_patch_w, d_patch_b, d_pos, d_ln_scale, d_ln_bias, d_qkv_w, d_qkv_b, d_out_w.reshape(3, 64, DIM), d_out_b, d_fc1_w, d_fc1_b, d_fc2_w, d_fc2_b)


def solution(mesh):
    in_specs = (P('dp', 'tp', None), P(), P(), P('tp', None), P(), P(), P(None, None, 'tp', None), P(None, 'tp', None), P('tp', None, None), P(), P(None, 'tp'), P('tp'), P('tp', None), P(), P('dp', 'tp', None))
    out_specs = (P('dp', 'tp', None), P('dp', None), P('dp'), P(('dp', 'tp'), None), P('dp', None), P('dp', None), P('dp', None, 'tp', None), P('dp', 'tp', None), P(('dp', 'tp'), None, None), P('dp'), P('dp', 'tp'), P(('dp', 'tp')), P(('dp', 'tp'), None), P('dp'))
    return jax.shard_map(group_step, mesh=mesh, in_specs=in_specs, out_specs=out_specs, check_vma=False)
```

```python
import functools
import jax
import jax.numpy as jnp
from jax import lax
from jax.experimental import pallas as pl
from jax.experimental.pallas import tpu as pltpu
from jax.sharding import PartitionSpec as P

LN_EPS = 1e-6
TP = 4
WIDE = jnp.float32
HALF = jnp.bfloat16
IMAGES = 16
TOK = 256
PART = 64
DIM = 768
GROUP = 1
ROWS = GROUP * TOK
STEPS = IMAGES // GROUP
FRONT = 2
FRONT_STEPS = IMAGES // FRONT
PAIRS = 6
EXP_SCALE = 0.125 * 1.4426950408889634
GELU_C = 0.7978845608028654
GELU_A = 0.044715
AHEAD = 6 // FRONT
PACK = 2 * DIM + 192
EARLY = 256
LATE = DIM - EARLY
CHUNKS = 6
CHUNK = PACK // CHUNKS


def dot_nn(a, b):
    return lax.dot_general(a, b, (((1,), (0,)), ((), ())), preferred_element_type=WIDE)


def dot_nt(a, b):
    return lax.dot_general(a, b, (((1,), (1,)), ((), ())), preferred_element_type=WIDE)


def dot_tn(a, b):
    return lax.dot_general(a, b, (((0,), (0,)), ((), ())), preferred_element_type=WIDE)


def normalize(x_f):
    mean = jnp.sum(x_f, axis=-1, keepdims=True) * (1.0 / DIM)
    centered = x_f - mean
    var = jnp.sum(centered * centered, axis=-1, keepdims=True) * (1.0 / DIM)
    inv = lax.rsqrt(var + LN_EPS)
    return centered * inv, inv


def norm_back(d_out_f, xhat, inv, scale):
    d_hat = d_out_f * scale
    m1 = jnp.sum(d_hat, axis=-1, keepdims=True) * (1.0 / DIM)
    m2 = jnp.sum(d_hat * xhat, axis=-1, keepdims=True) * (1.0 / DIM)
    return (d_hat - m1 - xhat * m2) * inv


def lane_half(j):
    lane = lax.broadcasted_iota(jnp.int32, (1, 128), 1)
    return (lane < 64) if j == 0 else (lane >= 64)


def mask_half(x, j):
    return jnp.where(lane_half(j), x, jnp.zeros_like(x))


def col_sum(x):
    return jnp.sum(x, axis=0, keepdims=True)


def row(ref):
    return ref[...].reshape(1, DIM).astype(WIDE)


def peers():
    me = lax.axis_index('tp')
    core = lax.rem(me, 2)
    chip = lax.div(me, 2)
    return me, core, (me, me + 1 - 2 * core, me + 2 - 4 * chip, 3 - me)


def meet(others):
    barrier = pltpu.get_barrier_semaphore()
    for k in range(1, TP):
        pl.semaphore_signal(barrier, inc=1, device_id={'tp': others[k]}, device_id_type=pl.DeviceIdType.MESH)
    pl.semaphore_wait(barrier, TP - 1)


def push(src, dst, send, recv, peer):
    return pltpu.make_async_remote_copy(src_ref=src, dst_ref=dst, send_sem=send, recv_sem=recv, device_id={'tp': peer}, device_id_type=pl.DeviceIdType.MESH)


def image_rows(owner, group, size):
    return pl.ds(owner * IMAGES + group * size, size)


def group_sends(src, buf, send, recv, others, group):
    return [push(src.at[image_rows(others[k], group, FRONT)], buf.at[k, pl.ds(group * FRONT, FRONT)], send.at[k - 1, group], recv.at[k - 1, group], others[k]) for k in (2, 3, 1)]


def slot_rows(buf, group):
    base = group * FRONT
    return jnp.concatenate([buf[k, base + g] for g in range(FRONT) for k in range(TP)], axis=0)


def mlp_slot(f, base, h2, dout, w1, w2, bias, y, dh2, dw1, dw2, db1_ref):
    hids = []
    dpres = []
    for c in range(w1.shape[1] // 256):
        cols = slice(256 * c, 256 * c + 256)
        units = slice(base + 256 * c, base + 256 * c + 256)
        pre = dot_nn(h2, w1[:, cols]) + bias[f, 3:4, units].astype(WIDE)
        sq = pre * pre
        t = jnp.tanh(pre * (GELU_C + (GELU_C * GELU_A) * sq))
        half_pre = 0.5 * pre
        hids.append((half_pre + half_pre * t).astype(HALF))
        slope = (0.5 + 0.5 * t) + (half_pre * (1.0 - t * t)) * (GELU_C + (3.0 * GELU_C * GELU_A) * sq)
        dpre = dot_nt(dout, w2[cols]).astype(HALF).astype(WIDE) * slope
        db1_ref[f:f + 1, units] += col_sum(dpre)
        dpres.append(dpre.astype(HALF))
    hid = jnp.concatenate(hids, axis=1)
    dpre_h = jnp.concatenate(dpres, axis=1)
    part_y = dot_nn(hid, w2)
    part_h = dot_nt(dpre_h, w1)
    y = part_y if y is None else y + part_y
    dh2 = part_h if dh2 is None else dh2 + part_h

    def grads():
        dw1[...] += dot_tn(h2, dpre_h)
        dw2[...] += dot_tn(dout, hid)

    return y, dh2, grads


def front_kernel(patches, d_out, wq_own, wo_own, pos_own, w1_own, w2_own, wp, patch_b, qkv_b, fc1_b, out_b, ln_scale, ln_bias, e_ref, qkv_ref, o_ref, x1_ref, x_ref, lse_ref, dout_ref, y_ref, dh_ref, wq_out, wop_out, bias_out, w1_far, w2_far, keep_out, give_out, part1_out, part2_out, dvec_ref, db1_ref, xbuf, dbuf, wq, wop, w1, w2, wa1, wa2, bias, bias_own, bqkv, dw1, dw2, dwa1, dwa2, x_send, x_recv, d_send, d_recv, w_send, w_recv, local, done):
    step = pl.program_id(0)
    me, core, others = peers()
    small = []
    for n, (src, cut) in enumerate(((wq_own, None), (wo_own, (0, 192)), (pos_own, (192, 256)))):
        at = [wq.at[k] if cut is None else wop.at[k, cut[0]:cut[1]] for k in range(TP)]
        small.append((push(src, at[2], w_send.at[n, 1], w_recv.at[n, 1], others[2]), push(src, at[1], w_send.at[n, 0], w_recv.at[n, 0], others[1]), push(at[2], at[3], w_send.at[n, 2], w_recv.at[n, 2], others[1])))
    near = [push(w1_own, w1.at[1], w_send.at[3, 0], w_recv.at[3, 0], others[1]), push(w2_own, w2.at[1], w_send.at[4, 0], w_recv.at[4, 0], others[1])]
    early = [push(w1_own.at[:, 0:EARLY], wa1.at[0], w_send.at[6, 0], w_recv.at[6, 0], others[2]), push(w2_own.at[0:EARLY], wa2.at[0], w_send.at[7, 0], w_recv.at[7, 0], others[2])]
    early_relay = [push(wa1.at[0], wa1.at[1], w_send.at[6, 1], w_recv.at[6, 1], others[1]), push(wa2.at[0], wa2.at[1], w_send.at[7, 1], w_recv.at[7, 1], others[1])]
    far = [push(w1_own.at[:, EARLY:DIM], w1_far.at[0], w_send.at[3, 1], w_recv.at[3, 1], others[2]), push(w2_own.at[EARLY:DIM - 256], w2_far.at[0, 0:256], w_send.at[4, 1], w_recv.at[4, 1], others[2]), push(w2_own.at[DIM - 256:DIM], w2_far.at[0, 256:512], w_send.at[8, 0], w_recv.at[8, 0], others[2])]
    relay = [push(w1_far.at[0], w1_far.at[1], w_send.at[3, 2], w_recv.at[3, 2], others[1]), push(w2_far.at[0, 0:256], w2_far.at[1, 0:256], w_send.at[4, 2], w_recv.at[4, 2], others[1]), push(w2_far.at[0, 256:512], w2_far.at[1, 256:512], w_send.at[8, 1], w_recv.at[8, 1], others[1])]
    biases = [push(bias_own, bias.at[k], w_send.at[5, k - 1], w_recv.at[5, k - 1], others[k]) for k in range(1, TP)]
    own = [pltpu.make_async_copy(wq_own, wq.at[0], local.at[0]), pltpu.make_async_copy(wo_own, wop.at[0, 0:192], local.at[1]), pltpu.make_async_copy(pos_own, wop.at[0, 192:256], local.at[2]), pltpu.make_async_copy(patches.at[pl.ds(me * IMAGES, IMAGES)], xbuf.at[0], local.at[3]), pltpu.make_async_copy(d_out.at[pl.ds(me * IMAGES, IMAGES)], dbuf.at[0], local.at[7]), pltpu.make_async_copy(w1_own, w1.at[0], local.at[8]), pltpu.make_async_copy(w2_own, w2.at[0], local.at[9])]
    flush = [pltpu.make_async_copy(wq, wq_out, local.at[4]), pltpu.make_async_copy(wop, wop_out, local.at[5]), pltpu.make_async_copy(bias, bias_out, local.at[6])]

    def arrivals(group):
        return group_sends(patches, xbuf, x_send, x_recv, others, group) + group_sends(d_out, dbuf, d_send, d_recv, others, group)

    @pl.when(step == 0)
    def _():
        bias_own[...] = jnp.zeros_like(bias_own)
        for s in range(3):
            for h in range(3):
                bias_own[s:s + 1, 64 * h:64 * h + 64] = qkv_b[s, h:h + 1]
        bias_own[3:4] = fc1_b[...].reshape(1, DIM)
        bias[0] = bias_own[...]
        meet(others)
        for n in range(3):
            small[n][0].start()
        for c in biases:
            c.start()
        for n in range(3):
            small[n][1].start()
        for g in range(AHEAD):
            for c in arrivals(g) + (early if g == 0 else []):
                c.start()
        for c in own + near:
            c.start()
        dw1[...] = jnp.zeros_like(dw1)
        dw2[...] = jnp.zeros_like(dw2)
        dwa1[...] = jnp.zeros_like(dwa1)
        dwa2[...] = jnp.zeros_like(dwa2)
        dvec_ref[...] = jnp.zeros_like(dvec_ref)
        db1_ref[...] = jnp.zeros_like(db1_ref)
        for n in range(3):
            small[n][0].wait_recv()
            small[n][2].start()
        for c in own:
            c.wait()
        for n in range(3):
            small[n][1].wait_recv()
            small[n][2].wait_recv()
        for c in biases + near:
            c.wait_recv()
        for s in range(3):
            for k in range(TP):
                bqkv[s:s + 1, 192 * k:192 * k + 192] = bias[k, s:s + 1, 0:192].astype(WIDE)
        for c in flush:
            c.start()

    @pl.when(step + AHEAD < FRONT_STEPS)
    def _():
        for c in arrivals(step + AHEAD):
            c.start()

    @pl.when(step == FRONT_STEPS - AHEAD)
    def _():
        for c in far:
            c.start()

    for c in group_sends(patches, xbuf, x_send, x_recv, others, step):
        c.wait_recv()
    x = slot_rows(xbuf, step)
    posb = jnp.concatenate([wop[k, 192:192 + PART] for k in range(TP)], axis=0).astype(WIDE) + row(patch_b)
    emb = dot_nn(x, wp[...]) + jnp.concatenate([posb] * FRONT, axis=0)
    e_h = emb.astype(HALF)
    for g in range(FRONT):
        x_ref[g] = x[TOK * g:TOK * g + TOK]
        e_ref[g] = e_h[TOK * g:TOK * g + TOK]
    e_f = e_h.astype(WIDE)
    xhat, _ = normalize(e_f)
    h1 = (xhat * ln_scale[0:1].astype(WIDE) + ln_bias[0:1].astype(WIDE)).astype(HALF)
    for s in range(3):
        part = (dot_nt(h1, jnp.concatenate([wq[k, s] for k in range(TP)], axis=0)) + bqkv[s:s + 1]).astype(HALF)
        for g in range(FRONT):
            qkv_ref[g, :, DIM * s:DIM * s + DIM] = part[TOK * g:TOK * g + TOK]
    for g in range(FRONT):
        for pr in range(PAIRS):
            q = qkv_ref[g, :, 128 * pr:128 * pr + 128]
            k = qkv_ref[g, :, DIM + 128 * pr:DIM + 128 * pr + 128]
            v = qkv_ref[g, :, 2 * DIM + 128 * pr:2 * DIM + 128 * pr + 128]
            probs = []
            for j in range(2):
                s = dot_nt(k, mask_half(q, j))
                m = jnp.max(s, axis=0, keepdims=True)
                e = jnp.exp2((s - m) * EXP_SCALE)
                l = jnp.sum(e, axis=0, keepdims=True)
                lse_ref[g, 2 * pr + j:2 * pr + j + 1] = m * EXP_SCALE + jnp.log2(l)
                probs.append((e * (1.0 / l)).astype(HALF))
            pv = dot_tn(jnp.concatenate(probs, axis=0), jnp.concatenate([mask_half(v, 0), mask_half(v, 1)], axis=0))
            o_ref[g, :, 128 * pr:128 * pr + 128] = pv.astype(HALF)
    o = jnp.concatenate([o_ref[g] for g in range(FRONT)], axis=0)
    e_f = jnp.concatenate([e_ref[g] for g in range(FRONT)], axis=0).astype(WIDE)
    x1 = (e_f + (dot_nn(o, jnp.concatenate([wop[k, 0:192] for k in range(TP)], axis=0)) + row(out_b))).astype(HALF)
    for g in range(FRONT):
        x1_ref[g] = x1[TOK * g:TOK * g + TOK]

    xhat, _ = normalize(x1.astype(WIDE))
    h2 = (xhat * ln_scale[1:2].astype(WIDE) + ln_bias[1:2].astype(WIDE)).astype(HALF)
    for c in group_sends(d_out, dbuf, d_send, d_recv, others, step):
        c.wait_recv()
    dout = slot_rows(dbuf, step)
    dvec_ref[2:3] += col_sum(dout.astype(WIDE))
    y = None
    dh2 = None
    for f in range(2):
        y, dh2, grads = mlp_slot(f, 0, h2, dout, w1[f], w2[f], bias, y, dh2, dw1.at[f], dw2.at[f], db1_ref)
        grads()

    @pl.when(step == 0)
    def _():
        for n in range(2):
            early[n].wait_recv()
            early_relay[n].start()
        for c in early_relay:
            c.wait_recv()

    for f in range(2):
        y, dh2, grads = mlp_slot(f + 2, 0, h2, dout, wa1[f], wa2[f], bias, y, dh2, dwa1.at[f], dwa2.at[f], db1_ref)
        grads()
    for g in range(FRONT):
        rows = slice(TOK * g, TOK * g + TOK)
        dout_ref[g] = dout[rows]
        y_ref[g] = y[rows]
        dh_ref[g] = dh2[rows]

    @pl.when(step == FRONT_STEPS - 1)
    def _():
        copies = []
        for n, out in enumerate((keep_out, give_out)):
            copies.append(pltpu.make_async_copy(dw1.at[n], out.at[0:DIM], done.at[2 * n]))
            copies.append(pltpu.make_async_copy(dw2.at[n], out.at[DIM:2 * DIM], done.at[2 * n + 1]))
        copies.append(pltpu.make_async_copy(dwa1, part1_out, done.at[4]))
        copies.append(pltpu.make_async_copy(dwa2, part2_out, done.at[5]))
        for c in copies:
            c.start()
        for n in range(3):
            far[n].wait_recv()
            relay[n].start()
        for c in relay:
            c.wait_recv()
        for c in small[0] + small[1] + small[2] + tuple(near + early + early_relay + far + relay + biases):
            c.wait_send()
        for c in copies + flush:
            c.wait()
        for g in range(FRONT_STEPS):
            for c in arrivals(g):
                c.wait_send()


def fixed(shape):
    return pl.BlockSpec(shape, lambda i: (0,) * len(shape), pipeline_mode=pl.Buffered(1))


def image_spec(width, size=GROUP):
    return pl.BlockSpec((size, TOK, width), lambda i: (i, 0, 0))


def lse_spec(size=GROUP):
    return pl.BlockSpec((size, 16, TOK), lambda i: (i, 0, 0))


def any_spec():
    return pl.BlockSpec(memory_space=pl.ANY)


def params(cid):
    return pltpu.CompilerParams(dimension_semantics=('arbitrary',), vmem_limit_bytes=67043328, collective_id=cid, has_side_effects=True)


def image_shape(width):
    return jax.ShapeDtypeStruct((IMAGES, TOK, width), HALF)


def half_shape(*shape):
    return jax.ShapeDtypeStruct(shape, HALF)


def wide_shape(*shape):
    return jax.ShapeDtypeStruct(shape, WIDE)


def vec_spec(*shape):
    return pl.BlockSpec(shape, lambda i: (0,) * len(shape))


def front(patches, d_out, wq, wo, pos, w1, w2, wp, patch_b, qkv_b, fc1_b, out_b, ln_scale, ln_bias):
    dma = pltpu.SemaphoreType.DMA
    wide_image = jax.ShapeDtypeStruct((IMAGES, TOK, DIM), WIDE)
    return pl.pallas_call(
        front_kernel,
        grid=(FRONT_STEPS,),
        in_specs=[any_spec()] * 7 + [fixed((DIM, DIM)), vec_spec(DIM), vec_spec(3, 3, 64), vec_spec(DIM), vec_spec(DIM), vec_spec(2, DIM), vec_spec(2, DIM)],
        out_specs=[image_spec(DIM, FRONT), image_spec(3 * DIM, FRONT)] + [image_spec(DIM, FRONT)] * 3 + [lse_spec(FRONT)] + [image_spec(DIM, FRONT)] * 3 + [any_spec()] * 9 + [vec_spec(8, DIM), vec_spec(8, DIM)],
        out_shape=[image_shape(DIM), image_shape(3 * DIM), image_shape(DIM), image_shape(DIM), image_shape(DIM), wide_shape(IMAGES, 16, TOK), image_shape(DIM), wide_image, wide_image, half_shape(TP, 3, 192, DIM), half_shape(TP, 256, DIM), half_shape(TP, 16, DIM), half_shape(2, DIM, LATE), half_shape(2, LATE, DIM), wide_shape(2 * DIM, DIM), wide_shape(2 * DIM, DIM), wide_shape(2, DIM, EARLY), wide_shape(2, DIM, EARLY), wide_shape(8, DIM), wide_shape(8, DIM)],
        scratch_shapes=[pltpu.VMEM((TP, IMAGES, PART, DIM), HALF), pltpu.VMEM((TP, IMAGES, PART, DIM), HALF), pltpu.VMEM((TP, 3, 192, DIM), HALF), pltpu.VMEM((TP, 256, DIM), HALF), pltpu.VMEM((2, DIM, DIM), HALF), pltpu.VMEM((2, DIM, DIM), HALF), pltpu.VMEM((2, DIM, EARLY), HALF), pltpu.VMEM((2, EARLY, DIM), HALF), pltpu.VMEM((TP, 16, DIM), HALF), pltpu.VMEM((16, DIM), HALF), pltpu.VMEM((8, DIM), WIDE), pltpu.VMEM((2, DIM, DIM), WIDE), pltpu.VMEM((2, DIM, DIM), WIDE), pltpu.VMEM((2, DIM, EARLY), WIDE), pltpu.VMEM((2, DIM, EARLY), WIDE), dma((3, FRONT_STEPS)), dma((3, FRONT_STEPS)), dma((3, FRONT_STEPS)), dma((3, FRONT_STEPS)), dma((9, 3)), dma((9, 3)), dma((10,)), dma((6,))],
        compiler_params=params(0),
        cost_estimate=pl.CostEstimate(flops=120_000_000_000, bytes_accessed=120_000_000, transcendentals=18_000_000),
        name='front',
    )(patches, d_out, wq, wo, pos, w1, w2, wp, patch_b, qkv_b, fc1_b, out_b, ln_scale, ln_bias)


def mlp_far_kernel(give, part1, part2, x1_ref, o_ref, dout_ref, y_ref, dh_ref, w1_far, w2_far, bias, ln_scale, ln_bias, fc2_b, dvec_near, db1_near, x2_out, dx1_ref, near_a, keep_o, near_o, keep_b, near_b, dvec_ref, db1_ref, ybuf, stage, dw1, dw2, dwo, y_send, y_recv, y_own, g_send, g_recv, local):
    step = pl.program_id(0)
    me, core, others = peers()
    slot = lax.rem(step, 2)

    def y_sends(at, group):
        return [push(ybuf.at[at, k], x2_out.at[image_rows(me, group, GROUP)], y_send.at[k - 1, at], y_recv.at[k - 1, group], others[k]) for k in (2, 3, 1)]

    def y_keep(at, group):
        return pltpu.make_async_copy(ybuf.at[at, 0], x2_out.at[image_rows(me, group, GROUP)], y_own.at[at])

    def y_wait(at, group):
        for c in y_sends(at, group):
            c.wait_send()
        y_keep(at, group).wait()

    early = [push(give, near_a, g_send.at[0], g_recv.at[0], others[1]), push(part1.at[1], near_b.at[0:DIM, 0:EARLY], g_send.at[5], g_recv.at[5], others[1]), push(part2.at[1], near_b.at[DIM:2 * DIM, 0:EARLY], g_send.at[6], g_recv.at[6], others[1])]
    grads = [push(dw1.at[1], near_b.at[0:DIM, EARLY:DIM], g_send.at[1], g_recv.at[1], others[1]), push(dw2.at[1], near_b.at[DIM:2 * DIM, EARLY:DIM], g_send.at[2], g_recv.at[2], others[1]), push(dwo.at[576:768], near_b.at[2 * DIM:PACK], g_send.at[3], g_recv.at[3], others[1]), push(dwo.at[192:384], near_o, g_send.at[4], g_recv.at[4], others[1])]
    keeps = [pltpu.make_async_copy(dw1.at[0], keep_b.at[0:DIM, EARLY:DIM], local.at[0]), pltpu.make_async_copy(dw2.at[0], keep_b.at[DIM:2 * DIM, EARLY:DIM], local.at[1]), pltpu.make_async_copy(dwo.at[384:576], keep_b.at[2 * DIM:PACK], local.at[2]), pltpu.make_async_copy(dwo.at[0:192], keep_o, local.at[3])]
    moves = [pltpu.make_async_copy(stage.at[0], keep_b.at[0:DIM, 0:EARLY], local.at[6]), pltpu.make_async_copy(stage.at[1], keep_b.at[DIM:2 * DIM, 0:EARLY], local.at[7])]

    @pl.when(step == 0)
    def _():
        meet(others)
        for c in early:
            c.start()
        loads = [pltpu.make_async_copy(part1.at[0], stage.at[0], local.at[4]), pltpu.make_async_copy(part2.at[0], stage.at[1], local.at[5])]
        for c in loads:
            c.start()
        dw1[...] = jnp.zeros_like(dw1)
        dw2[...] = jnp.zeros_like(dw2)
        for c in loads:
            c.wait()
        for c in moves:
            c.start()
        dwo[...] = jnp.zeros_like(dwo)
        dvec_ref[...] = dvec_near[...]
        db1_ref[...] = db1_near[...]

    x1 = jnp.concatenate([x1_ref[g] for g in range(GROUP)], axis=0)
    dout = jnp.concatenate([dout_ref[g] for g in range(GROUP)], axis=0)
    xhat, inv = normalize(x1.astype(WIDE))
    h2 = (xhat * ln_scale[1:2].astype(WIDE) + ln_bias[1:2].astype(WIDE)).astype(HALF)
    y = jnp.concatenate([y_ref[g] for g in range(GROUP)], axis=0)
    dh2 = jnp.concatenate([dh_ref[g] for g in range(GROUP)], axis=0)
    weight_grads = []
    for f in range(2):
        y, dh2, late = mlp_slot(f + 2, EARLY, h2, dout, w1_far[f], w2_far[f], bias, y, dh2, dw1.at[f], dw2.at[f], db1_ref)
        weight_grads.append(late)
    x2 = (x1.astype(WIDE) + (y + row(fc2_b))).astype(HALF)

    @pl.when(step >= 2)
    def _():
        y_wait(slot, step - 2)

    for g in range(GROUP):
        for k in range(TP):
            ybuf[slot, k, g] = x2[TOK * g + PART * k:TOK * g + PART * k + PART]
    weight_grads[1]()

    for c in y_sends(slot, step):
        c.start()
    y_keep(slot, step).start()

    @pl.when(step == STEPS - 1)
    def _():
        grads[0].start()
        grads[1].start()

    weight_grads[0]()
    dh2 = dh2.astype(HALF).astype(WIDE)
    xhat, inv = normalize(x1.astype(WIDE))
    dout_f = dout.astype(WIDE)
    dx1 = (dout_f + norm_back(dh2, xhat, inv, ln_scale[1:2].astype(WIDE))).astype(HALF)
    dvec_ref[0:1] += col_sum(dh2 * xhat)
    dvec_ref[1:2] += col_sum(dh2)
    dvec_ref[3:4] += col_sum(dx1.astype(WIDE))
    for g in range(GROUP):
        dx1_ref[g] = dx1[TOK * g:TOK * g + TOK]
    o = jnp.concatenate([o_ref[g] for g in range(GROUP)], axis=0)
    dwo[...] += dot_tn(o, dx1)


    @pl.when(step == STEPS - 1)
    def _():
        for c in grads[2:] + keeps:
            c.start()
        for c in keeps + moves:
            c.wait()
        for c in early + grads:
            c.wait()
        for g in range(STEPS):
            for c in y_sends(g % 2, g):
                c.wait_recv()
        for g in (STEPS - 2, STEPS - 1):
            y_wait(g % 2, g)


def mlp_far(give, part1, part2, x1, o, dout, y, dh, w1_far, w2_far, bias, ln_scale, ln_bias, fc2_b, dvec_near, db1_near):
    dma = pltpu.SemaphoreType.DMA
    return pl.pallas_call(
        mlp_far_kernel,
        grid=(STEPS,),
        in_specs=[any_spec()] * 3 + [image_spec(DIM)] * 5 + [fixed((2, DIM, LATE)), fixed((2, LATE, DIM)), fixed((TP, 16, DIM)), vec_spec(2, DIM), vec_spec(2, DIM), vec_spec(DIM), vec_spec(8, DIM), vec_spec(8, DIM)],
        out_specs=[any_spec(), image_spec(DIM)] + [any_spec()] * 5 + [vec_spec(8, DIM), vec_spec(8, DIM)],
        out_shape=[half_shape(TP * IMAGES, PART, DIM), image_shape(DIM), wide_shape(2 * DIM, DIM), wide_shape(192, DIM), wide_shape(192, DIM), wide_shape(PACK, DIM), wide_shape(PACK, DIM), wide_shape(8, DIM), wide_shape(8, DIM)],
        scratch_shapes=[pltpu.VMEM((2, TP, GROUP, PART, DIM), HALF), pltpu.VMEM((2, DIM, EARLY), WIDE), pltpu.VMEM((2, DIM, LATE), WIDE), pltpu.VMEM((2, DIM, LATE), WIDE), pltpu.VMEM((DIM, DIM), WIDE), dma((3, 2)), dma((3, STEPS)), dma((2,)), dma((7,)), dma((7,)), dma((8,))],
        compiler_params=params(2),
        cost_estimate=pl.CostEstimate(flops=70_000_000_000, bytes_accessed=80_000_000, transcendentals=6_000_000),
        name='mlp_far',
    )(give, part1, part2, x1, o, dout, y, dh, w1_far, w2_far, bias, ln_scale, ln_bias, fc2_b, dvec_near, db1_near)


def attn_bwd_kernel(keep_b, near_b, keep_a, near_a, keep_o, near_o, e_ref, qkv_ref, lse_ref, dx1_ref, x_ref, wq_all, wop, ln_scale, ln_bias, dvec2_ref, db1_ref, cross_out, dfc1_out, dfc2_out, dwo_out, dqkv_out, dwp_out, dpos_out, tiny_out, fetch_k, fetch_n, sums, do_buf, wq, dqkv, dwq, dwp, dpos, tiny, near_q, near_p, near_pos, far_q, far_p, far_pos, half_q, half_p, half_pos, p_send, p_recv, t_send, t_recv, n_send, n_recv, f_send, f_recv, h_send, h_recv, c_sem, o_sem, total1, total2, total3, fq_send, fq_recv, local):
    step = pl.program_id(0)
    me, core, others = peers()
    pairs = [push(sums.at[n], cross_out.at[CHUNK * n:CHUNK * n + CHUNK], p_send.at[n], p_recv.at[n], others[2]) for n in range(CHUNKS)]

    def fetch(n):
        rows = pl.ds(n * CHUNK, CHUNK)
        at = lax.rem(n, 2)
        return (pltpu.make_async_copy(keep_b.at[rows], fetch_k.at[at], c_sem.at[0, at]), pltpu.make_async_copy(near_b.at[rows], fetch_n.at[at], c_sem.at[1, at]))

    @pl.when(step == 0)
    def _():
        meet(others)
        for c in fetch(0):
            c.start()

    @pl.when(step < CHUNKS)
    def _():
        @pl.when(step + 1 < CHUNKS)
        def _():
            for c in fetch(step + 1):
                c.start()
        for c in fetch(step):
            c.wait()
        at = lax.rem(step, 2)
        sums[step] = fetch_k[at] + fetch_n[at]

    @pl.when(step == 0)
    def _():
        dwp[...] = jnp.zeros_like(dwp)
        dpos[...] = jnp.zeros_like(dpos)
        tiny[...] = jnp.zeros_like(tiny)

    @pl.when(step < CHUNKS)
    def _():
        push(sums.at[step], cross_out.at[pl.ds(step * CHUNK, CHUNK)], p_send.at[step], p_recv.at[step], others[2]).start()

    @pl.when(step == 0)
    def _():
        wq_copy = pltpu.make_async_copy(wq_all, wq, local.at[4])
        wq_copy.start()
        dwq[...] = jnp.zeros_like(dwq)
        wq_copy.wait()

    wo = jnp.concatenate([wop[k, 0:192] for k in range(TP)], axis=0)
    for g in range(GROUP):
        do_buf[g] = dot_nt(dx1_ref[g], wo).astype(HALF)
    for g in range(GROUP):
        rows = slice(TOK * g, TOK * g + TOK)
        for pr in range(PAIRS):
            cols = slice(128 * pr, 128 * pr + 128)
            q = qkv_ref[g, :, 128 * pr:128 * pr + 128]
            k = qkv_ref[g, :, DIM + 128 * pr:DIM + 128 * pr + 128]
            v = qkv_ref[g, :, 2 * DIM + 128 * pr:2 * DIM + 128 * pr + 128]
            d_o = do_buf[g, :, 128 * pr:128 * pr + 128]
            probs = []
            dscores = []
            for j in range(2):
                s = dot_nt(k, mask_half(q, j))
                p = jnp.exp2(s * EXP_SCALE - lse_ref[g, 2 * pr + j:2 * pr + j + 1])
                dp = dot_nt(v, mask_half(d_o, j)).astype(HALF).astype(WIDE)
                delta = jnp.sum(dp * p, axis=0, keepdims=True)
                ds = (p * ((dp - delta) * 0.125)).astype(HALF)
                probs.append(p.astype(HALF))
                dscores.append(ds)
            dv = dot_nn(jnp.concatenate(probs, axis=1), jnp.concatenate([mask_half(d_o, 0), mask_half(d_o, 1)], axis=0))
            dk = dot_nn(jnp.concatenate(dscores, axis=1), jnp.concatenate([mask_half(q, 0), mask_half(q, 1)], axis=0))
            dq = dot_tn(jnp.concatenate(dscores, axis=0), jnp.concatenate([mask_half(k, 0), mask_half(k, 1)], axis=0))
            dqkv[rows, 128 * pr:128 * pr + 128] = dq.astype(HALF)
            dqkv[rows, DIM + 128 * pr:DIM + 128 * pr + 128] = dk.astype(HALF)
            dqkv[rows, 2 * DIM + 128 * pr:2 * DIM + 128 * pr + 128] = dv.astype(HALF)
    e_f = jnp.concatenate([e_ref[g] for g in range(GROUP)], axis=0).astype(WIDE)
    xhat, inv = normalize(e_f)
    h1 = (xhat * ln_scale[0:1].astype(WIDE) + ln_bias[0:1].astype(WIDE)).astype(HALF)
    dh1 = None
    for s in range(3):
        part = dqkv[:, DIM * s:DIM * s + DIM]
        tiny[s:s + 1] += col_sum(part.astype(WIDE))
        grad = dot_tn(part, h1)
        for k in range(TP):
            dwq[k, s] += grad[192 * k:192 * k + 192]
        term = dot_nn(part, jnp.concatenate([wq[k, s] for k in range(TP)], axis=0))
        dh1 = term if dh1 is None else dh1 + term
    dh1 = dh1.astype(HALF).astype(WIDE)
    dx1 = jnp.concatenate([dx1_ref[g] for g in range(GROUP)], axis=0).astype(WIDE)
    de = (dx1 + norm_back(dh1, xhat, inv, ln_scale[0:1].astype(WIDE))).astype(HALF)
    de_f = de.astype(WIDE)
    tiny[8:9] += col_sum(dh1 * xhat)
    tiny[9:10] += col_sum(dh1)
    acc = de_f[0:TOK]
    for g in range(1, GROUP):
        acc = acc + de_f[TOK * g:TOK * g + TOK]
    dpos[...] += acc
    x = jnp.concatenate([x_ref[g] for g in range(GROUP)], axis=0)
    dwp[...] += dot_tn(x, de)

    @pl.when(step == STEPS - 1)
    def _():
        tiny[4:8] = db1_ref[0:4]
        tiny[10:11] = col_sum(dpos[...])
        tiny[12:16] = dvec2_ref[0:4]
        chip = lax.div(me, 2)
        my_quarter = pl.ds(384 * core + 192 * chip, 192)
        far_quarter = pl.ds(384 * core + 192 * (1 - chip), 192)
        my_part = pl.ds(192 * chip, 192)
        other_half = pl.ds(384 * (1 - core), 384)
        my_half = pl.ds(384 * core, 384)
        near = [push(dwq.at[3], near_q.at[1], n_send.at[0], n_recv.at[0], others[1]), push(dwq.at[1], near_q.at[0], n_send.at[1], n_recv.at[1], others[1]), push(dpos.at[3 * PART:4 * PART], near_pos.at[1], n_send.at[2], n_recv.at[2], others[1]), push(dpos.at[PART:2 * PART], near_pos.at[0], n_send.at[3], n_recv.at[3], others[1]), push(dwp.at[other_half], near_p, n_send.at[4], n_recv.at[4], others[1])]
        tinies = [push(tiny, tiny_out.at[k - 1], t_send.at[k - 1], t_recv.at[k - 1], others[k]) for k in range(1, TP)]
        far = [None, push(dwp.at[far_quarter], far_p, f_send.at[1], f_recv.at[1], others[2]), push(dpos.at[2 * PART:3 * PART], far_pos, f_send.at[2], f_recv.at[2], others[2])]
        far_qs = [push(dwq.at[2, s], far_q.at[s], fq_send.at[s], fq_recv.at[s], others[2]) for s in range(3)]
        near[4].start()
        near[0].start()
        for c in near[1:4] + tinies:
            c.start()
        near[4].wait_recv()
        dwp[my_half] += near_p[...]
        far[1].start()
        near[0].wait_recv()
        for s in range(3):
            dwq[2, s] += near_q[1, s]
        for c in far_qs:
            c.start()
        near[2].wait_recv()
        dpos[2 * PART:3 * PART] += near_pos[1]
        far[2].start()
        near[1].wait_recv()
        near[3].wait_recv()
        far[1].wait()
        half_p[my_part] = (dwp[my_quarter] + far_p[...]).astype(HALF)
        spread = push(half_p.at[my_part], half_p.at[my_part], h_send.at[1], h_recv.at[1], others[2])
        spread.start()
        for c in pairs:
            c.wait()
        outs = []

        def total(keep_ref, near_ref, cross_ref, rows):
            copies = [pltpu.make_async_copy(r, sums.at[n, 0:rows], c_sem.at[n, 0]) for n, r in enumerate((keep_ref, near_ref, cross_ref))]
            for c in copies:
                c.start()
            for c in copies:
                c.wait()
            return (sums[0, 0:rows] + sums[1, 0:rows]) + sums[2, 0:rows]

        for n in range(3):
            rows = slice(256 * n, 256 * n + 256)
            total1[rows] = total(keep_a.at[rows], near_a.at[rows], cross_out.at[rows], 256).astype(HALF)
        outs.append(pltpu.make_async_copy(total1, dfc1_out, o_sem.at[0]))
        outs[0].start()
        for n in range(3):
            rows = slice(DIM + 256 * n, DIM + 256 * n + 256)
            part = total(keep_a.at[rows], near_a.at[rows], cross_out.at[rows], 256)
            total2[:, 256 * n:256 * n + 256] = part.T.astype(HALF)
        outs.append(pltpu.make_async_copy(total2, dfc2_out, o_sem.at[1]))
        outs[1].start()
        total3[...] = total(keep_o, near_o, cross_out.at[2 * DIM:PACK], 192).astype(HALF)
        outs.append(pltpu.make_async_copy(total3, dwo_out, o_sem.at[2]))
        outs[2].start()
        for s in range(3):
            far_qs[s].wait_recv()
            half_q[s] = ((dwq[0, s] + near_q[0, s]) + far_q[s]).astype(HALF)
        q_copy = pltpu.make_async_copy(half_q, dqkv_out, local.at[0])
        q_copy.start()
        spread.wait()
        swap = push(half_p, dwp_out.at[my_half], h_send.at[0], h_recv.at[0], others[1])
        swap.start()
        p_copy = pltpu.make_async_copy(half_p, dwp_out.at[my_half], local.at[1])
        p_copy.start()
        far[2].wait_recv()
        half_pos[...] = ((dpos[0:PART] + near_pos[0]) + far_pos[...]).astype(HALF)
        pos_copy = pltpu.make_async_copy(half_pos, dpos_out, local.at[2])
        pos_copy.start()
        for c in near:
            c.wait_send()
        for c in tinies:
            c.wait()
        for c in far_qs:
            c.wait_send()
        far[2].wait_send()
        tiny_copy = pltpu.make_async_copy(tiny, tiny_out.at[3], local.at[3])
        tiny_copy.start()
        for c in outs:
            c.wait()
        q_copy.wait()
        p_copy.wait()
        pos_copy.wait()
        tiny_copy.wait()
        swap.wait()


def attn_bwd(keep_b, near_b, keep_a, near_a, keep_o, near_o, e, qkv, lse, dx1, x, wq, wop, ln_scale, ln_bias, dvec2, db1):
    dma = pltpu.SemaphoreType.DMA
    return pl.pallas_call(
        attn_bwd_kernel,
        grid=(STEPS,),
        in_specs=[any_spec()] * 6 + [image_spec(DIM), image_spec(3 * DIM), lse_spec(), image_spec(DIM), image_spec(DIM), any_spec(), fixed((TP, 256, DIM)), vec_spec(2, DIM), vec_spec(2, DIM), vec_spec(8, DIM), vec_spec(8, DIM)],
        out_specs=[any_spec()] * 8,
        out_shape=[wide_shape(PACK, DIM), half_shape(DIM, DIM), half_shape(DIM, DIM), half_shape(192, DIM), half_shape(3, 192, DIM), half_shape(DIM, DIM), half_shape(PART, DIM), wide_shape(TP, 16, DIM)],
        scratch_shapes=[pltpu.VMEM((2, CHUNK, DIM), WIDE), pltpu.VMEM((2, CHUNK, DIM), WIDE), pltpu.VMEM((CHUNKS, CHUNK, DIM), WIDE), pltpu.VMEM((GROUP, TOK, DIM), HALF), pltpu.VMEM((TP, 3, 192, DIM), HALF), pltpu.VMEM((ROWS, 3 * DIM), HALF), pltpu.VMEM((TP, 3, 192, DIM), WIDE), pltpu.VMEM((DIM, DIM), WIDE), pltpu.VMEM((TOK, DIM), WIDE), pltpu.VMEM((16, DIM), WIDE), pltpu.VMEM((2, 3, 192, DIM), WIDE), pltpu.VMEM((384, DIM), WIDE), pltpu.VMEM((2, PART, DIM), WIDE), pltpu.VMEM((3, 192, DIM), WIDE), pltpu.VMEM((192, DIM), WIDE), pltpu.VMEM((PART, DIM), WIDE), pltpu.VMEM((3, 192, DIM), HALF), pltpu.VMEM((384, DIM), HALF), pltpu.VMEM((PART, DIM), HALF), dma((CHUNKS,)), dma((CHUNKS,)), dma((3,)), dma((3,)), dma((5,)), dma((5,)), dma((3,)), dma((3,)), dma((2,)), dma((2,)), dma((3, 2)), dma((3,)), pltpu.VMEM((DIM, DIM), HALF), pltpu.VMEM((DIM, DIM), HALF), pltpu.VMEM((192, DIM), HALF), dma((3,)), dma((3,)), dma((5,))],
        compiler_params=params(3),
        cost_estimate=pl.CostEstimate(flops=100_000_000_000, bytes_accessed=80_000_000, transcendentals=12_000_000),
        name='attn_bwd',
    )(keep_b, near_b, keep_a, near_a, keep_o, near_o, e, qkv, lse, dx1, x, wq, wop, ln_scale, ln_bias, dvec2, db1)


def finish_kernel(x2, fc1, fc2, wo, qkv, wp, pos, tiny, x2_out, fc1_out, fc2_out, wo_out, qkv_out, wp_out, pos_out, patch_b, ln_scale, ln_bias, qkv_b, out_b, fc1_b, fc2_b):
    for src, dst in ((x2, x2_out), (fc1, fc1_out), (fc2, fc2_out), (wo, wo_out), (qkv, qkv_out), (wp, wp_out), (pos, pos_out)):
        dst[...] = src[...]

    @pl.when(pl.program_id(0) == 0)
    def _():
        vec = ((tiny[3] + tiny[0]) + (tiny[1] + tiny[2])).astype(HALF)
        patch_b[...] = vec[10:11].reshape(DIM)
        ln_scale[0:1] = vec[8:9]
        ln_scale[1:2] = vec[12:13]
        ln_bias[0:1] = vec[9:10]
        ln_bias[1:2] = vec[13:14]
        fc2_b[...] = vec[14:15].reshape(DIM)
        out_b[...] = vec[15:16].reshape(DIM)
        fc1_b[...] = ((tiny[3, 4:5] + tiny[0, 5:6]) + (tiny[1, 6:7] + tiny[2, 7:8])).astype(HALF).reshape(DIM)
        for s in range(3):
            for h in range(3):
                at = [tiny[j, s:s + 1, 192 * k + 64 * h:192 * k + 64 * h + 64] for k, j in enumerate((3, 0, 1, 2))]
                qkv_b[s, h:h + 1] = ((at[0] + at[1]) + (at[2] + at[3])).astype(HALF)


def finish(x2, fc1, fc2, wo, qkv, wp, pos, tiny):
    arrays = (x2, fc1, fc2, wo, qkv, wp, pos)
    specs = [pl.BlockSpec((a.shape[0] // 2,) + a.shape[1:], lambda i, n=a.ndim: (i,) + (0,) * (n - 1)) for a in arrays]
    smalls = [(DIM,), (2, DIM), (2, DIM), (3, 3, 64), (DIM,), (DIM,), (DIM,)]
    return pl.pallas_call(
        finish_kernel,
        grid=(2,),
        in_specs=specs + [vec_spec(TP, 16, DIM)],
        out_specs=specs + [vec_spec(*shape) for shape in smalls],
        out_shape=[jax.ShapeDtypeStruct(a.shape, a.dtype) for a in arrays] + [half_shape(*shape) for shape in smalls],
        compiler_params=pltpu.CompilerParams(dimension_semantics=('arbitrary',), vmem_limit_bytes=67043328),
        name='finish',
    )(*arrays, tiny)


def group_step(patches, patch_w, patch_b, pos_emb, ln_scale, ln_bias, qkv_w, qkv_b, out_w, out_b, fc1_w, fc1_b, fc2_w, fc2_b, d_out):
    wq = qkv_w.transpose(0, 2, 3, 1).reshape(3, 192, DIM)
    wo = out_w.reshape(192, DIM)
    e, qkv, o, x1, x, lse, dout, y, dh, wq_all, wop_all, bias_all, w1_far, w2_far, keep_a, give_a, part1, part2, dvec_n, db1_n = front(patches, d_out, wq, wo, pos_emb, fc1_w, fc2_w, patch_w, patch_b, qkv_b, fc1_b, out_b, ln_scale, ln_bias)
    x_two, dx1, near_a, keep_o, near_o, keep_b, near_b, dvec2, db1 = mlp_far(give_a, part1, part2, x1, o, dout, y, dh, w1_far, w2_far, bias_all, ln_scale, ln_bias, fc2_b, dvec_n, db1_n)
    _, d_fc1_w, d_fc2_w, d_out_w, d_qkv, d_patch_w, d_pos, tiny = attn_bwd(keep_b, near_b, keep_a, near_a, keep_o, near_o, e, qkv, lse, dx1, x, wq_all, wop_all, ln_scale, ln_bias, dvec2, db1)
    x_two, d_fc1_w, d_fc2_w, d_out_w, d_qkv, d_patch_w, d_pos, d_patch_b, d_ln_scale, d_ln_bias, d_qkv_b, d_out_b, d_fc1_b, d_fc2_b = finish(x_two, d_fc1_w, d_fc2_w, d_out_w, d_qkv.reshape(576, DIM), d_patch_w, d_pos, tiny)
    d_qkv_w = d_qkv.reshape(3, 3, 64, DIM).transpose(0, 3, 1, 2)
    return (x_two, d_patch_w, d_patch_b, d_pos, d_ln_scale, d_ln_bias, d_qkv_w, d_qkv_b, d_out_w.reshape(3, 64, DIM), d_out_b, d_fc1_w, d_fc1_b, d_fc2_w, d_fc2_b)


def solution(mesh):
    in_specs = (P('dp', 'tp', None), P(), P(), P('tp', None), P(), P(), P(None, None, 'tp', None), P(None, 'tp', None), P('tp', None, None), P(), P(None, 'tp'), P('tp'), P('tp', None), P(), P('dp', 'tp', None))
    out_specs = (P('dp', 'tp', None), P('dp', None), P('dp'), P(('dp', 'tp'), None), P('dp', None), P('dp', None), P('dp', None, 'tp', None), P('dp', 'tp', None), P(('dp', 'tp'), None, None), P('dp'), P('dp', 'tp'), P(('dp', 'tp')), P(('dp', 'tp'), None), P('dp'))
    return jax.shard_map(group_step, mesh=mesh, in_specs=in_specs, out_specs=out_specs, check_vma=False)
```

```python
import functools
import jax
import jax.numpy as jnp
from jax import lax
from jax.experimental import pallas as pl
from jax.experimental.pallas import tpu as pltpu
from jax.sharding import PartitionSpec as P

LN_EPS = 1e-6
TP = 4
WIDE = jnp.float32
HALF = jnp.bfloat16
IMAGES = 16
TOK = 256
PART = 64
DIM = 768
GROUP = 1
ROWS = GROUP * TOK
STEPS = IMAGES // GROUP
FRONT = 2
FRONT_STEPS = IMAGES // FRONT
PAIRS = 6
EXP_SCALE = 0.125 * 1.4426950408889634
GELU_C = 0.7978845608028654
GELU_A = 0.044715
AHEAD = 6 // FRONT
PACK = 2 * DIM + 192
EARLY = 256
LATE = DIM - EARLY
CHUNKS = 6
CHUNK = PACK // CHUNKS


def dot_nn(a, b):
    return lax.dot_general(a, b, (((1,), (0,)), ((), ())), preferred_element_type=WIDE)


def dot_nt(a, b):
    return lax.dot_general(a, b, (((1,), (1,)), ((), ())), preferred_element_type=WIDE)


def dot_tn(a, b):
    return lax.dot_general(a, b, (((0,), (0,)), ((), ())), preferred_element_type=WIDE)


def normalize(x_f):
    mean = jnp.sum(x_f, axis=-1, keepdims=True) * (1.0 / DIM)
    centered = x_f - mean
    var = jnp.sum(centered * centered, axis=-1, keepdims=True) * (1.0 / DIM)
    inv = lax.rsqrt(var + LN_EPS)
    return centered * inv, inv


def norm_back(d_out_f, xhat, inv, scale):
    d_hat = d_out_f * scale
    m1 = jnp.sum(d_hat, axis=-1, keepdims=True) * (1.0 / DIM)
    m2 = jnp.sum(d_hat * xhat, axis=-1, keepdims=True) * (1.0 / DIM)
    return (d_hat - m1 - xhat * m2) * inv


def lane_half(j):
    lane = lax.broadcasted_iota(jnp.int32, (1, 128), 1)
    return (lane < 64) if j == 0 else (lane >= 64)


def mask_half(x, j):
    return jnp.where(lane_half(j), x, jnp.zeros_like(x))


def col_sum(x):
    return jnp.sum(x, axis=0, keepdims=True)


def row(ref):
    return ref[...].reshape(1, DIM).astype(WIDE)


def peers():
    me = lax.axis_index('tp')
    core = lax.rem(me, 2)
    chip = lax.div(me, 2)
    return me, core, (me, me + 1 - 2 * core, me + 2 - 4 * chip, 3 - me)


def meet(others):
    barrier = pltpu.get_barrier_semaphore()
    for k in range(1, TP):
        pl.semaphore_signal(barrier, inc=1, device_id={'tp': others[k]}, device_id_type=pl.DeviceIdType.MESH)
    pl.semaphore_wait(barrier, TP - 1)


def push(src, dst, send, recv, peer):
    return pltpu.make_async_remote_copy(src_ref=src, dst_ref=dst, send_sem=send, recv_sem=recv, device_id={'tp': peer}, device_id_type=pl.DeviceIdType.MESH)


def image_rows(owner, group, size):
    return pl.ds(owner * IMAGES + group * size, size)


def group_sends(src, buf, send, recv, others, group):
    return [push(src.at[image_rows(others[k], group, FRONT)], buf.at[k, pl.ds(group * FRONT, FRONT)], send.at[k - 1, group], recv.at[k - 1, group], others[k]) for k in (2, 3, 1)]


def slot_rows(buf, group):
    base = group * FRONT
    return jnp.concatenate([buf[k, base + g] for g in range(FRONT) for k in range(TP)], axis=0)


def mlp_slot(f, base, h2, dout, w1, w2, bias, y, dh2, dw1, dw2, db1_ref):
    hids = []
    dpres = []
    for c in range(w1.shape[1] // 256):
        cols = slice(256 * c, 256 * c + 256)
        units = slice(base + 256 * c, base + 256 * c + 256)
        pre = dot_nn(h2, w1[:, cols]) + bias[f, 3:4, units].astype(WIDE)
        sq = pre * pre
        t = jnp.tanh(pre * (GELU_C + (GELU_C * GELU_A) * sq))
        half_pre = 0.5 * pre
        hids.append((half_pre + half_pre * t).astype(HALF))
        slope = (0.5 + 0.5 * t) + (half_pre * (1.0 - t * t)) * (GELU_C + (3.0 * GELU_C * GELU_A) * sq)
        dpre = dot_nt(dout, w2[cols]).astype(HALF).astype(WIDE) * slope
        db1_ref[f:f + 1, units] += col_sum(dpre)
        dpres.append(dpre.astype(HALF))
    hid = jnp.concatenate(hids, axis=1)
    dpre_h = jnp.concatenate(dpres, axis=1)
    part_y = dot_nn(hid, w2)
    part_h = dot_nt(dpre_h, w1)
    y = part_y if y is None else y + part_y
    dh2 = part_h if dh2 is None else dh2 + part_h

    def grads():
        dw1[...] += dot_tn(h2, dpre_h)
        dw2[...] += dot_tn(dout, hid)

    return y, dh2, grads


def front_kernel(patches, d_out, wq_own, wo_own, pos_own, w1_own, w2_own, wp, patch_b, qkv_b, fc1_b, out_b, ln_scale, ln_bias, e_ref, qkv_ref, o_ref, x1_ref, x_ref, lse_ref, dout_ref, y_ref, dh_ref, wq_out, wop_out, bias_out, w1_far, w2_far, keep_out, give_out, part1_out, part2_out, dvec_ref, db1_ref, xbuf, dbuf, wq, wop, w1, w2, wa1, wa2, bias, bias_own, bqkv, dw1, dw2, dwa1, dwa2, x_send, x_recv, d_send, d_recv, w_send, w_recv, local, done):
    step = pl.program_id(0)
    me, core, others = peers()
    small = []
    for n, (src, cut) in enumerate(((wq_own, None), (wo_own, (0, 192)), (pos_own, (192, 256)))):
        at = [wq.at[k] if cut is None else wop.at[k, cut[0]:cut[1]] for k in range(TP)]
        small.append((push(src, at[2], w_send.at[n, 1], w_recv.at[n, 1], others[2]), push(src, at[1], w_send.at[n, 0], w_recv.at[n, 0], others[1]), push(at[2], at[3], w_send.at[n, 2], w_recv.at[n, 2], others[1])))
    near = [push(w1_own, w1.at[1], w_send.at[3, 0], w_recv.at[3, 0], others[1]), push(w2_own, w2.at[1], w_send.at[4, 0], w_recv.at[4, 0], others[1])]
    early = [push(w1_own.at[:, 0:EARLY], wa1.at[0], w_send.at[6, 0], w_recv.at[6, 0], others[2]), push(w2_own.at[0:EARLY], wa2.at[0], w_send.at[7, 0], w_recv.at[7, 0], others[2])]
    early_relay = [push(wa1.at[0], wa1.at[1], w_send.at[6, 1], w_recv.at[6, 1], others[1]), push(wa2.at[0], wa2.at[1], w_send.at[7, 1], w_recv.at[7, 1], others[1])]
    far = [push(w1_own.at[:, EARLY:DIM], w1_far.at[0], w_send.at[3, 1], w_recv.at[3, 1], others[2]), push(w2_own.at[EARLY:DIM - 256], w2_far.at[0, 0:256], w_send.at[4, 1], w_recv.at[4, 1], others[2]), push(w2_own.at[DIM - 256:DIM], w2_far.at[0, 256:512], w_send.at[8, 0], w_recv.at[8, 0], others[2])]
    relay = [push(w1_far.at[0], w1_far.at[1], w_send.at[3, 2], w_recv.at[3, 2], others[1]), push(w2_far.at[0, 0:256], w2_far.at[1, 0:256], w_send.at[4, 2], w_recv.at[4, 2], others[1]), push(w2_far.at[0, 256:512], w2_far.at[1, 256:512], w_send.at[8, 1], w_recv.at[8, 1], others[1])]
    biases = [push(bias_own, bias.at[k], w_send.at[5, k - 1], w_recv.at[5, k - 1], others[k]) for k in range(1, TP)]
    own = [pltpu.make_async_copy(wq_own, wq.at[0], local.at[0]), pltpu.make_async_copy(wo_own, wop.at[0, 0:192], local.at[1]), pltpu.make_async_copy(pos_own, wop.at[0, 192:256], local.at[2]), pltpu.make_async_copy(patches.at[pl.ds(me * IMAGES, IMAGES)], xbuf.at[0], local.at[3]), pltpu.make_async_copy(d_out.at[pl.ds(me * IMAGES, IMAGES)], dbuf.at[0], local.at[7]), pltpu.make_async_copy(w1_own, w1.at[0], local.at[8]), pltpu.make_async_copy(w2_own, w2.at[0], local.at[9])]
    flush = [pltpu.make_async_copy(wq, wq_out, local.at[4]), pltpu.make_async_copy(wop, wop_out, local.at[5]), pltpu.make_async_copy(bias, bias_out, local.at[6])]

    def arrivals(group):
        return group_sends(patches, xbuf, x_send, x_recv, others, group) + group_sends(d_out, dbuf, d_send, d_recv, others, group)

    @pl.when(step == 0)
    def _():
        bias_own[...] = jnp.zeros_like(bias_own)
        for s in range(3):
            for h in range(3):
                bias_own[s:s + 1, 64 * h:64 * h + 64] = qkv_b[s, h:h + 1]
        bias_own[3:4] = fc1_b[...].reshape(1, DIM)
        bias[0] = bias_own[...]
        meet(others)
        for n in range(3):
            small[n][0].start()
        for c in biases:
            c.start()
        for n in range(3):
            small[n][1].start()
        for g in range(AHEAD):
            for c in arrivals(g) + (early if g == 0 else []):
                c.start()
        for c in own + near:
            c.start()
        dw1[...] = jnp.zeros_like(dw1)
        dw2[...] = jnp.zeros_like(dw2)
        dwa1[...] = jnp.zeros_like(dwa1)
        dwa2[...] = jnp.zeros_like(dwa2)
        dvec_ref[...] = jnp.zeros_like(dvec_ref)
        db1_ref[...] = jnp.zeros_like(db1_ref)
        for n in range(3):
            small[n][0].wait_recv()
            small[n][2].start()
        for c in own:
            c.wait()
        for n in range(3):
            small[n][1].wait_recv()
            small[n][2].wait_recv()
        for c in biases + near:
            c.wait_recv()
        for s in range(3):
            for k in range(TP):
                bqkv[s:s + 1, 192 * k:192 * k + 192] = bias[k, s:s + 1, 0:192].astype(WIDE)
        for c in flush:
            c.start()

    @pl.when(step + AHEAD < FRONT_STEPS)
    def _():
        for c in arrivals(step + AHEAD):
            c.start()

    @pl.when(step == FRONT_STEPS - AHEAD)
    def _():
        for c in far:
            c.start()

    for c in group_sends(patches, xbuf, x_send, x_recv, others, step):
        c.wait_recv()
    x = slot_rows(xbuf, step)
    posb = jnp.concatenate([wop[k, 192:192 + PART] for k in range(TP)], axis=0).astype(WIDE) + row(patch_b)
    emb = dot_nn(x, wp[...]) + jnp.concatenate([posb] * FRONT, axis=0)
    e_h = emb.astype(HALF)
    for g in range(FRONT):
        x_ref[g] = x[TOK * g:TOK * g + TOK]
        e_ref[g] = e_h[TOK * g:TOK * g + TOK]
    e_f = e_h.astype(WIDE)
    xhat, _ = normalize(e_f)
    h1 = (xhat * ln_scale[0:1].astype(WIDE) + ln_bias[0:1].astype(WIDE)).astype(HALF)
    for s in range(3):
        part = (dot_nt(h1, jnp.concatenate([wq[k, s] for k in range(TP)], axis=0)) + bqkv[s:s + 1]).astype(HALF)
        for g in range(FRONT):
            qkv_ref[g, :, DIM * s:DIM * s + DIM] = part[TOK * g:TOK * g + TOK]
    for g in range(FRONT):
        for pr in range(PAIRS):
            q = qkv_ref[g, :, 128 * pr:128 * pr + 128]
            k = qkv_ref[g, :, DIM + 128 * pr:DIM + 128 * pr + 128]
            v = qkv_ref[g, :, 2 * DIM + 128 * pr:2 * DIM + 128 * pr + 128]
            probs = []
            for j in range(2):
                s = dot_nt(k, mask_half(q, j))
                m = jnp.max(s, axis=0, keepdims=True)
                e = jnp.exp2((s - m) * EXP_SCALE)
                l = jnp.sum(e, axis=0, keepdims=True)
                lse_ref[g, 2 * pr + j:2 * pr + j + 1] = m * EXP_SCALE + jnp.log2(l)
                probs.append((e * (1.0 / l)).astype(HALF))
            pv = dot_tn(jnp.concatenate(probs, axis=0), jnp.concatenate([mask_half(v, 0), mask_half(v, 1)], axis=0))
            o_ref[g, :, 128 * pr:128 * pr + 128] = pv.astype(HALF)
    o = jnp.concatenate([o_ref[g] for g in range(FRONT)], axis=0)
    e_f = jnp.concatenate([e_ref[g] for g in range(FRONT)], axis=0).astype(WIDE)
    x1 = (e_f + (dot_nn(o, jnp.concatenate([wop[k, 0:192] for k in range(TP)], axis=0)) + row(out_b))).astype(HALF)
    for g in range(FRONT):
        x1_ref[g] = x1[TOK * g:TOK * g + TOK]

    xhat, _ = normalize(x1.astype(WIDE))
    h2 = (xhat * ln_scale[1:2].astype(WIDE) + ln_bias[1:2].astype(WIDE)).astype(HALF)
    for c in group_sends(d_out, dbuf, d_send, d_recv, others, step):
        c.wait_recv()
    dout = slot_rows(dbuf, step)
    dvec_ref[2:3] += col_sum(dout.astype(WIDE))
    y = None
    dh2 = None
    for f in range(2):
        y, dh2, grads = mlp_slot(f, 0, h2, dout, w1[f], w2[f], bias, y, dh2, dw1.at[f], dw2.at[f], db1_ref)
        grads()

    @pl.when(step == 0)
    def _():
        for n in range(2):
            early[n].wait_recv()
            early_relay[n].start()
        for c in early_relay:
            c.wait_recv()

    for f in range(2):
        y, dh2, grads = mlp_slot(f + 2, 0, h2, dout, wa1[f], wa2[f], bias, y, dh2, dwa1.at[f], dwa2.at[f], db1_ref)
        grads()
    for g in range(FRONT):
        rows = slice(TOK * g, TOK * g + TOK)
        dout_ref[g] = dout[rows]
        y_ref[g] = y[rows]
        dh_ref[g] = dh2[rows]

    @pl.when(step == FRONT_STEPS - 1)
    def _():
        copies = []
        for n, out in enumerate((keep_out, give_out)):
            copies.append(pltpu.make_async_copy(dw1.at[n], out.at[0:DIM], done.at[2 * n]))
            copies.append(pltpu.make_async_copy(dw2.at[n], out.at[DIM:2 * DIM], done.at[2 * n + 1]))
        copies.append(pltpu.make_async_copy(dwa1, part1_out, done.at[4]))
        copies.append(pltpu.make_async_copy(dwa2, part2_out, done.at[5]))
        for c in copies:
            c.start()
        for n in range(3):
            far[n].wait_recv()
            relay[n].start()
        for c in relay:
            c.wait_recv()
        for c in small[0] + small[1] + small[2] + tuple(near + early + early_relay + far + relay + biases):
            c.wait_send()
        for c in copies + flush:
            c.wait()
        for g in range(FRONT_STEPS):
            for c in arrivals(g):
                c.wait_send()


def fixed(shape):
    return pl.BlockSpec(shape, lambda i: (0,) * len(shape), pipeline_mode=pl.Buffered(1))


def image_spec(width, size=GROUP):
    return pl.BlockSpec((size, TOK, width), lambda i: (i, 0, 0))


def lse_spec(size=GROUP):
    return pl.BlockSpec((size, 16, TOK), lambda i: (i, 0, 0))


def any_spec():
    return pl.BlockSpec(memory_space=pl.ANY)


def params(cid):
    return pltpu.CompilerParams(dimension_semantics=('arbitrary',), vmem_limit_bytes=67043328, collective_id=cid, has_side_effects=True)


def image_shape(width):
    return jax.ShapeDtypeStruct((IMAGES, TOK, width), HALF)


def half_shape(*shape):
    return jax.ShapeDtypeStruct(shape, HALF)


def wide_shape(*shape):
    return jax.ShapeDtypeStruct(shape, WIDE)


def vec_spec(*shape):
    return pl.BlockSpec(shape, lambda i: (0,) * len(shape))


def front(patches, d_out, wq, wo, pos, w1, w2, wp, patch_b, qkv_b, fc1_b, out_b, ln_scale, ln_bias):
    dma = pltpu.SemaphoreType.DMA
    wide_image = jax.ShapeDtypeStruct((IMAGES, TOK, DIM), WIDE)
    return pl.pallas_call(
        front_kernel,
        grid=(FRONT_STEPS,),
        in_specs=[any_spec()] * 7 + [fixed((DIM, DIM)), vec_spec(DIM), vec_spec(3, 3, 64), vec_spec(DIM), vec_spec(DIM), vec_spec(2, DIM), vec_spec(2, DIM)],
        out_specs=[image_spec(DIM, FRONT), image_spec(3 * DIM, FRONT)] + [image_spec(DIM, FRONT)] * 3 + [lse_spec(FRONT)] + [image_spec(DIM, FRONT)] * 3 + [any_spec()] * 9 + [vec_spec(8, DIM), vec_spec(8, DIM)],
        out_shape=[image_shape(DIM), image_shape(3 * DIM), image_shape(DIM), image_shape(DIM), image_shape(DIM), wide_shape(IMAGES, 16, TOK), image_shape(DIM), wide_image, wide_image, half_shape(TP, 3, 192, DIM), half_shape(TP, 256, DIM), half_shape(TP, 8, DIM), half_shape(2, DIM, LATE), half_shape(2, LATE, DIM), wide_shape(2 * DIM, DIM), wide_shape(2 * DIM, DIM), wide_shape(2, DIM, EARLY), wide_shape(2, DIM, EARLY), wide_shape(8, DIM), wide_shape(8, DIM)],
        scratch_shapes=[pltpu.VMEM((TP, IMAGES, PART, DIM), HALF), pltpu.VMEM((TP, IMAGES, PART, DIM), HALF), pltpu.VMEM((TP, 3, 192, DIM), HALF), pltpu.VMEM((TP, 256, DIM), HALF), pltpu.VMEM((2, DIM, DIM), HALF), pltpu.VMEM((2, DIM, DIM), HALF), pltpu.VMEM((2, DIM, EARLY), HALF), pltpu.VMEM((2, EARLY, DIM), HALF), pltpu.VMEM((TP, 8, DIM), HALF), pltpu.VMEM((8, DIM), HALF), pltpu.VMEM((8, DIM), WIDE), pltpu.VMEM((2, DIM, DIM), WIDE), pltpu.VMEM((2, DIM, DIM), WIDE), pltpu.VMEM((2, DIM, EARLY), WIDE), pltpu.VMEM((2, DIM, EARLY), WIDE), dma((3, FRONT_STEPS)), dma((3, FRONT_STEPS)), dma((3, FRONT_STEPS)), dma((3, FRONT_STEPS)), dma((9, 3)), dma((9, 3)), dma((10,)), dma((6,))],
        compiler_params=params(0),
        cost_estimate=pl.CostEstimate(flops=120_000_000_000, bytes_accessed=120_000_000, transcendentals=18_000_000),
        name='front',
    )(patches, d_out, wq, wo, pos, w1, w2, wp, patch_b, qkv_b, fc1_b, out_b, ln_scale, ln_bias)


def mlp_far_kernel(give, part1, part2, x1_ref, o_ref, dout_ref, y_ref, dh_ref, w1_far, w2_far, bias, ln_scale, ln_bias, fc2_b, dvec_near, db1_near, x2_out, dx1_ref, near_a, keep_o, near_o, keep_b, near_b, dvec_ref, db1_ref, ybuf, stage, dw1, dw2, dwo, y_send, y_recv, y_own, g_send, g_recv, local):
    step = pl.program_id(0)
    me, core, others = peers()
    slot = lax.rem(step, 2)

    def y_sends(at, group):
        return [push(ybuf.at[at, k], x2_out.at[image_rows(me, group, GROUP)], y_send.at[k - 1, at], y_recv.at[k - 1, group], others[k]) for k in (2, 3, 1)]

    def y_keep(at, group):
        return pltpu.make_async_copy(ybuf.at[at, 0], x2_out.at[image_rows(me, group, GROUP)], y_own.at[at])

    def y_wait(at, group):
        for c in y_sends(at, group):
            c.wait_send()
        y_keep(at, group).wait()

    early = [push(give, near_a, g_send.at[0], g_recv.at[0], others[1]), push(part1.at[1], near_b.at[0:DIM, 0:EARLY], g_send.at[5], g_recv.at[5], others[1]), push(part2.at[1], near_b.at[DIM:2 * DIM, 0:EARLY], g_send.at[6], g_recv.at[6], others[1])]
    grads = [push(dw1.at[1], near_b.at[0:DIM, EARLY:DIM], g_send.at[1], g_recv.at[1], others[1]), push(dw2.at[1], near_b.at[DIM:2 * DIM, EARLY:DIM], g_send.at[2], g_recv.at[2], others[1]), push(dwo.at[576:768], near_b.at[2 * DIM:PACK], g_send.at[3], g_recv.at[3], others[1]), push(dwo.at[192:384], near_o, g_send.at[4], g_recv.at[4], others[1])]
    keeps = [pltpu.make_async_copy(dw1.at[0], keep_b.at[0:DIM, EARLY:DIM], local.at[0]), pltpu.make_async_copy(dw2.at[0], keep_b.at[DIM:2 * DIM, EARLY:DIM], local.at[1]), pltpu.make_async_copy(dwo.at[384:576], keep_b.at[2 * DIM:PACK], local.at[2]), pltpu.make_async_copy(dwo.at[0:192], keep_o, local.at[3])]
    moves = [pltpu.make_async_copy(stage.at[0], keep_b.at[0:DIM, 0:EARLY], local.at[6]), pltpu.make_async_copy(stage.at[1], keep_b.at[DIM:2 * DIM, 0:EARLY], local.at[7])]

    @pl.when(step == 0)
    def _():
        meet(others)
        for c in early:
            c.start()
        loads = [pltpu.make_async_copy(part1.at[0], stage.at[0], local.at[4]), pltpu.make_async_copy(part2.at[0], stage.at[1], local.at[5])]
        for c in loads:
            c.start()
        dw1[...] = jnp.zeros_like(dw1)
        dw2[...] = jnp.zeros_like(dw2)
        for c in loads:
            c.wait()
        for c in moves:
            c.start()
        dwo[...] = jnp.zeros_like(dwo)
        dvec_ref[...] = dvec_near[...]
        db1_ref[...] = db1_near[...]

    x1 = jnp.concatenate([x1_ref[g] for g in range(GROUP)], axis=0)
    dout = jnp.concatenate([dout_ref[g] for g in range(GROUP)], axis=0)
    xhat, inv = normalize(x1.astype(WIDE))
    h2 = (xhat * ln_scale[1:2].astype(WIDE) + ln_bias[1:2].astype(WIDE)).astype(HALF)
    y = jnp.concatenate([y_ref[g] for g in range(GROUP)], axis=0)
    dh2 = jnp.concatenate([dh_ref[g] for g in range(GROUP)], axis=0)
    weight_grads = []
    for f in range(2):
        y, dh2, late = mlp_slot(f + 2, EARLY, h2, dout, w1_far[f], w2_far[f], bias, y, dh2, dw1.at[f], dw2.at[f], db1_ref)
        weight_grads.append(late)
    x2 = (x1.astype(WIDE) + (y + row(fc2_b))).astype(HALF)

    @pl.when(step >= 2)
    def _():
        y_wait(slot, step - 2)

    for g in range(GROUP):
        for k in range(TP):
            ybuf[slot, k, g] = x2[TOK * g + PART * k:TOK * g + PART * k + PART]
    weight_grads[1]()

    for c in y_sends(slot, step):
        c.start()
    y_keep(slot, step).start()

    @pl.when(step == STEPS - 1)
    def _():
        grads[0].start()
        grads[1].start()

    weight_grads[0]()
    dh2 = dh2.astype(HALF).astype(WIDE)
    xhat, inv = normalize(x1.astype(WIDE))
    dout_f = dout.astype(WIDE)
    dx1 = (dout_f + norm_back(dh2, xhat, inv, ln_scale[1:2].astype(WIDE))).astype(HALF)
    dvec_ref[0:1] += col_sum(dh2 * xhat)
    dvec_ref[1:2] += col_sum(dh2)
    dvec_ref[3:4] += col_sum(dx1.astype(WIDE))
    for g in range(GROUP):
        dx1_ref[g] = dx1[TOK * g:TOK * g + TOK]
    o = jnp.concatenate([o_ref[g] for g in range(GROUP)], axis=0)
    dwo[...] += dot_tn(o, dx1)


    @pl.when(step == STEPS - 1)
    def _():
        for c in grads[2:] + keeps:
            c.start()
        for c in keeps + moves:
            c.wait()
        for c in early + grads:
            c.wait()
        for g in range(STEPS):
            for c in y_sends(g % 2, g):
                c.wait_recv()
        for g in (STEPS - 2, STEPS - 1):
            y_wait(g % 2, g)


def mlp_far(give, part1, part2, x1, o, dout, y, dh, w1_far, w2_far, bias, ln_scale, ln_bias, fc2_b, dvec_near, db1_near):
    dma = pltpu.SemaphoreType.DMA
    return pl.pallas_call(
        mlp_far_kernel,
        grid=(STEPS,),
        in_specs=[any_spec()] * 3 + [image_spec(DIM)] * 5 + [fixed((2, DIM, LATE)), fixed((2, LATE, DIM)), fixed((TP, 8, DIM)), vec_spec(2, DIM), vec_spec(2, DIM), vec_spec(DIM), vec_spec(8, DIM), vec_spec(8, DIM)],
        out_specs=[any_spec(), image_spec(DIM)] + [any_spec()] * 5 + [vec_spec(8, DIM), vec_spec(8, DIM)],
        out_shape=[half_shape(TP * IMAGES, PART, DIM), image_shape(DIM), wide_shape(2 * DIM, DIM), wide_shape(192, DIM), wide_shape(192, DIM), wide_shape(PACK, DIM), wide_shape(PACK, DIM), wide_shape(8, DIM), wide_shape(8, DIM)],
        scratch_shapes=[pltpu.VMEM((2, TP, GROUP, PART, DIM), HALF), pltpu.VMEM((2, DIM, EARLY), WIDE), pltpu.VMEM((2, DIM, LATE), WIDE), pltpu.VMEM((2, DIM, LATE), WIDE), pltpu.VMEM((DIM, DIM), WIDE), dma((3, 2)), dma((3, STEPS)), dma((2,)), dma((7,)), dma((7,)), dma((8,))],
        compiler_params=params(2),
        cost_estimate=pl.CostEstimate(flops=70_000_000_000, bytes_accessed=80_000_000, transcendentals=6_000_000),
        name='mlp_far',
    )(give, part1, part2, x1, o, dout, y, dh, w1_far, w2_far, bias, ln_scale, ln_bias, fc2_b, dvec_near, db1_near)


def attn_bwd_kernel(keep_b, near_b, keep_a, near_a, keep_o, near_o, e_ref, qkv_ref, lse_ref, dx1_ref, x_ref, wq_all, wop, ln_scale, ln_bias, dvec2_ref, db1_ref, cross_out, dfc1_out, dfc2_out, dwo_out, dqkv_out, dwp_out, dpos_out, tiny_out, fetch_k, fetch_n, sums, do_buf, wq, dqkv, dwq, dwp, dpos, tiny, near_q, near_p, near_pos, far_q, far_p, far_pos, half_q, half_p, half_pos, p_send, p_recv, t_send, t_recv, n_send, n_recv, f_send, f_recv, h_send, h_recv, c_sem, o_sem, total1, total2, total3, fq_send, fq_recv, local):
    step = pl.program_id(0)
    me, core, others = peers()
    pairs = [push(sums.at[n], cross_out.at[CHUNK * n:CHUNK * n + CHUNK], p_send.at[n], p_recv.at[n], others[2]) for n in range(CHUNKS)]

    def fetch(n):
        rows = pl.ds(n * CHUNK, CHUNK)
        at = lax.rem(n, 2)
        return (pltpu.make_async_copy(keep_b.at[rows], fetch_k.at[at], c_sem.at[0, at]), pltpu.make_async_copy(near_b.at[rows], fetch_n.at[at], c_sem.at[1, at]))

    @pl.when(step == 0)
    def _():
        meet(others)
        for c in fetch(0):
            c.start()

    @pl.when(step < CHUNKS)
    def _():
        @pl.when(step + 1 < CHUNKS)
        def _():
            for c in fetch(step + 1):
                c.start()
        for c in fetch(step):
            c.wait()
        at = lax.rem(step, 2)
        sums[step] = fetch_k[at] + fetch_n[at]

    @pl.when(step == 0)
    def _():
        dwp[...] = jnp.zeros_like(dwp)
        dpos[...] = jnp.zeros_like(dpos)
        tiny[...] = jnp.zeros_like(tiny)

    @pl.when(step < CHUNKS)
    def _():
        push(sums.at[step], cross_out.at[pl.ds(step * CHUNK, CHUNK)], p_send.at[step], p_recv.at[step], others[2]).start()

    @pl.when(step == 0)
    def _():
        wq_copy = pltpu.make_async_copy(wq_all, wq, local.at[4])
        wq_copy.start()
        dwq[...] = jnp.zeros_like(dwq)
        wq_copy.wait()

    wo = jnp.concatenate([wop[k, 0:192] for k in range(TP)], axis=0)
    for g in range(GROUP):
        do_buf[g] = dot_nt(dx1_ref[g], wo).astype(HALF)
    for g in range(GROUP):
        rows = slice(TOK * g, TOK * g + TOK)
        for pr in range(PAIRS):
            cols = slice(128 * pr, 128 * pr + 128)
            q = qkv_ref[g, :, 128 * pr:128 * pr + 128]
            k = qkv_ref[g, :, DIM + 128 * pr:DIM + 128 * pr + 128]
            v = qkv_ref[g, :, 2 * DIM + 128 * pr:2 * DIM + 128 * pr + 128]
            d_o = do_buf[g, :, 128 * pr:128 * pr + 128]
            probs = []
            dscores = []
            for j in range(2):
                s = dot_nt(k, mask_half(q, j))
                p = jnp.exp2(s * EXP_SCALE - lse_ref[g, 2 * pr + j:2 * pr + j + 1])
                dp = dot_nt(v, mask_half(d_o, j)).astype(HALF).astype(WIDE)
                delta = jnp.sum(dp * p, axis=0, keepdims=True)
                ds = (p * ((dp - delta) * 0.125)).astype(HALF)
                probs.append(p.astype(HALF))
                dscores.append(ds)
            dv = dot_nn(jnp.concatenate(probs, axis=1), jnp.concatenate([mask_half(d_o, 0), mask_half(d_o, 1)], axis=0))
            dk = dot_nn(jnp.concatenate(dscores, axis=1), jnp.concatenate([mask_half(q, 0), mask_half(q, 1)], axis=0))
            dq = dot_tn(jnp.concatenate(dscores, axis=0), jnp.concatenate([mask_half(k, 0), mask_half(k, 1)], axis=0))
            dqkv[rows, 128 * pr:128 * pr + 128] = dq.astype(HALF)
            dqkv[rows, DIM + 128 * pr:DIM + 128 * pr + 128] = dk.astype(HALF)
            dqkv[rows, 2 * DIM + 128 * pr:2 * DIM + 128 * pr + 128] = dv.astype(HALF)
    e_f = jnp.concatenate([e_ref[g] for g in range(GROUP)], axis=0).astype(WIDE)
    xhat, inv = normalize(e_f)
    h1 = (xhat * ln_scale[0:1].astype(WIDE) + ln_bias[0:1].astype(WIDE)).astype(HALF)
    dh1 = None
    for s in range(3):
        part = dqkv[:, DIM * s:DIM * s + DIM]
        tiny[s:s + 1] += col_sum(part.astype(WIDE))
        grad = dot_tn(part, h1)
        for k in range(TP):
            dwq[k, s] += grad[192 * k:192 * k + 192]
        term = dot_nn(part, jnp.concatenate([wq[k, s] for k in range(TP)], axis=0))
        dh1 = term if dh1 is None else dh1 + term
    dh1 = dh1.astype(HALF).astype(WIDE)
    dx1 = jnp.concatenate([dx1_ref[g] for g in range(GROUP)], axis=0).astype(WIDE)
    de = (dx1 + norm_back(dh1, xhat, inv, ln_scale[0:1].astype(WIDE))).astype(HALF)
    de_f = de.astype(WIDE)
    tiny[8:9] += col_sum(dh1 * xhat)
    tiny[9:10] += col_sum(dh1)
    acc = de_f[0:TOK]
    for g in range(1, GROUP):
        acc = acc + de_f[TOK * g:TOK * g + TOK]
    dpos[...] += acc
    x = jnp.concatenate([x_ref[g] for g in range(GROUP)], axis=0)
    dwp[...] += dot_tn(x, de)

    @pl.when(step == STEPS - 1)
    def _():
        tiny[4:8] = db1_ref[0:4]
        tiny[10:11] = col_sum(dpos[...])
        tiny[12:16] = dvec2_ref[0:4]
        chip = lax.div(me, 2)
        my_quarter = pl.ds(384 * core + 192 * chip, 192)
        far_quarter = pl.ds(384 * core + 192 * (1 - chip), 192)
        my_part = pl.ds(192 * chip, 192)
        other_half = pl.ds(384 * (1 - core), 384)
        my_half = pl.ds(384 * core, 384)
        near = [push(dwq.at[3], near_q.at[1], n_send.at[0], n_recv.at[0], others[1]), push(dwq.at[1], near_q.at[0], n_send.at[1], n_recv.at[1], others[1]), push(dpos.at[3 * PART:4 * PART], near_pos.at[1], n_send.at[2], n_recv.at[2], others[1]), push(dpos.at[PART:2 * PART], near_pos.at[0], n_send.at[3], n_recv.at[3], others[1]), push(dwp.at[other_half], near_p, n_send.at[4], n_recv.at[4], others[1])]
        tinies = [push(tiny, tiny_out.at[k - 1], t_send.at[k - 1], t_recv.at[k - 1], others[k]) for k in range(1, TP)]
        far = [None, push(dwp.at[far_quarter], far_p, f_send.at[1], f_recv.at[1], others[2]), push(dpos.at[2 * PART:3 * PART], far_pos, f_send.at[2], f_recv.at[2], others[2])]
        far_qs = [push(dwq.at[2, s], far_q.at[s], fq_send.at[s], fq_recv.at[s], others[2]) for s in range(3)]
        near[4].start()
        near[0].start()
        for c in near[1:4] + tinies:
            c.start()
        near[4].wait_recv()
        dwp[my_half] += near_p[...]
        far[1].start()
        near[0].wait_recv()
        for s in range(3):
            dwq[2, s] += near_q[1, s]
        for c in far_qs:
            c.start()
        near[2].wait_recv()
        dpos[2 * PART:3 * PART] += near_pos[1]
        far[2].start()
        near[1].wait_recv()
        near[3].wait_recv()
        far[1].wait()
        half_p[my_part] = (dwp[my_quarter] + far_p[...]).astype(HALF)
        spread = push(half_p.at[my_part], half_p.at[my_part], h_send.at[1], h_recv.at[1], others[2])
        spread.start()
        for c in pairs:
            c.wait()
        outs = []

        def total(keep_ref, near_ref, cross_ref, rows):
            copies = [pltpu.make_async_copy(r, sums.at[n, 0:rows], c_sem.at[n, 0]) for n, r in enumerate((keep_ref, near_ref, cross_ref))]
            for c in copies:
                c.start()
            for c in copies:
                c.wait()
            return (sums[0, 0:rows] + sums[1, 0:rows]) + sums[2, 0:rows]

        for n in range(3):
            rows = slice(256 * n, 256 * n + 256)
            total1[rows] = total(keep_a.at[rows], near_a.at[rows], cross_out.at[rows], 256).astype(HALF)
        outs.append(pltpu.make_async_copy(total1, dfc1_out, o_sem.at[0]))
        outs[0].start()
        for n in range(3):
            rows = slice(DIM + 256 * n, DIM + 256 * n + 256)
            part = total(keep_a.at[rows], near_a.at[rows], cross_out.at[rows], 256)
            total2[:, 256 * n:256 * n + 256] = part.T.astype(HALF)
        outs.append(pltpu.make_async_copy(total2, dfc2_out, o_sem.at[1]))
        outs[1].start()
        total3[...] = total(keep_o, near_o, cross_out.at[2 * DIM:PACK], 192).astype(HALF)
        outs.append(pltpu.make_async_copy(total3, dwo_out, o_sem.at[2]))
        outs[2].start()
        for s in range(3):
            far_qs[s].wait_recv()
            half_q[s] = ((dwq[0, s] + near_q[0, s]) + far_q[s]).astype(HALF)
        q_copy = pltpu.make_async_copy(half_q, dqkv_out, local.at[0])
        q_copy.start()
        spread.wait()
        swap = push(half_p, dwp_out.at[my_half], h_send.at[0], h_recv.at[0], others[1])
        swap.start()
        p_copy = pltpu.make_async_copy(half_p, dwp_out.at[my_half], local.at[1])
        p_copy.start()
        far[2].wait_recv()
        half_pos[...] = ((dpos[0:PART] + near_pos[0]) + far_pos[...]).astype(HALF)
        pos_copy = pltpu.make_async_copy(half_pos, dpos_out, local.at[2])
        pos_copy.start()
        for c in near:
            c.wait_send()
        for c in tinies:
            c.wait()
        for c in far_qs:
            c.wait_send()
        far[2].wait_send()
        tiny_copy = pltpu.make_async_copy(tiny, tiny_out.at[3], local.at[3])
        tiny_copy.start()
        for c in outs:
            c.wait()
        q_copy.wait()
        p_copy.wait()
        pos_copy.wait()
        tiny_copy.wait()
        swap.wait()


def attn_bwd(keep_b, near_b, keep_a, near_a, keep_o, near_o, e, qkv, lse, dx1, x, wq, wop, ln_scale, ln_bias, dvec2, db1):
    dma = pltpu.SemaphoreType.DMA
    return pl.pallas_call(
        attn_bwd_kernel,
        grid=(STEPS,),
        in_specs=[any_spec()] * 6 + [image_spec(DIM), image_spec(3 * DIM), lse_spec(), image_spec(DIM), image_spec(DIM), any_spec(), fixed((TP, 256, DIM)), vec_spec(2, DIM), vec_spec(2, DIM), vec_spec(8, DIM), vec_spec(8, DIM)],
        out_specs=[any_spec()] * 8,
        out_shape=[wide_shape(PACK, DIM), half_shape(DIM, DIM), half_shape(DIM, DIM), half_shape(192, DIM), half_shape(3, 192, DIM), half_shape(DIM, DIM), half_shape(PART, DIM), wide_shape(TP, 16, DIM)],
        scratch_shapes=[pltpu.VMEM((2, CHUNK, DIM), WIDE), pltpu.VMEM((2, CHUNK, DIM), WIDE), pltpu.VMEM((CHUNKS, CHUNK, DIM), WIDE), pltpu.VMEM((GROUP, TOK, DIM), HALF), pltpu.VMEM((TP, 3, 192, DIM), HALF), pltpu.VMEM((ROWS, 3 * DIM), HALF), pltpu.VMEM((TP, 3, 192, DIM), WIDE), pltpu.VMEM((DIM, DIM), WIDE), pltpu.VMEM((TOK, DIM), WIDE), pltpu.VMEM((16, DIM), WIDE), pltpu.VMEM((2, 3, 192, DIM), WIDE), pltpu.VMEM((384, DIM), WIDE), pltpu.VMEM((2, PART, DIM), WIDE), pltpu.VMEM((3, 192, DIM), WIDE), pltpu.VMEM((192, DIM), WIDE), pltpu.VMEM((PART, DIM), WIDE), pltpu.VMEM((3, 192, DIM), HALF), pltpu.VMEM((384, DIM), HALF), pltpu.VMEM((PART, DIM), HALF), dma((CHUNKS,)), dma((CHUNKS,)), dma((3,)), dma((3,)), dma((5,)), dma((5,)), dma((3,)), dma((3,)), dma((2,)), dma((2,)), dma((3, 2)), dma((3,)), pltpu.VMEM((DIM, DIM), HALF), pltpu.VMEM((DIM, DIM), HALF), pltpu.VMEM((192, DIM), HALF), dma((3,)), dma((3,)), dma((5,))],
        compiler_params=params(3),
        cost_estimate=pl.CostEstimate(flops=100_000_000_000, bytes_accessed=80_000_000, transcendentals=12_000_000),
        name='attn_bwd',
    )(keep_b, near_b, keep_a, near_a, keep_o, near_o, e, qkv, lse, dx1, x, wq, wop, ln_scale, ln_bias, dvec2, db1)


def finish_kernel(x2, fc1, fc2, wo, qkv, wp, pos, tiny, x2_out, fc1_out, fc2_out, wo_out, qkv_out, wp_out, pos_out, patch_b, ln_scale, ln_bias, qkv_b, out_b, fc1_b, fc2_b):
    for src, dst in ((x2, x2_out), (fc1, fc1_out), (fc2, fc2_out), (wo, wo_out), (qkv, qkv_out), (wp, wp_out), (pos, pos_out)):
        dst[...] = src[...]

    @pl.when(pl.program_id(0) == 0)
    def _():
        vec = ((tiny[3] + tiny[0]) + (tiny[1] + tiny[2])).astype(HALF)
        patch_b[...] = vec[10:11].reshape(DIM)
        ln_scale[0:1] = vec[8:9]
        ln_scale[1:2] = vec[12:13]
        ln_bias[0:1] = vec[9:10]
        ln_bias[1:2] = vec[13:14]
        fc2_b[...] = vec[14:15].reshape(DIM)
        out_b[...] = vec[15:16].reshape(DIM)
        fc1_b[...] = ((tiny[3, 4:5] + tiny[0, 5:6]) + (tiny[1, 6:7] + tiny[2, 7:8])).astype(HALF).reshape(DIM)
        for s in range(3):
            for h in range(3):
                at = [tiny[j, s:s + 1, 192 * k + 64 * h:192 * k + 64 * h + 64] for k, j in enumerate((3, 0, 1, 2))]
                qkv_b[s, h:h + 1] = ((at[0] + at[1]) + (at[2] + at[3])).astype(HALF)


def finish(x2, fc1, fc2, wo, qkv, wp, pos, tiny):
    arrays = (x2, fc1, fc2, wo, qkv, wp, pos)
    specs = [pl.BlockSpec((a.shape[0] // 2,) + a.shape[1:], lambda i, n=a.ndim: (i,) + (0,) * (n - 1)) for a in arrays]
    smalls = [(DIM,), (2, DIM), (2, DIM), (3, 3, 64), (DIM,), (DIM,), (DIM,)]
    return pl.pallas_call(
        finish_kernel,
        grid=(2,),
        in_specs=specs + [vec_spec(TP, 16, DIM)],
        out_specs=specs + [vec_spec(*shape) for shape in smalls],
        out_shape=[jax.ShapeDtypeStruct(a.shape, a.dtype) for a in arrays] + [half_shape(*shape) for shape in smalls],
        compiler_params=pltpu.CompilerParams(dimension_semantics=('arbitrary',), vmem_limit_bytes=67043328),
        name='finish',
    )(*arrays, tiny)


def group_step(patches, patch_w, patch_b, pos_emb, ln_scale, ln_bias, qkv_w, qkv_b, out_w, out_b, fc1_w, fc1_b, fc2_w, fc2_b, d_out):
    wq = qkv_w.transpose(0, 2, 3, 1).reshape(3, 192, DIM)
    wo = out_w.reshape(192, DIM)
    e, qkv, o, x1, x, lse, dout, y, dh, wq_all, wop_all, bias_all, w1_far, w2_far, keep_a, give_a, part1, part2, dvec_n, db1_n = front(patches, d_out, wq, wo, pos_emb, fc1_w, fc2_w, patch_w, patch_b, qkv_b, fc1_b, out_b, ln_scale, ln_bias)
    x_two, dx1, near_a, keep_o, near_o, keep_b, near_b, dvec2, db1 = mlp_far(give_a, part1, part2, x1, o, dout, y, dh, w1_far, w2_far, bias_all, ln_scale, ln_bias, fc2_b, dvec_n, db1_n)
    _, d_fc1_w, d_fc2_w, d_out_w, d_qkv, d_patch_w, d_pos, tiny = attn_bwd(keep_b, near_b, keep_a, near_a, keep_o, near_o, e, qkv, lse, dx1, x, wq_all, wop_all, ln_scale, ln_bias, dvec2, db1)
    x_two, d_fc1_w, d_fc2_w, d_out_w, d_qkv, d_patch_w, d_pos, d_patch_b, d_ln_scale, d_ln_bias, d_qkv_b, d_out_b, d_fc1_b, d_fc2_b = finish(x_two, d_fc1_w, d_fc2_w, d_out_w, d_qkv.reshape(576, DIM), d_patch_w, d_pos, tiny)
    d_qkv_w = d_qkv.reshape(3, 3, 64, DIM).transpose(0, 3, 1, 2)
    return (x_two, d_patch_w, d_patch_b, d_pos, d_ln_scale, d_ln_bias, d_qkv_w, d_qkv_b, d_out_w.reshape(3, 64, DIM), d_out_b, d_fc1_w, d_fc1_b, d_fc2_w, d_fc2_b)


def solution(mesh):
    in_specs = (P('dp', 'tp', None), P(), P(), P('tp', None), P(), P(), P(None, None, 'tp', None), P(None, 'tp', None), P('tp', None, None), P(), P(None, 'tp'), P('tp'), P('tp', None), P(), P('dp', 'tp', None))
    out_specs = (P('dp', 'tp', None), P('dp', None), P('dp'), P(('dp', 'tp'), None), P('dp', None), P('dp', None), P('dp', None, 'tp', None), P('dp', 'tp', None), P(('dp', 'tp'), None, None), P('dp'), P('dp', 'tp'), P(('dp', 'tp')), P(('dp', 'tp'), None), P('dp'))
    return jax.shard_map(group_step, mesh=mesh, in_specs=in_specs, out_specs=out_specs, check_vma=False)
```
